256 devices in a mesh: member: 2 (over y_hi), seq: 32 (over z, x), head: 4 (over y_lo, core).
Axes of the slice: x: 4, y: 4 (y_hi: 2, y_lo: 2; y = y_hi * 2 + y_lo), z: 8, core: 2. Of those that a mesh axis runs over, the one named last changes fastest.
Arguments:
- tokens: bfloat16 [16384, 5120], P(('seq', 'head')), may hold values from -24 to 24
- lattice: int32 [3, 16384], P(None, 'seq'), may hold values from 0 to 63
- timestep: int32 [32], replicated, may hold values from 0 to 999
- time_weight: bfloat16 [2, 256, 5120], P(None, None, 'seq'), may hold values from -0.375 to 0.375
- query_weight: bfloat16 [2, 5120, 2560], P('member', 'seq', 'head'), may hold values from -6 to 6
- key_weight: bfloat16 [5120, 2560], P('seq', 'head'), may hold values from -6 to 6
- values: bfloat16 [16384, 2560], P(('seq', 'head')), may hold values from -6 to 6
- cotangent: bfloat16 [2, 16384, 2560], P('member', ('seq', 'head')), may hold values from -72 to 72
Outputs:
- fisher: float32 [2, 5120, 2560], P('member', 'seq', 'head')
- merged: float32 [5120, 2560], P('seq', 'head')
The draws below stay inside these ranges and needn't reach their ends.
All inputs are finite; a program needn't handle non-finite values.
Results may differ from the reference program's by a relative error of at most 0.022.
Values may be sent and summed in bfloat16 or wider, within the bound.
A program may use at most 128 MiB of HBM per device.

```python
import math
import jax
import jax.numpy as jnp
from jax import lax

D = 5120
HEAD_SIZE = 128
FREQ = 256
CLIPS = 32
TOKENS = 16384
ATTN = 2560
MEMBERS = 2


def touch_ends(result, own_key, least, largest):
    place = [jax.random.randint(jax.random.fold_in(own_key, axis), (), 0, length) for axis, length in enumerate(result.shape)]
    main_axis = result.shape.index(max(result.shape))
    neighbour = place[:main_axis] + [(place[main_axis] + 1) % result.shape[main_axis]] + place[main_axis + 1:]
    return result.at[tuple(place)].set(least).at[tuple(neighbour)].set(largest)


def strengthened(result, rng, source, target, blocks, factor):
    def block_of(axis_at):
        return (jnp.arange(result.shape[axis_at]) // (result.shape[axis_at] // blocks)).reshape((-1,) + (1,) * (result.ndim - 1 - axis_at))

    one_side = jax.random.permutation(rng, blocks)[block_of(target)]
    far = (block_of(target) + blocks // 2) % blocks
    return jnp.where((block_of(source) == one_side) | (block_of(source) == far), factor * result, result)


def steps_of(own_key, shape, shards, smallest, high):
    loudness, own = 1.0, jax.random.fold_in(own_key, 6)
    for dim, blocks in shards:
        steps = jnp.exp(jax.random.uniform(jax.random.fold_in(own, dim), (blocks,), jnp.float32, smallest / len(shards), high / len(shards)))
        loudness = loudness * jnp.repeat(steps, shape[dim] // blocks).reshape([-1 if axis == dim else 1 for axis in range(len(shape))])
    return loudness


def noise(own_key, extent, scale, most, pieces=(), dtype=jnp.bfloat16):
    loudness = steps_of(own_key, extent, pieces, -0.22, 0.18) if pieces else 1.0
    array = jax.random.normal(own_key, extent, jnp.float32) * scale * loudness
    return jnp.minimum(jnp.maximum(array, -most), most).astype(dtype)


def noise_with(own_key, shape, scale, limit, split, heavy, kind=jnp.bfloat16):
    result = scale * jax.random.normal(own_key, shape, jnp.float32)
    if split:
        result = result * steps_of(own_key, shape, split, -0.22, 0.18)
    return jnp.clip(strengthened(result, jax.random.fold_in(own_key, 3), *heavy), -limit, limit).astype(kind)


def setup_inputs(seed: int = 0) -> dict:
    arg_keys = jax.random.split(jax.random.key(seed), 9)
    tokens = noise_with(arg_keys[0], (TOKENS, D), 1.0, 24.0, ((0, 128),), (0, 1, 128, 5.5))
    lattice = touch_ends(jax.random.randint(arg_keys[1], (3, TOKENS), 0, 64), jax.random.fold_in(arg_keys[1], 1), 0, 63).astype(jnp.int32)
    timestep = touch_ends(jax.random.randint(arg_keys[2], (CLIPS,), 0, 1000), jax.random.fold_in(arg_keys[2], 1), 0, 999).astype(jnp.int32)
    time_weight = noise(arg_keys[3], (2, FREQ, D), FREQ ** -0.5, 0.375, ((2, 32),))
    query_weight = noise(arg_keys[4], (MEMBERS, D, ATTN), 1.0, 6.0, ((0, 2), (1, 32), (2, 4)))
    key_weight = noise(arg_keys[5], (D, ATTN), 1.0, 6.0, ((0, 32), (1, 4)))
    values = noise(arg_keys[6], (TOKENS, ATTN), 1.0, 6.0, ((0, 128),))
    cotangent = noise(arg_keys[7], (MEMBERS, TOKENS, ATTN), 12.0, 72.0, ((0, 2), (1, 128)))
    return {"tokens": tokens, "lattice": lattice, "timestep": timestep, "time_weight": time_weight, "query_weight": query_weight, "key_weight": key_weight, "values": values, "cotangent": cotangent}


damping = 0.01

def time_features(timestep, feature_count):
    halfway = feature_count // 2
    ladder = jnp.arange(halfway).astype(jnp.float32)
    frequency = jnp.exp(-math.log(10000.0) * 2.0 * ladder / feature_count)
    angles = timestep.astype(jnp.float32)[:, None] * frequency[None, :]
    return jnp.concatenate([jnp.cos(angles), jnp.sin(angles)], axis=1).astype(jnp.bfloat16)

def rope_tables(lattice, head_width):
    halfway = head_width // 2
    side_pairs = head_width // 6
    frame_pairs = halfway - 2 * side_pairs
    column = jnp.arange(head_width)
    pair_index = column % halfway
    which_axis = jnp.where(pair_index < frame_pairs, 0, jnp.where(pair_index < frame_pairs + side_pairs, 1, 2))
    anchor = jnp.where(which_axis == 0, 0, jnp.where(which_axis == 1, frame_pairs, frame_pairs + side_pairs))
    pair_span = jnp.where(which_axis == 0, frame_pairs, side_pairs)
    frequency = jnp.exp(-math.log(10000.0) * (pair_index - anchor).astype(jnp.float32) / pair_span.astype(jnp.float32))
    position = lattice.astype(jnp.float32)
    angles = jnp.zeros((lattice.shape[1], head_width), jnp.float32)
    for axis_number in range(3):
        chosen = jnp.where(which_axis == axis_number, frequency, 0.0)
        angles = angles + position[axis_number][:, None] * chosen[None, :]
    sign_flip = jnp.where(column < halfway, -1.0, 1.0).astype(jnp.float32)
    return (jnp.cos(angles), jnp.sin(angles) * sign_flip[None, :])

def normed_rotation(stacked, cosine, sine_table):
    halfway = stacked.shape[2] // 2
    inverse = lax.rsqrt(lax.optimization_barrier(jnp.mean(stacked * stacked, axis=2, keepdims=True)) + 1e-06)
    normed = stacked * inverse
    rotated = normed * cosine[:, None, :] + jnp.roll(normed, halfway, axis=2) * sine_table[:, None, :]
    return (normed, inverse, rotated)

def attention_backward(query_pre, key_pre, values, cotangent, cosine, sine_table, head_width):
    length, width = query_pre.shape
    head_count = width // head_width
    halfway = head_width // 2
    query_normed, query_inverse, query_rotated = normed_rotation(query_pre.reshape(length, head_count, head_width), cosine, sine_table)
    unused_normed, unused_inverse, key_rotated = normed_rotation(key_pre.reshape(length, head_count, head_width), cosine, sine_table)
    query_round = query_rotated.astype(jnp.bfloat16)
    key_wide = key_rotated.astype(jnp.bfloat16).astype(jnp.float32)
    value_heads = values.reshape(length, head_count, head_width).astype(jnp.float32)
    block_rows = min(length, 512)
    block_count = length // block_rows
    score_scale = head_width ** (-0.5)

    def one_block(portion):
        query_block, grad_block = portion
        grad_wide = grad_block.astype(jnp.float32)
        scores = jnp.einsum('qhd,khd->hqk', query_block.astype(jnp.float32), key_wide) * score_scale
        raised = jnp.exp(scores)
        weights = raised / lax.optimization_barrier(jnp.sum(raised, axis=2, keepdims=True))
        rounded = weights.astype(jnp.bfloat16)
        attended = jnp.einsum('hqk,khd->qhd', rounded.astype(jnp.float32), value_heads)
        inner = lax.optimization_barrier(jnp.sum(grad_wide * attended, axis=2))
        grad_weights = jnp.einsum('qhd,khd->hqk', grad_wide, value_heads)
        grad_scores = (weights * (grad_weights - inner.T[:, :, None])).astype(jnp.bfloat16)
        return jnp.einsum('hqk,khd->qhd', grad_scores.astype(jnp.float32), key_wide) * score_scale
    grad_rotated = lax.map(one_block, (query_round.reshape(block_count, block_rows, head_count, head_width), cotangent.reshape(block_count, block_rows, head_count, head_width)))
    grad_rotated = grad_rotated.reshape(length, head_count, head_width)
    grad_normed = grad_rotated * cosine[:, None, :] + jnp.roll(grad_rotated * sine_table[:, None, :], halfway, axis=2)
    grad_query = query_inverse * (grad_normed - query_normed * lax.optimization_barrier(jnp.mean(grad_normed * query_normed, axis=2, keepdims=True)))
    return grad_query.reshape(length, width).astype(jnp.bfloat16)

def reference(tokens, lattice, timestep, time_weight, query_weight, key_weight, values, cotangent):
    model_width = tokens.shape[1]
    clip_count = timestep.shape[0]
    clip_length = tokens.shape[0] // clip_count
    attn_width = key_weight.shape[1]
    features = time_features(timestep, time_weight.shape[1])
    modulation = jnp.einsum('cf,jfd->cjd', features.astype(jnp.float32), time_weight.astype(jnp.float32))
    hidden = tokens.astype(jnp.float32).reshape(clip_count, clip_length, model_width)
    average = lax.optimization_barrier(jnp.mean(hidden, axis=2, keepdims=True))
    centred = hidden - average
    variance = lax.optimization_barrier(jnp.mean(centred * centred, axis=2, keepdims=True))
    normed = centred * lax.rsqrt(variance + 1e-06)
    modulated = (normed * (1.0 + modulation[:, 1][:, None, :]) + modulation[:, 0][:, None, :]).astype(jnp.bfloat16)
    lattices = lattice.reshape(3, clip_count, clip_length).transpose(1, 0, 2)
    value_clips = values.reshape(clip_count, clip_length, attn_width)
    results = []
    for member in range(query_weight.shape[0]):
        own_query = query_weight[member]
        cot_clips = cotangent[member].reshape(clip_count, clip_length, attn_width)

        def step(running, portion):
            rows, grid_rows, value_rows, cot_rows = portion
            cosine, sine_table = rope_tables(grid_rows, HEAD_SIZE)
            query_pre = jnp.dot(rows, own_query, preferred_element_type=jnp.float32)
            key_pre = jnp.dot(rows, key_weight, preferred_element_type=jnp.float32)
            grad_query = attention_backward(query_pre, key_pre, value_rows, cot_rows, cosine, sine_table, HEAD_SIZE)
            grad = lax.dot_general(rows, grad_query, (((0,), (0,)), ((), ())), preferred_element_type=jnp.float32)
            squared = lax.optimization_barrier((grad * grad).astype(jnp.bfloat16))
            return (running + squared.astype(jnp.float32), None)
        running, unused_out = lax.scan(step, jnp.zeros((model_width, attn_width), jnp.float32), (modulated, lattices, value_clips, cot_clips))
        results.append(running)
    fisher = jnp.stack(results, axis=0)
    weighted = fisher + damping
    merged = lax.optimization_barrier(jnp.sum(weighted * query_weight.astype(jnp.float32), axis=0)) / lax.optimization_barrier(jnp.sum(weighted, axis=0))
    return (fisher, merged)
```

```python
import functools
import math

import jax
import jax.numpy as jnp
from jax import lax
from jax.experimental import pallas as pl
from jax.experimental.pallas import tpu as pltpu
from jax.sharding import Mesh
from jax.sharding import PartitionSpec as P

HEAD_SIZE = 128
AXES = ("member", "z", "x", "ylo", "core")
SEQ = ("z", "x")
HEAD = ("ylo", "core")
SEQ_HEAD = ("z", "x", "ylo", "core")
MESH = pl.DeviceIdType.MESH

damping = 0.01
SLICE = 160
HALF = 320
KHEADS = 3
ROW_CHUNK = 32


def time_features(timestep, feature_count):
    halfway = feature_count // 2
    ladder = jnp.arange(halfway).astype(jnp.float32)
    frequency = jnp.exp(-math.log(10000.0) * 2.0 * ladder / feature_count)
    angles = timestep.astype(jnp.float32)[:, None] * frequency[None, :]
    return jnp.concatenate([jnp.cos(angles), jnp.sin(angles)], axis=1).astype(jnp.bfloat16)


def rope_tables(lattice, head_width):
    halfway = head_width // 2
    side_pairs = head_width // 6
    frame_pairs = halfway - 2 * side_pairs
    column = jnp.arange(head_width)
    pair_index = column % halfway
    which_axis = jnp.where(
        pair_index < frame_pairs, 0, jnp.where(pair_index < frame_pairs + side_pairs, 1, 2)
    )
    anchor = jnp.where(
        which_axis == 0, 0, jnp.where(which_axis == 1, frame_pairs, frame_pairs + side_pairs)
    )
    pair_span = jnp.where(which_axis == 0, frame_pairs, side_pairs)
    frequency = jnp.exp(
        -math.log(10000.0)
        * (pair_index - anchor).astype(jnp.float32)
        / pair_span.astype(jnp.float32)
    )
    position = lattice.astype(jnp.float32)
    angles = jnp.zeros((lattice.shape[1], head_width), jnp.float32)
    for axis_number in range(3):
        chosen = jnp.where(which_axis == axis_number, frequency, 0.0)
        angles = angles + position[axis_number][:, None] * chosen[None, :]
    sign_flip = jnp.where(column < halfway, -1.0, 1.0).astype(jnp.float32)
    return (jnp.cos(angles), jnp.sin(angles) * sign_flip[None, :])


def place():
    return tuple(lax.axis_index(a) for a in AXES)


def remote(src, dst, send, recv, to):
    return pltpu.make_async_remote_copy(
        src_ref=src, dst_ref=dst, send_sem=send, recv_sem=recv, device_id=to, device_id_type=MESH
    )


def hello(to):
    pl.semaphore_signal(pltpu.get_barrier_semaphore(), inc=1, device_id=to, device_id_type=MESH)


def gather_kernel(
    tok, shl, w, val, cot, rows, big, vals, cots,
    made, buf1, tot, buf2, mod,
    s_m1, r_m1, s_m2, r_m2, s_s1, r_s1, s_rg, r_rg, s_dd, r_dd,
    s_r1, r_r1, s_r2, r_r2, s_v, r_v,
):
    m, z, x, yl, c = place()
    px, pair, hh = lax.rem(x, 2), x // 2, x // 2
    sib = (m, z, x, yl, 1 - c)
    dz = 1 - 2 * c
    znext = lax.rem(z + dz + 8, 8)
    xc = 2 * pair + c
    home = c == px
    up = (jnp.where(yl == 0, m, 1 - m), z, x, 1 - yl, c)
    down = (jnp.where(yl == 0, 1 - m, m), z, x, 1 - yl, c)

    for j in range(1, 16):
        q = lax.rem(x * 4 + yl * 2 + c + j, 16)
        hello((m, z, q // 4, lax.rem(q, 4) // 2, lax.rem(q, 2)))
    for j in range(1, 8):
        hello((m, lax.rem(z + j, 8), x, yl, c))
    hello((1 - m, z, x, 1 - yl, c))
    pl.semaphore_wait(pltpu.get_barrier_semaphore(), 23)

    def m1(j):
        to = lax.rem(x + j, 4)
        return remote(shl.at[to], buf1.at[x], s_m1.at[j], r_m1.at[j], (m, z, to, yl, c))

    for j in range(1, 4):
        m1(j).start()

    def s1(t):
        return remote(
            w, big.at[z, pl.ds(x * SLICE, SLICE), :], s_s1.at[t], r_s1.at[lax.rem(x, 2)],
            (m, z, c + 2 * t, yl, hh),
        )

    for t in range(2):
        own = (c + 2 * t == x) & (hh == c)

        @pl.when(jnp.logical_not(own))
        def _():
            s1(t).start()

        @pl.when(own)
        def _():
            big[z, pl.ds(pl.multiple_of(x * SLICE, SLICE), SLICE), :] = w[...]

    buf1[x] = shl[x]
    for j in range(1, 4):
        m1(j).wait_recv()
    tot[...] = buf1[0] + buf1[1] + buf1[2] + buf1[3]

    def m2(j):
        to = lax.rem(z + j, 8)
        return remote(tot.at[to], buf2.at[z], s_m2.at[j], r_m2.at[j], (m, to, x, yl, c))

    for j in range(1, 8):
        m2(j).start()
    buf2[z] = tot[z]

    def half_of(n):
        return c if n % 2 == 0 else 1 - c

    def ring(n):
        origin = lax.rem(z - dz * (n // 2) + 8, 8)
        spot = big.at[origin, pl.ds(half_of(n) * HALF, HALF), :]
        return remote(spot, spot, s_rg.at[n], r_rg.at[n], (m, znext, x, yl, c))

    def across(n):
        k = n - 1
        if n == 0:
            spot = big.at[z, pl.ds(c * HALF, HALF), :]
        else:
            origin = lax.rem(z - dz * (k // 2 + 1) + 8, 8)
            spot = big.at[origin, pl.ds(half_of(k) * HALF, HALF), :]
        return remote(spot, spot, s_dd.at[n], r_dd.at[n], sib)

    for u in range(2):
        own = (2 * c + u == x) & home

        @pl.when(jnp.logical_not(own))
        def _():
            remote(
                w, big.at[z, pl.ds((2 * c + u) * SLICE, SLICE), :], s_s1.at[0], r_s1.at[u], sib
            ).wait_recv()

    ring(0).start()
    across(0).start()

    for j in range(1, 8):
        m2(j).wait_recv()
    for k in range(8):
        mod[:, k * 640 : (k + 1) * 640] = buf2[k]

    def r1(t, k):
        return remote(
            made.at[pl.ds(k * ROW_CHUNK, ROW_CHUNK), :],
            rows.at[pl.ds((2 * yl + c) * 128 + k * ROW_CHUNK, ROW_CHUNK), :],
            s_r1.at[t, k], r_r1.at[c, k], (m, z, 2 * pair + t, yl, px),
        )

    for k in range(4):

        @pl.loop(0, ROW_CHUNK // 16)
        def _(i):
            at = pl.multiple_of(k * ROW_CHUNK + i * 16, 16)
            hidden = tok[pl.ds(at, 16), :].astype(jnp.float32)
            average = jnp.mean(hidden, axis=1, keepdims=True)
            centred = hidden - average
            variance = jnp.mean(centred * centred, axis=1, keepdims=True)
            normed = centred * lax.rsqrt(variance + 1e-06)
            out = normed * (1.0 + mod[1:2, :]) + mod[0:1, :]
            made[pl.ds(at, 16), :] = out.astype(jnp.bfloat16)

        for t in range(2):
            own = (2 * pair + t == x) & home

            @pl.when(jnp.logical_not(own))
            def _():
                r1(t, k).start()

            @pl.when(own)
            def _():
                at = pl.multiple_of((2 * yl + c) * 128 + k * ROW_CHUNK, ROW_CHUNK)
                rows[pl.ds(at, ROW_CHUNK), :] = made[k * ROW_CHUNK : (k + 1) * ROW_CHUNK, :]

    across(0).wait_recv()
    ring(1).start()

    def share(a, t, y2):
        h2 = 2 * y2 + t
        src, dst = (val, vals) if a == 0 else (cot, cots)
        return remote(
            src.at[:, h2 * 640 : (h2 + 1) * 640],
            dst.at[pl.ds((2 * yl + c) * 128, 128), :],
            s_v.at[a, t, y2], r_v.at[a, 2 * yl + c], (m, z, 2 * pair + t, y2, px),
        )

    for t in range(2):
        for y2 in range(2):
            own = (2 * pair + t == x) & (y2 == yl) & home

            @pl.when(jnp.logical_not(own))
            def _():
                share(0, t, y2).start()
                share(1, t, y2).start()

            @pl.when(own)
            def _():
                h2 = 2 * y2 + t
                at = pl.multiple_of((2 * yl + c) * 128, 128)
                vals[pl.ds(at, 128), :] = val[:, h2 * 640 : (h2 + 1) * 640]
                cots[pl.ds(at, 128), :] = cot[:, h2 * 640 : (h2 + 1) * 640]

    def r2(p, k, ylo):
        spot = rows.at[pl.ds((2 * ylo + p) * 128 + k * ROW_CHUNK, ROW_CHUNK), :]
        return remote(spot, spot, s_r2.at[p, k], r_r2.at[p, k], up if p == 0 else down)

    for k in range(7):
        if k < 4:
            for p in range(2):
                own = home & (c == p)

                @pl.when(jnp.logical_not(own))
                def _():
                    spot = rows.at[pl.ds((2 * yl + p) * 128 + k * ROW_CHUNK, ROW_CHUNK), :]
                    remote(
                        made.at[pl.ds(k * ROW_CHUNK, ROW_CHUNK), :],
                        spot, s_r1.at[0, k], r_r1.at[p, k], sib,
                    ).wait_recv()

                r2(p, k, yl).start()
        ring(k).wait_recv()
        if k + 2 < 7:
            ring(k + 2).start()
        across(k + 1).start()

    for k in range(4):
        for p in range(2):
            r2(p, k, 1 - yl).wait_recv()
    for hd in range(4):
        own = home & (hd == 2 * yl + c)

        @pl.when(jnp.logical_not(own))
        def _():
            for a, (src, dst) in enumerate(((val, vals), (cot, cots))):
                remote(
                    src.at[:, 0:640], dst.at[hd * 128 : (hd + 1) * 128, :],
                    s_v.at[a, 0, 0], r_v.at[a, hd], sib,
                ).wait_recv()

    for n in range(1, 8):
        across(n).wait_recv()

    for j in range(1, 4):
        m1(j).wait_send()
    for j in range(1, 8):
        m2(j).wait_send()
    for t in range(2):
        own = (c + 2 * t == x) & (hh == c)

        @pl.when(jnp.logical_not(own))
        def _():
            s1(t).wait_send()

        own_r = (2 * pair + t == x) & home

        @pl.when(jnp.logical_not(own_r))
        def _():
            for k in range(4):
                r1(t, k).wait_send()

        for y2 in range(2):
            own_v = (2 * pair + t == x) & (y2 == yl) & home

            @pl.when(jnp.logical_not(own_v))
            def _():
                share(0, t, y2).wait_send()
                share(1, t, y2).wait_send()

    for n in range(7):
        ring(n).wait_send()
    for n in range(8):
        across(n).wait_send()
    for k in range(4):
        for p in range(2):
            r2(p, k, yl).wait_send()


def gather(tok, shl, w, val, cot):
    bf, f32 = jnp.bfloat16, jnp.float32
    width = w.shape[1]
    vmem = pl.BlockSpec(memory_space=pltpu.VMEM)
    dma = pltpu.SemaphoreType.DMA
    return pl.pallas_call(
        gather_kernel,
        out_shape=(
            jax.ShapeDtypeStruct((512, 5120), bf),
            jax.ShapeDtypeStruct((8, 640, width), bf),
            jax.ShapeDtypeStruct((512, 640), bf),
            jax.ShapeDtypeStruct((512, 640), bf),
        ),
        in_specs=[vmem] * 5,
        out_specs=(vmem,) * 4,
        scratch_shapes=[
            pltpu.VMEM((128, 5120), bf),
            pltpu.VMEM((4, 8, 2, 640), f32),
            pltpu.VMEM((8, 2, 640), f32),
            pltpu.VMEM((8, 2, 640), f32),
            pltpu.VMEM((2, 5120), f32),
            dma((4,)), dma((4,)), dma((8,)), dma((8,)), dma((2,)), dma((2,)),
            dma((7,)), dma((7,)), dma((8,)), dma((8,)),
            dma((2, 4)), dma((2, 4)), dma((2, 4)), dma((2, 4)), dma((2, 2, 2)), dma((2, 4)),
        ],
        compiler_params=pltpu.CompilerParams(
            collective_id=0, has_side_effects=True, vmem_limit_bytes=48 * 1024 * 1024
        ),
        cost_estimate=pl.CostEstimate(flops=50_000_000_000, bytes_accessed=20_000_000, transcendentals=0),
        name="gather_all",
    )(tok, shl, w, val, cot)


def scatter_kernel(
    rows, gq, qw, fish, merged,
    own_sq, sib_sq, got_sq, arrived, out, last_sq, last_got, last_arr, fin, xb, qo, wo, wi,
    s_dd, r_dd, s_rg, r_rg, s_x, r_x, s_q, r_q, s_w, r_w,
):
    m, z, x, yl, c = place()
    px, hh = lax.rem(x, 2), x // 2
    sib = (m, z, x, yl, 1 - c)
    dz = 1 - 2 * c
    znext = lax.rem(z + dz + 8, 8)
    mate = (1 - m, z, x, yl, c)
    f32, bf = jnp.float32, jnp.bfloat16

    for j in range(1, 8):
        q = lax.rem(x * 2 + c + j, 8)
        hello((m, z, q // 2, yl, lax.rem(q, 2)))
    hello((m, lax.rem(z + 1, 8), x, yl, c))
    hello((m, lax.rem(z + 7, 8), x, yl, c))
    hello(mate)
    pl.semaphore_wait(pltpu.get_barrier_semaphore(), 10)

    copy_q = remote(qw, qo, s_q, r_q, mate)
    copy_q.start()

    def squares(zs, dst):
        @pl.loop(0, 5)
        def _(r):
            cols = pl.ds(pl.multiple_of(zs * 640 + r * 128, 128), 128)
            g = lax.dot_general(
                rows[:, cols], gq[...], (((0,), (0,)), ((), ())), preferred_element_type=f32
            )
            dst[pl.ds(pl.multiple_of(r * 128, 128), 128), :] = (g * g).astype(bf)

    mine, other = pl.ds(c * HALF, HALF), pl.ds((1 - c) * HALF, HALF)

    def zat(j):
        return lax.rem(z + dz * j + 16, 8)

    def across(q):
        if q == 0:
            src, dst = own_sq.at[3, other, :], got_sq.at[3, other, :]
        elif q < 4:
            src, dst = sib_sq.at[3 - q], got_sq.at[3 - q]
        elif q == 4:
            src, dst = last_sq.at[other, :], last_got
        else:
            src, dst = arrived.at[5], last_arr
        return remote(src, dst, s_dd.at[q], r_dd.at[q], sib)

    def across_in(q):
        if q == 0:
            return remote(
                own_sq.at[3, mine, :], got_sq.at[3, mine, :], s_dd.at[q], r_dd.at[q], sib
            )
        return across(q)

    def ring(n):
        return remote(out.at[n], arrived.at[n], s_rg.at[n], r_rg.at[n], (m, znext, x, yl, c))

    def send_on(n):
        j = (8 - n) // 2 - 1
        base = (c if n % 2 == 0 else 1 - c) * HALF

        @pl.loop(0, HALF // 32)
        def _(i):
            at = pl.ds(pl.multiple_of(i * 32, 32), 32)
            far = pl.ds(pl.multiple_of(base + i * 32, 32), 32)
            total = own_sq[j, far, :].astype(f32) + got_sq[j, far, :].astype(f32)
            if n >= 2:
                total = total + arrived[n - 2, at, :].astype(f32)
            out[n, at, :] = total.astype(bf)

        ring(n).start()

    squares(zat(4), own_sq.at[3])
    across(0).start()
    squares(zat(-3), sib_sq.at[2])
    across(1).start()
    across_in(0).wait_recv()
    send_on(0)
    squares(zat(3), own_sq.at[2])
    across_in(1).wait_recv()
    send_on(1)
    squares(zat(-2), sib_sq.at[1])
    across(2).start()
    squares(zat(2), own_sq.at[1])
    ring(0).wait_recv()
    send_on(2)
    across_in(2).wait_recv()
    ring(1).wait_recv()
    send_on(3)
    squares(zat(-1), sib_sq.at[0])
    across(3).start()
    squares(zat(1), own_sq.at[0])
    ring(2).wait_recv()
    send_on(4)
    across_in(3).wait_recv()
    ring(3).wait_recv()
    send_on(5)
    squares(z, last_sq)
    across(4).start()
    ring(4).wait_recv()
    send_on(6)
    ring(5).wait_recv()
    across(5).start()
    across_in(4).wait_recv()
    across_in(5).wait_recv()
    ring(6).wait_recv()

    for u in range(2):

        @pl.loop(0, SLICE // 32)
        def _(i):
            at = pl.ds(pl.multiple_of(u * SLICE + i * 32, 32), 32)
            far = pl.ds(pl.multiple_of(c * HALF + u * SLICE + i * 32, 32), 32)
            total = last_sq[far, :].astype(f32) + last_got[at, :].astype(f32)
            total = total + arrived[6, at, :].astype(f32) + last_arr[at, :].astype(f32)
            fin[u, pl.ds(pl.multiple_of(i * 32, 32), 32), :] = total.astype(bf)

    def xs(u):
        return remote(
            fin.at[u], xb.at[hh], s_x.at[u], r_x.at[hh], (m, z, 2 * c + u, yl, px)
        )

    for u in range(2):
        own = (2 * c + u == x) & (px == c)

        @pl.when(jnp.logical_not(own))
        def _():
            xs(u).start()

        @pl.when(own)
        def _():
            xb[hh] = fin[u]

    for t in range(2):
        own = (c + 2 * t == x) & (hh == c)

        @pl.when(jnp.logical_not(own))
        def _():
            remote(fin.at[0], xb.at[t], s_x.at[0], r_x.at[t], sib).wait_recv()

    total = xb[0].astype(f32) + xb[1].astype(f32)
    fish[...] = total
    wo[...] = (total + damping).astype(bf)
    copy_w = remote(wo, wi, s_w, r_w, mate)
    copy_w.start()
    copy_q.wait_recv()
    copy_w.wait_recv()
    first = m == 0
    wa, wb = wo[...].astype(f32), wi[...].astype(f32)
    qa, qb = qw[...].astype(f32), qo[...].astype(f32)
    w0, w1 = jnp.where(first, wa, wb), jnp.where(first, wb, wa)
    q0, q1 = jnp.where(first, qa, qb), jnp.where(first, qb, qa)
    merged[...] = (w0 * q0 + w1 * q1) / (w0 + w1)

    copy_q.wait_send()
    copy_w.wait_send()
    for u in range(2):
        own = (2 * c + u == x) & (px == c)

        @pl.when(jnp.logical_not(own))
        def _():
            xs(u).wait_send()

    for n in range(7):
        ring(n).wait_send()
    for q in range(6):
        across(q).wait_send()


def scatter(rows, gq, qw):
    bf, f32 = jnp.bfloat16, jnp.float32
    vmem = pl.BlockSpec(memory_space=pltpu.VMEM)
    dma = pltpu.SemaphoreType.DMA
    return pl.pallas_call(
        scatter_kernel,
        out_shape=(
            jax.ShapeDtypeStruct((SLICE, 640), f32),
            jax.ShapeDtypeStruct((SLICE, 640), f32),
        ),
        in_specs=[vmem] * 3,
        out_specs=(vmem,) * 2,
        scratch_shapes=[
            pltpu.VMEM((4, 640, 640), bf),
            pltpu.VMEM((3, 640, 640), bf),
            pltpu.VMEM((4, 640, 640), bf),
            pltpu.VMEM((7, HALF, 640), bf),
            pltpu.VMEM((7, HALF, 640), bf),
            pltpu.VMEM((640, 640), bf),
            pltpu.VMEM((HALF, 640), bf),
            pltpu.VMEM((HALF, 640), bf),
            pltpu.VMEM((2, SLICE, 640), bf),
            pltpu.VMEM((2, SLICE, 640), bf),
            pltpu.VMEM((SLICE, 640), bf),
            pltpu.VMEM((SLICE, 640), bf),
            pltpu.VMEM((SLICE, 640), bf),
            dma((6,)), dma((6,)), dma((7,)), dma((7,)), dma((2,)), dma((2,)),
            dma, dma, dma, dma,
        ],
        compiler_params=pltpu.CompilerParams(
            collective_id=1, has_side_effects=True, vmem_limit_bytes=48 * 1024 * 1024
        ),
        cost_estimate=pl.CostEstimate(flops=30_000_000_000, bytes_accessed=20_000_000, transcendentals=0),
        name="square_scatter",
    )(rows, gq, qw)


def normed_rotation(pre, cosine, sine_table):
    halfway = pre.shape[2] // 2
    inverse = lax.rsqrt(jnp.mean(pre * pre, axis=2, keepdims=True) + 1e-06)
    normed = pre * inverse
    rotated = (
        normed * cosine[None] + jnp.roll(normed, halfway, axis=2) * sine_table[None]
    )
    return (normed, inverse, rotated.astype(jnp.bfloat16))


def on_device(tokens, lattice, timestep, time_weight, query_weight, key_weight, values, cotangent):
    member, z, x, ylo, core = place()
    f32, bf = jnp.float32, jnp.bfloat16
    features = time_features(timestep, time_weight.shape[1])
    local = jnp.einsum("cf,jfd->cjd", features, time_weight, preferred_element_type=f32)
    local = local.reshape(8, 4, 2, SLICE).transpose(1, 0, 2, 3)
    local = lax.dynamic_update_slice(
        jnp.zeros((4, 8, 2, 640), f32), local, (0, 0, 0, x * SLICE)
    )
    own_query = query_weight[0]
    own_key = lax.dynamic_slice(key_weight, (0, member * 256), (SLICE, KHEADS * HEAD_SIZE))
    both = jnp.concatenate([own_query, own_key], axis=1)

    swap = []
    for i in range(2):
        for a in range(2):
            for c in range(2):
                swap.append(((2 * i + c) * 2 + a, (2 * i + a) * 2 + c))
    grid = lax.ppermute(lattice.astype(f32), ("x", "core"), swap)
    cosine, sine_table = rope_tables(grid, HEAD_SIZE)

    rows, weights, value_heads, cot_heads = gather(tokens, local, both, values, cotangent[0])
    weights = weights.reshape(5120, 640 + KHEADS * HEAD_SIZE)

    def heads(a, count):
        return a.reshape(512, count, HEAD_SIZE).transpose(1, 0, 2)

    pre = jnp.dot(rows, weights, preferred_element_type=f32)
    key_part = normed_rotation(heads(pre[:, 640:], KHEADS), cosine, sine_table)[2]
    sent = jnp.where(member == 0, key_part[:2], key_part[1:])
    came = lax.ppermute(sent, "member", [(0, 1), (1, 0)])
    key_round = jnp.where(
        member == 0,
        jnp.concatenate([key_part, came], axis=0),
        jnp.concatenate([came, key_part], axis=0),
    )
    query_normed, query_inverse, query_round = normed_rotation(
        heads(pre[:, :640], 5), cosine, sine_table
    )
    vh, ch = heads(value_heads, 5), heads(cot_heads, 5)
    scale = HEAD_SIZE ** (-0.5)
    grad_weights = jnp.einsum("hqd,hkd->hqk", ch, vh, preferred_element_type=f32)
    scores = jnp.einsum("hqd,hkd->hqk", query_round, key_round, preferred_element_type=f32) * scale
    raised = jnp.exp(scores)
    probs = raised / jnp.sum(raised, axis=2, keepdims=True)
    attended = jnp.einsum("hqk,hkd->hqd", probs.astype(bf), vh, preferred_element_type=f32)
    inner = jnp.sum(ch.astype(f32) * attended, axis=2, keepdims=True)
    grad_scores = (probs * (grad_weights - inner)).astype(bf)
    grad_rotated = (
        jnp.einsum("hqk,hkd->hqd", grad_scores, key_round, preferred_element_type=f32) * scale
    )
    grad_normed = grad_rotated * cosine[None] + jnp.roll(
        grad_rotated * sine_table[None], HEAD_SIZE // 2, axis=2
    )
    grad_query = query_inverse * (
        grad_normed - query_normed * jnp.mean(grad_normed * query_normed, axis=2, keepdims=True)
    )
    grad_query = grad_query.transpose(1, 0, 2).reshape(512, 640).astype(bf)
    fisher, merged = scatter(rows, grad_query, own_query)
    return (fisher[None], merged)


def solution(mesh):
    finer = Mesh(mesh.devices.reshape(mesh.shape["member"], 8, 4, 2, 2), AXES)
    in_specs = (
        P(SEQ_HEAD, None),
        P(None, SEQ),
        P(),
        P(None, None, SEQ),
        P("member", SEQ, HEAD),
        P(SEQ, HEAD),
        P(SEQ_HEAD, None),
        P("member", SEQ_HEAD, None),
    )
    out_specs = (P("member", SEQ, HEAD), P(SEQ, HEAD))
    return jax.shard_map(
        on_device, mesh=finer, in_specs=in_specs, out_specs=out_specs, check_vma=False
    )
```

```python
import math

import jax
import jax.numpy as jnp
from jax import lax
from jax.experimental import pallas as pl
from jax.experimental.pallas import tpu as pltpu
from jax.sharding import Mesh
from jax.sharding import PartitionSpec as P

HEAD_SIZE = 128
AXES = ("member", "z", "x", "ylo", "core")
SEQ = ("z", "x")
HEAD = ("ylo", "core")
SEQ_HEAD = ("z", "x", "ylo", "core")
MESH = pl.DeviceIdType.MESH

damping = 0.01
SLICE = 160
HALF = 320
KW = 384
ROW_CHUNK = 32
BLOCK = 128
F32, BF = jnp.float32, jnp.bfloat16


def place():
    return tuple(lax.axis_index(a) for a in AXES)


def remote(src, dst, send, recv, to):
    return pltpu.make_async_remote_copy(
        src_ref=src, dst_ref=dst, send_sem=send, recv_sem=recv, device_id=to, device_id_type=MESH
    )


def hello(to):
    pl.semaphore_signal(pltpu.get_barrier_semaphore(), inc=1, device_id=to, device_id_type=MESH)


def rope_frequency():
    halfway, side = HEAD_SIZE // 2, HEAD_SIZE // 6
    frame = halfway - 2 * side
    shape = (8, HEAD_SIZE)
    row = lax.broadcasted_iota(jnp.int32, shape, 0)
    column = lax.broadcasted_iota(jnp.int32, shape, 1)
    pair = jnp.where(column < halfway, column, column - halfway)
    axis = jnp.where(pair < frame, 0, jnp.where(pair < frame + side, 1, 2))
    anchor = jnp.where(axis == 0, 0, jnp.where(axis == 1, frame, frame + side))
    span = jnp.where(axis == 0, frame, side).astype(F32)
    frequency = jnp.exp(-math.log(10000.0) * (pair - anchor).astype(F32) / span)
    return jnp.where(row == axis, frequency, 0.0)


def kernel(
    when, tw, lat, tok_hbm, wq_hbm, wk_hbm, val, cot,
    xb, wo, wi, qo, wqv,
    tok, wkv, bigq, bigk, rows, vals, cots, made,
    ang, wide, shl, buf1, tot, buf2, mod, latb, latf, cosb, sinb,
    qacc, kacc, krot, gq,
    own_sq, sib_sq, got_sq, arrived, out, last_sq, last_got, last_arr, fin,
    s_in, s_self, s_l, r_l,
    s_m1, r_m1, s_m2, r_m2, s_s1, r_s1, s_rg, r_rg, s_dd, r_dd,
    s_r1, r_r1, s_r2, r_r2, s_v, r_v, s_k, r_k,
    s_sd, r_sd, s_sr, r_sr, s_x, r_x, s_q, r_q, s_w, r_w,
):
    m, z, x, yl, c = place()
    px, pair, hh = lax.rem(x, 2), x // 2, x // 2
    sib = (m, z, x, yl, 1 - c)
    mate = (1 - m, z, x, yl, c)
    dz = 1 - 2 * c
    znext = lax.rem(z + dz + 8, 8)
    home = c == px
    up = (jnp.where(yl == 0, m, 1 - m), z, x, 1 - yl, c)
    down = (jnp.where(yl == 0, 1 - m, m), z, x, 1 - yl, c)
    away = jnp.logical_not(home)

    loads = [
        pltpu.make_async_copy(wk_hbm.at[:, pl.ds(pl.multiple_of(m * 256, 128), KW)], wkv, s_in.at[0]),
        pltpu.make_async_copy(wq_hbm, wqv, s_in.at[1]),
        pltpu.make_async_copy(tok_hbm, tok, s_in.at[2]),
    ]
    for load in loads:
        load.start()

    for j in range(1, 16):
        q = lax.rem(x * 4 + yl * 2 + c + j, 16)
        hello((m, z, q // 4, lax.rem(q, 4) // 2, lax.rem(q, 2)))
    for j in range(1, 8):
        hello((m, lax.rem(z + j, 8), x, yl, c))
    hello((1 - m, z, x, 1 - yl, c))
    hello(mate)

    ladder = lax.broadcasted_iota(jnp.int32, (1, 128), 1).astype(F32)
    frequency = jnp.exp(-math.log(10000.0) * 2.0 * ladder / 256)
    for a in range(4):
        for b in range(8):
            r = a * 8 + b
            ang[r : r + 1, :] = when[b * 4 + a].astype(F32) * frequency
    for j in range(2):
        wide[j] = jnp.zeros((640, 256), BF)
        wide[j, pl.ds(pl.multiple_of(x * SLICE, SLICE), SLICE), :] = tw[j]
    angle = ang[...]
    feature = jnp.concatenate([jnp.cos(angle), jnp.sin(angle)], axis=1).astype(BF)
    for j in range(2):
        part = lax.dot_general(
            feature, wide[j], (((1,), (1,)), ((), ())), preferred_element_type=F32
        )
        for a in range(4):
            shl[a, j] = part[a * 8 : (a + 1) * 8, :]
    for load in loads[:2]:
        load.wait()

    pl.semaphore_wait(pltpu.get_barrier_semaphore(), 24)

    def m1(j):
        to = lax.rem(x + j, 4)
        return remote(shl.at[to], buf1.at[x], s_m1.at[j], r_m1.at[j], (m, z, to, yl, c))

    for j in range(1, 4):
        m1(j).start()

    def s1(a, t):
        src, dst = ((wkv, bigk), (wqv, bigq))[a]
        return remote(
            src, dst.at[z, pl.ds(x * SLICE, SLICE), :], s_s1.at[a, t],
            r_s1.at[a, lax.rem(x, 2)], (m, z, c + 2 * t, yl, hh),
        )

    for a in range(2):
        for t in range(2):
            own = (c + 2 * t == x) & (hh == c)

            @pl.when(jnp.logical_not(own))
            def _():
                s1(a, t).start()

            @pl.when(own)
            def _():
                src, dst = ((wkv, bigk), (wqv, bigq))[a]
                dst[z, pl.ds(pl.multiple_of(x * SLICE, SLICE), SLICE), :] = src[...]

    send_lat = remote(lat, latb, s_l, r_l, (m, z, 2 * pair + 1 - px, yl, px))

    @pl.when(home)
    def _():
        latf[...] = jnp.zeros((8, 512), F32)
        latf[0:3, :] = lat[...].astype(F32)

    @pl.when(home)
    def _():
        send_lat.start()

    buf1[x] = shl[x]
    for j in range(1, 4):
        m1(j).wait_recv()
    total = buf1[0] + buf1[1] + buf1[2] + buf1[3]
    for k in range(8):
        for j in range(2):
            tot[k, j : j + 1, :] = total[j, k : k + 1, :]

    def m2(j):
        to = lax.rem(z + j, 8)
        return remote(tot.at[to], buf2.at[z], s_m2.at[j], r_m2.at[j], (m, to, x, yl, c))

    for j in range(1, 8):
        m2(j).start()
    buf2[z] = tot[z]

    def half_of(n):
        return c if n % 2 == 0 else 1 - c

    def ring(a, n):
        origin = lax.rem(z - dz * (n // 2) + 8, 8)
        spot = (bigk, bigq)[a].at[origin, pl.ds(half_of(n) * HALF, HALF), :]
        return remote(spot, spot, s_rg.at[a, n], r_rg.at[a, n], (m, znext, x, yl, c))

    def across(a, n):
        k = n - 1
        big = (bigk, bigq)[a]
        if n == 0:
            spot = big.at[z, pl.ds(c * HALF, HALF), :]
        else:
            origin = lax.rem(z - dz * (k // 2 + 1) + 8, 8)
            spot = big.at[origin, pl.ds(half_of(k) * HALF, HALF), :]
        return remote(spot, spot, s_dd.at[a, n], r_dd.at[a, n], sib)

    def s1_arrived(a):
        for u in range(2):
            own = (2 * c + u == x) & home

            @pl.when(jnp.logical_not(own))
            def _():
                src, dst = ((wkv, bigk), (wqv, bigq))[a]
                remote(
                    src, dst.at[z, pl.ds((2 * c + u) * SLICE, SLICE), :],
                    s_s1.at[a, 0], r_s1.at[a, u], sib,
                ).wait_recv()

    for a in range(2):
        s1_arrived(a)
        ring(a, 0).start()
        across(a, 0).start()

    @pl.when(away)
    def _():
        send_lat.wait_recv()
        latf[...] = jnp.zeros((8, 512), F32)
        latf[0:3, :] = latb[...].astype(F32)

    for j in range(1, 8):
        m2(j).wait_recv()
    for k in range(8):
        mod[:, k * 640 : (k + 1) * 640] = buf2[k]
    loads[2].wait()

    def r1(t, k):
        return remote(
            made.at[pl.ds(k * ROW_CHUNK, ROW_CHUNK), :],
            rows.at[pl.ds((2 * yl + c) * 128 + k * ROW_CHUNK, ROW_CHUNK), :],
            s_r1.at[t, k], r_r1.at[c, k], (m, z, 2 * pair + t, yl, px),
        )

    for k in range(4):

        @pl.loop(0, ROW_CHUNK // 16)
        def _(i):
            at = pl.multiple_of(k * ROW_CHUNK + i * 16, 16)
            hidden = tok[pl.ds(at, 16), :].astype(F32)
            average = jnp.mean(hidden, axis=1, keepdims=True)
            centred = hidden - average
            variance = jnp.mean(centred * centred, axis=1, keepdims=True)
            normed = centred * lax.rsqrt(variance + 1e-06)
            made[pl.ds(at, 16), :] = (normed * (1.0 + mod[1:2, :]) + mod[0:1, :]).astype(BF)

        for t in range(2):
            own = (2 * pair + t == x) & home

            @pl.when(jnp.logical_not(own))
            def _():
                r1(t, k).start()

            @pl.when(own)
            def _():
                at = pl.multiple_of((2 * yl + c) * 128 + k * ROW_CHUNK, ROW_CHUNK)
                rows[pl.ds(at, ROW_CHUNK), :] = made[k * ROW_CHUNK : (k + 1) * ROW_CHUNK, :]

    for a in range(2):
        across(a, 0).wait_recv()
        ring(a, 1).start()

    def share(a, t, y2):
        h2 = 2 * y2 + t
        src, dst = ((val, vals), (cot, cots))[a]
        return remote(
            src.at[:, h2 * 640 : (h2 + 1) * 640],
            dst.at[pl.ds((2 * yl + c) * 128, 128), :],
            s_v.at[a, t, y2], r_v.at[a, 2 * yl + c], (m, z, 2 * pair + t, y2, px),
        )

    def keep(a):
        src, dst = ((val, vals), (cot, cots))[a]
        return pltpu.make_async_copy(
            src.at[:, pl.ds(pl.multiple_of((2 * yl + px) * 640, 128), 640)],
            dst.at[pl.ds((2 * yl + c) * 128, 128), :],
            s_self.at[a],
        )

    for t in range(2):
        for y2 in range(2):
            own = (2 * pair + t == x) & (y2 == yl) & home

            @pl.when(jnp.logical_not(own))
            def _():
                share(1, t, y2).start()
                share(0, t, y2).start()

    @pl.when(home)
    def _():
        keep(0).start()
        keep(1).start()

    copy_q = remote(wqv, qo, s_q, r_q, mate)
    copy_q.start()

    @pl.loop(0, 4)
    def _(i):
        at = pl.multiple_of(i * BLOCK, BLOCK)
        angles = lax.dot_general(
            latf[:, pl.ds(at, BLOCK)], rope_frequency(), (((0,), (0,)), ((), ())),
            precision=lax.Precision.HIGHEST, preferred_element_type=F32,
        )
        column = lax.broadcasted_iota(jnp.int32, (BLOCK, HEAD_SIZE), 1)
        cosb[pl.ds(at, BLOCK), :] = jnp.cos(angles)
        sine = jnp.sin(angles)
        sinb[pl.ds(at, BLOCK), :] = jnp.where(column < HEAD_SIZE // 2, -sine, sine)

    def r2(p, k, ylo):
        spot = rows.at[pl.ds((2 * ylo + p) * 128 + k * ROW_CHUNK, ROW_CHUNK), :]
        return remote(spot, spot, s_r2.at[p, k], r_r2.at[p, k], up if p == 0 else down)

    def ring_step(n):
        for a in range(2):
            ring(a, n).wait_recv()
            if n + 2 < 7:
                ring(a, n + 2).start()
            across(a, n + 1).start()

    for k in range(4):
        for p in range(2):
            own = home & (c == p)

            @pl.when(jnp.logical_not(own))
            def _():
                spot = rows.at[pl.ds((2 * yl + p) * 128 + k * ROW_CHUNK, ROW_CHUNK), :]
                remote(
                    made.at[pl.ds(k * ROW_CHUNK, ROW_CHUNK), :],
                    spot, s_r1.at[0, k], r_r1.at[p, k], sib,
                ).wait_recv()

            r2(p, k, yl).start()
        ring_step(k)

    for k in range(4):
        for p in range(2):
            r2(p, k, 1 - yl).wait_recv()

    def project(a, zo, first):
        acc, big = ((kacc, bigk), (qacc, bigq))[a]
        cols = pl.ds(pl.multiple_of(zo * 640, 128), 640)

        @pl.loop(0, acc.shape[1] // 128)
        def _(i):
            lanes = pl.ds(pl.multiple_of(i * 128, 128), 128)
            term = jnp.dot(rows[:, cols], big[zo, :, lanes], preferred_element_type=F32)
            if first:
                acc[:, lanes] = term
            else:
                acc[:, lanes] = acc[:, lanes] + term

    def at_distance(d):
        return lax.rem(z + d + 8, 8)

    ring_step(4)
    for a in range(2):
        project(a, z, True)
    for n in range(1, 5):
        for a in range(2):
            across(a, n).wait_recv()
    for d in (1, -1, 2, -2):
        for a in range(2):
            project(a, at_distance(d), False)
    ring_step(5)
    for n in (5, 6):
        for a in range(2):
            across(a, n).wait_recv()
    for d in (3, -3):
        for a in range(2):
            project(a, at_distance(d), False)

    def last_step(a):
        ring(a, 6).wait_recv()
        across(a, 7).start()
        across(a, 7).wait_recv()
        project(a, at_distance(4), False)

    def turned(pre, at):
        inverse = lax.rsqrt(jnp.mean(pre * pre, axis=1, keepdims=True) + 1e-06)
        normed = pre * inverse
        rotated = normed * cosb[at, :] + pltpu.roll(normed, HEAD_SIZE // 2, 1) * sinb[at, :]
        return inverse, normed, rotated.astype(BF)

    last_step(0)

    @pl.loop(0, 4)
    def _(i):
        at = pl.ds(pl.multiple_of(i * BLOCK, BLOCK), BLOCK)
        for j in range(3):
            lanes = pl.ds(pl.multiple_of((2 * m + j) * 128, 128), 128)
            krot[at, lanes] = turned(kacc[at, j * 128 : (j + 1) * 128], at)[2]

    def keys(who):
        spot = krot.at[:, pl.ds(pl.multiple_of(who * KW, 128), 256)]
        return remote(spot, spot, s_k, r_k, mate)

    keys(m).start()
    last_step(1)

    for hd in range(4):
        own = home & (hd == 2 * yl + c)

        @pl.when(jnp.logical_not(own))
        def _():
            for a, (src, dst) in enumerate(((val, vals), (cot, cots))):
                remote(
                    src.at[:, 0:640], dst.at[hd * 128 : (hd + 1) * 128, :],
                    s_v.at[a, 0, 0], r_v.at[a, hd], sib,
                ).wait_recv()

    @pl.when(home)
    def _():
        keep(0).wait()
        keep(1).wait()

    scale = HEAD_SIZE ** (-0.5)

    def attend(first, count):
        @pl.loop(0, 4 * count)
        def _(i):
            lanes = pl.ds(pl.multiple_of((first + i // 4) * 128, 128), 128)
            at = pl.ds(pl.multiple_of(lax.rem(i, 4) * BLOCK, BLOCK), BLOCK)
            inverse, normed, query = turned(qacc[at, lanes], at)
            key, value = krot[:, lanes], vals[:, lanes]
            nt = (((1,), (1,)), ((), ()))
            scores = lax.dot_general(query, key, nt, preferred_element_type=F32)
            raised = jnp.exp2(scores * (scale * math.log2(math.e)))
            probs = raised / jnp.sum(raised, axis=1, keepdims=True)
            grad_probs = lax.dot_general(cots[at, lanes], value, nt, preferred_element_type=F32)
            inner = jnp.sum(probs * grad_probs, axis=1, keepdims=True)
            grad_scores = (probs * (grad_probs - inner)).astype(BF)
            turn = jnp.dot(grad_scores, key, preferred_element_type=F32) * scale
            grad = turn * cosb[at, :] + pltpu.roll(turn * sinb[at, :], HEAD_SIZE // 2, 1)
            mean = jnp.mean(grad * normed, axis=1, keepdims=True)
            gq[at, lanes] = (inverse * (grad - normed * mean)).astype(BF)

    attend(2 * m, 3)
    keys(1 - m).wait_recv()
    attend(3 - 3 * m, 2)

    def squares(zs, dst):
        @pl.loop(0, 5)
        def _(r):
            cols = pl.ds(pl.multiple_of(zs * 640 + r * 128, 128), 128)
            g = lax.dot_general(
                rows[:, cols], gq[...], (((0,), (0,)), ((), ())), preferred_element_type=F32
            )
            dst[pl.ds(pl.multiple_of(r * 128, 128), 128), :] = (g * g).astype(BF)

    mine, other = pl.ds(c * HALF, HALF), pl.ds((1 - c) * HALF, HALF)

    def zat(j):
        return lax.rem(z + dz * j + 16, 8)

    def pass_on(q):
        if q == 0:
            src, dst = own_sq.at[3, other, :], got_sq.at[3, other, :]
        elif q < 4:
            src, dst = sib_sq.at[3 - q], got_sq.at[3 - q]
        elif q == 4:
            src, dst = last_sq.at[other, :], last_got
        else:
            u = q - 5
            src, dst = arrived.at[5, u], last_arr.at[u]
        return remote(src, dst, s_sd.at[q], r_sd.at[q], sib)

    def passed(q):
        if q == 0:
            return remote(
                own_sq.at[3, mine, :], got_sq.at[3, mine, :], s_sd.at[q], r_sd.at[q], sib
            )
        return pass_on(q)

    def sums(n, u):
        return remote(out.at[n, u], arrived.at[n, u], s_sr.at[n, u], r_sr.at[n, u], (m, znext, x, yl, c))

    def send_on(n):
        j = (8 - n) // 2 - 1
        base = (c if n % 2 == 0 else 1 - c) * HALF
        for u in range(2):
            if n >= 2:
                sums(n - 2, u).wait_recv()

            @pl.loop(0, SLICE // 32)
            def _(i):
                at = pl.ds(pl.multiple_of(i * 32, 32), 32)
                far = pl.ds(pl.multiple_of(base + u * SLICE + i * 32, 32), 32)
                total = own_sq[j, far, :].astype(F32) + got_sq[j, far, :].astype(F32)
                if n >= 2:
                    total = total + arrived[n - 2, u, at, :].astype(F32)
                out[n, u, at, :] = total.astype(BF)

            sums(n, u).start()

    squares(zat(4), own_sq.at[3])
    pass_on(0).start()
    squares(zat(-3), sib_sq.at[2])
    pass_on(1).start()
    passed(0).wait_recv()
    send_on(0)
    squares(zat(3), own_sq.at[2])
    passed(1).wait_recv()
    send_on(1)
    squares(zat(-2), sib_sq.at[1])
    pass_on(2).start()
    squares(zat(2), own_sq.at[1])
    send_on(2)
    passed(2).wait_recv()
    send_on(3)
    squares(zat(-1), sib_sq.at[0])
    pass_on(3).start()
    squares(zat(1), own_sq.at[0])
    send_on(4)
    passed(3).wait_recv()
    send_on(5)
    squares(z, last_sq)
    pass_on(4).start()
    send_on(6)

    def xs(u):
        return remote(fin.at[u], xb.at[hh], s_x.at[u], r_x.at[hh], (m, z, 2 * c + u, yl, px))

    for u in range(2):
        sums(5, u).wait_recv()
        pass_on(5 + u).start()
    passed(4).wait_recv()
    for u in range(2):
        passed(5 + u).wait_recv()
        sums(6, u).wait_recv()

        @pl.loop(0, SLICE // 32)
        def _(i):
            at = pl.ds(pl.multiple_of(i * 32, 32), 32)
            near = pl.ds(pl.multiple_of(u * SLICE + i * 32, 32), 32)
            far = pl.ds(pl.multiple_of(c * HALF + u * SLICE + i * 32, 32), 32)
            total = last_sq[far, :].astype(F32) + last_got[near, :].astype(F32)
            total = total + arrived[6, u, at, :].astype(F32) + last_arr[u, at, :].astype(F32)
            fin[u, at, :] = total.astype(BF)

        own = (2 * c + u == x) & home

        @pl.when(jnp.logical_not(own))
        def _():
            xs(u).start()

        @pl.when(own)
        def _():
            xb[hh] = fin[u]

    for t in range(2):
        own = (c + 2 * t == x) & (hh == c)

        @pl.when(jnp.logical_not(own))
        def _():
            remote(fin.at[0], xb.at[t], s_x.at[0], r_x.at[t], sib).wait_recv()

    wo[...] = (xb[0].astype(F32) + xb[1].astype(F32) + damping).astype(BF)
    copy_w = remote(wo, wi, s_w, r_w, mate)
    copy_w.start()

    for j in range(1, 4):
        m1(j).wait_send()
    for j in range(1, 8):
        m2(j).wait_send()

    @pl.when(home)
    def _():
        send_lat.wait_send()

    for t in range(2):
        own = (c + 2 * t == x) & (hh == c)

        @pl.when(jnp.logical_not(own))
        def _():
            for a in range(2):
                s1(a, t).wait_send()

        own_r = (2 * pair + t == x) & home

        @pl.when(jnp.logical_not(own_r))
        def _():
            for k in range(4):
                r1(t, k).wait_send()

        for y2 in range(2):
            own_v = (2 * pair + t == x) & (y2 == yl) & home

            @pl.when(jnp.logical_not(own_v))
            def _():
                share(0, t, y2).wait_send()
                share(1, t, y2).wait_send()

    for a in range(2):
        for n in range(7):
            ring(a, n).wait_send()
        for n in range(8):
            across(a, n).wait_send()
    for k in range(4):
        for p in range(2):
            r2(p, k, yl).wait_send()
    keys(m).wait_send()
    for n in range(7):
        for u in range(2):
            sums(n, u).wait_send()
    for q in range(7):
        pass_on(q).wait_send()
    for u in range(2):
        own = (2 * c + u == x) & home

        @pl.when(jnp.logical_not(own))
        def _():
            xs(u).wait_send()

    copy_q.wait()
    copy_w.wait()


def step(timestep, tw, lattice, tokens, own_query, own_key, values, cotangent):
    vmem = pl.BlockSpec(memory_space=pltpu.VMEM)
    hbm = pl.BlockSpec(memory_space=pl.ANY)
    dma = pltpu.SemaphoreType.DMA

    def v(shape, dtype=BF):
        return pltpu.VMEM(shape, dtype)

    return pl.pallas_call(
        kernel,
        out_shape=(
            jax.ShapeDtypeStruct((2, SLICE, 640), BF),
            jax.ShapeDtypeStruct((SLICE, 640), BF),
            jax.ShapeDtypeStruct((SLICE, 640), BF),
            jax.ShapeDtypeStruct((SLICE, 640), BF),
            jax.ShapeDtypeStruct((SLICE, 640), BF),
        ),
        in_specs=[pl.BlockSpec(memory_space=pltpu.SMEM), vmem, vmem] + [hbm] * 5,
        out_specs=(vmem,) * 5,
        scratch_shapes=[
            v((128, 5120)), v((SLICE, KW)), v((8, 640, 640)), v((8, 640, KW)),
            v((512, 5120)), v((512, 640)), v((512, 640)), v((128, 5120)),
            v((32, 128), F32), v((2, 640, 256)), v((4, 2, 8, 640), F32), v((4, 2, 8, 640), F32),
            v((8, 2, 640), F32), v((8, 2, 640), F32), v((2, 5120), F32),
            v((3, 512), jnp.int32), v((8, 512), F32), v((512, 128), F32), v((512, 128), F32),
            v((512, 640), F32), v((512, KW), F32), v((512, 640)), v((512, 640)),
            v((4, 640, 640)), v((3, 640, 640)), v((4, 640, 640)),
            v((7, 2, SLICE, 640)), v((7, 2, SLICE, 640)),
            v((640, 640)), v((HALF, 640)), v((2, SLICE, 640)), v((2, SLICE, 640)),
            dma((3,)), dma((2,)), dma, dma,
            dma((4,)), dma((4,)), dma((8,)), dma((8,)), dma((2, 2)), dma((2, 2)),
            dma((2, 7)), dma((2, 7)), dma((2, 8)), dma((2, 8)),
            dma((2, 4)), dma((2, 4)), dma((2, 4)), dma((2, 4)), dma((2, 2, 2)), dma((2, 4)),
            dma, dma,
            dma((7,)), dma((7,)), dma((7, 2)), dma((7, 2)), dma((2,)), dma((2,)),
            dma, dma, dma, dma,
        ],
        compiler_params=pltpu.CompilerParams(
            collective_id=0, has_side_effects=True, vmem_limit_bytes=60 * 1024 * 1024
        ),
        name="fisher_step",
    )(timestep, tw, lattice, tokens, own_query, own_key, values, cotangent)


def on_device(tokens, lattice, timestep, time_weight, query_weight, key_weight, values, cotangent):
    member = lax.axis_index("member")
    xb, wo, wi, qo, mine = step(
        timestep, time_weight.transpose(0, 2, 1), lattice, tokens,
        query_weight[0], key_weight, values, cotangent[0],
    )
    fisher = xb[0].astype(F32) + xb[1].astype(F32)
    first = member == 0
    w0, w1 = jnp.where(first, wo, wi).astype(F32), jnp.where(first, wi, wo).astype(F32)
    q0, q1 = jnp.where(first, mine, qo).astype(F32), jnp.where(first, qo, mine).astype(F32)
    return (fisher[None], (w0 * q0 + w1 * q1) / (w0 + w1))


def solution(mesh):
    finer = Mesh(mesh.devices.reshape(mesh.shape["member"], 8, 4, 2, 2), AXES)
    in_specs = (
        P(SEQ_HEAD, None),
        P(None, SEQ),
        P(),
        P(None, None, SEQ),
        P("member", SEQ, HEAD),
        P(SEQ, HEAD),
        P(SEQ_HEAD, None),
        P("member", SEQ_HEAD, None),
    )
    out_specs = (P("member", SEQ, HEAD), P(SEQ, HEAD))
    return jax.shard_map(
        on_device, mesh=finer, in_specs=in_specs, out_specs=out_specs, check_vma=False
    )
```

```python
import math

import jax
import jax.numpy as jnp
from jax import lax
from jax.experimental import pallas as pl
from jax.experimental.pallas import tpu as pltpu
from jax.sharding import Mesh
from jax.sharding import PartitionSpec as P

HEAD_SIZE = 128
AXES = ("member", "z", "x", "ylo", "core")
SEQ = ("z", "x")
HEAD = ("ylo", "core")
SEQ_HEAD = ("z", "x", "ylo", "core")
MESH = pl.DeviceIdType.MESH

damping = 0.01
SLICE = 160
HALF = 320
KW = 384
ROW_CHUNK = 32
BLOCK = 128
QUERY = 256
F32, BF = jnp.float32, jnp.bfloat16


def place():
    return tuple(lax.axis_index(a) for a in AXES)


def remote(src, dst, send, recv, to):
    return pltpu.make_async_remote_copy(
        src_ref=src, dst_ref=dst, send_sem=send, recv_sem=recv, device_id=to, device_id_type=MESH
    )


def hello(to):
    pl.semaphore_signal(pltpu.get_barrier_semaphore(), inc=1, device_id=to, device_id_type=MESH)


def rope_frequency():
    halfway, side = HEAD_SIZE // 2, HEAD_SIZE // 6
    frame = halfway - 2 * side
    shape = (8, HEAD_SIZE)
    row = lax.broadcasted_iota(jnp.int32, shape, 0)
    column = lax.broadcasted_iota(jnp.int32, shape, 1)
    pair = jnp.where(column < halfway, column, column - halfway)
    axis = jnp.where(pair < frame, 0, jnp.where(pair < frame + side, 1, 2))
    anchor = jnp.where(axis == 0, 0, jnp.where(axis == 1, frame, frame + side))
    span = jnp.where(axis == 0, frame, side).astype(F32)
    frequency = jnp.exp(-math.log(10000.0) * (pair - anchor).astype(F32) / span)
    return jnp.where(row == axis, frequency, 0.0)


def kernel(
    when, tw, lat, tok_hbm, wq_hbm, wk_hbm, val, cot,
    xb, wo, wi, qo, wqv,
    tok, wkv, bigq, bigk, rows, vals, cots, made,
    ang, wide, shl, buf1, tot, buf2, mod, latb, latf, cosb, sinb,
    qacc, kacc, krot, gq,
    own_a, sib_a, got_a, arr_a, out_a, last_a, lgot_a, larr_a, fin_a,
    own_b, sib_b, got_b, arr_b, out_b, last_b, lgot_b, larr_b, fin_b,
    s_in, s_self, s_l, r_l,
    s_m1, r_m1, s_m2, r_m2, s_s1, r_s1, s_rg, r_rg, s_dd, r_dd,
    s_r1, r_r1, s_r2, r_r2, s_v, r_v, s_k, r_k,
    s_sd, r_sd, s_sr, r_sr, s_x, r_x, s_q, r_q, s_w, r_w,
):
    m, z, x, yl, c = place()
    px, pair, hh = lax.rem(x, 2), x // 2, x // 2
    sib = (m, z, x, yl, 1 - c)
    mate = (1 - m, z, x, yl, c)
    dz = 1 - 2 * c
    znext = lax.rem(z + dz + 8, 8)
    home = c == px
    up = (jnp.where(yl == 0, m, 1 - m), z, x, 1 - yl, c)
    down = (jnp.where(yl == 0, 1 - m, m), z, x, 1 - yl, c)
    away = jnp.logical_not(home)

    loads = [
        pltpu.make_async_copy(wk_hbm.at[:, pl.ds(pl.multiple_of(m * 256, 128), KW)], wkv, s_in.at[0]),
        pltpu.make_async_copy(wq_hbm, wqv, s_in.at[1]),
        pltpu.make_async_copy(tok_hbm, tok, s_in.at[2]),
    ]
    for load in loads:
        load.start()

    for j in range(1, 16):
        q = lax.rem(x * 4 + yl * 2 + c + j, 16)
        hello((m, z, q // 4, lax.rem(q, 4) // 2, lax.rem(q, 2)))
    for j in range(1, 8):
        hello((m, lax.rem(z + j, 8), x, yl, c))
    hello((1 - m, z, x, 1 - yl, c))
    hello(mate)

    ladder = lax.broadcasted_iota(jnp.int32, (1, 128), 1).astype(F32)
    frequency = jnp.exp(-math.log(10000.0) * 2.0 * ladder / 256)
    for a in range(4):
        for b in range(8):
            r = a * 8 + b
            ang[r : r + 1, :] = when[b * 4 + a].astype(F32) * frequency
    for j in range(2):
        wide[j] = jnp.zeros((640, 256), BF)
        wide[j, pl.ds(pl.multiple_of(x * SLICE, SLICE), SLICE), :] = tw[j]
    angle = ang[...]
    feature = jnp.concatenate([jnp.cos(angle), jnp.sin(angle)], axis=1).astype(BF)
    for j in range(2):
        part = lax.dot_general(
            feature, wide[j], (((1,), (1,)), ((), ())), preferred_element_type=F32
        )
        for a in range(4):
            shl[a, j] = part[a * 8 : (a + 1) * 8, :]
    for load in loads[:2]:
        load.wait()

    pl.semaphore_wait(pltpu.get_barrier_semaphore(), 24)

    def m1(j):
        to = lax.rem(x + j, 4)
        return remote(shl.at[to], buf1.at[x], s_m1.at[j], r_m1.at[j], (m, z, to, yl, c))

    for j in range(1, 4):
        m1(j).start()

    def s1(a, t):
        src, dst = ((wkv, bigk), (wqv, bigq))[a]
        return remote(
            src, dst.at[z, pl.ds(x * SLICE, SLICE), :], s_s1.at[a, t],
            r_s1.at[a, lax.rem(x, 2)], (m, z, c + 2 * t, yl, hh),
        )

    def s1_sends(two_hops):
        for a in range(2):
            for t in range(2):
                own = (c + 2 * t == x) & (hh == c)
                far = home & (c + 2 * t != x)

                @pl.when(far if two_hops else jnp.logical_not(own | far))
                def _():
                    s1(a, t).start()

    s1_sends(False)

    @pl.when(home & (hh == c))
    def _():
        for a in range(2):
            src, dst = ((wkv, bigk), (wqv, bigq))[a]
            dst[z, pl.ds(pl.multiple_of(x * SLICE, SLICE), SLICE), :] = src[...]

    send_lat = remote(lat, latb, s_l, r_l, (m, z, 2 * pair + 1 - px, yl, px))

    @pl.when(home)
    def _():
        latf[...] = jnp.zeros((8, 512), F32)
        latf[0:3, :] = lat[...].astype(F32)

    @pl.when(home)
    def _():
        send_lat.start()

    buf1[x] = shl[x]
    for j in range(1, 4):
        m1(j).wait_recv()
    s1_sends(True)
    total = buf1[0] + buf1[1] + buf1[2] + buf1[3]
    for k in range(8):
        for j in range(2):
            tot[k, j : j + 1, :] = total[j, k : k + 1, :]

    def m2(j):
        to = lax.rem(z + j, 8)
        return remote(tot.at[to], buf2.at[z], s_m2.at[j], r_m2.at[j], (m, to, x, yl, c))

    for j in range(1, 8):
        m2(j).start()
    buf2[z] = tot[z]

    def half_of(n):
        return c if n % 2 == 0 else 1 - c

    def piece(half, e):
        near = jnp.where(hh == half, px, 1 - px)
        return pl.ds((2 * half + (near if e == 0 else 1 - near)) * SLICE, SLICE)

    def ring(a, n, e):
        origin = lax.rem(z - dz * (n // 2) + 8, 8)
        spot = (bigk, bigq)[a].at[origin, piece(half_of(n), e), :]
        return remote(spot, spot, s_rg.at[a, n, e], r_rg.at[a, n, e], (m, znext, x, yl, c))

    def across(a, n, e):
        k = n - 1
        big = (bigk, bigq)[a]
        if n == 0:
            spot = big.at[z, piece(c, e), :]
        else:
            origin = lax.rem(z - dz * (k // 2 + 1) + 8, 8)
            spot = big.at[origin, piece(half_of(k), e), :]
        return remote(spot, spot, s_dd.at[a, n, e], r_dd.at[a, n, e], sib)

    def s1_arrived(a, e):
        near = jnp.where(hh == c, px, 1 - px)
        u = near if e == 0 else 1 - near
        own = (2 * c + u == x) & home

        @pl.when(jnp.logical_not(own))
        def _():
            src, dst = ((wkv, bigk), (wqv, bigq))[a]
            remote(
                src, dst.at[z, pl.ds((2 * c + u) * SLICE, SLICE), :],
                s_s1.at[a, 0], r_s1.at[a, u], sib,
            ).wait_recv()

    def set_off(e):
        for a in range(2):
            s1_arrived(a, e)
            ring(a, 0, e).start()
            across(a, 0, e).start()

    set_off(0)

    for j in range(1, 8):
        m2(j).wait_recv()
    for k in range(8):
        mod[:, k * 640 : (k + 1) * 640] = buf2[k]
    loads[2].wait()

    def r1(t, k):
        return remote(
            made.at[pl.ds(k * ROW_CHUNK, ROW_CHUNK), :],
            rows.at[pl.ds((2 * yl + c) * 128 + k * ROW_CHUNK, ROW_CHUNK), :],
            s_r1.at[t, k], r_r1.at[c, k], (m, z, 2 * pair + t, yl, px),
        )

    for k in range(4):

        @pl.loop(0, ROW_CHUNK // 16)
        def _(i):
            at = pl.multiple_of(k * ROW_CHUNK + i * 16, 16)
            hidden = tok[pl.ds(at, 16), :].astype(F32)
            average = jnp.mean(hidden, axis=1, keepdims=True)
            centred = hidden - average
            variance = jnp.mean(centred * centred, axis=1, keepdims=True)
            normed = centred * lax.rsqrt(variance + 1e-06)
            made[pl.ds(at, 16), :] = (normed * (1.0 + mod[1:2, :]) + mod[0:1, :]).astype(BF)

        for t in range(2):
            own = (2 * pair + t == x) & home

            @pl.when(jnp.logical_not(own))
            def _():
                r1(t, k).start()

            @pl.when(own)
            def _():
                at = pl.multiple_of((2 * yl + c) * 128 + k * ROW_CHUNK, ROW_CHUNK)
                rows[pl.ds(at, ROW_CHUNK), :] = made[k * ROW_CHUNK : (k + 1) * ROW_CHUNK, :]

        if k == 0:
            set_off(1)

    for e in range(2):
        for a in range(2):
            across(a, 0, e).wait_recv()
            ring(a, 1, e).start()

    def share(a, t, y2):
        h2 = 2 * y2 + t
        src, dst = ((val, vals), (cot, cots))[a]
        return remote(
            src.at[:, h2 * 640 : (h2 + 1) * 640],
            dst.at[pl.ds((2 * yl + c) * 128, 128), :],
            s_v.at[a, t, y2], r_v.at[a, 2 * yl + c], (m, z, 2 * pair + t, y2, px),
        )

    def keep(a):
        src, dst = ((val, vals), (cot, cots))[a]
        return pltpu.make_async_copy(
            src.at[:, pl.ds(pl.multiple_of((2 * yl + px) * 640, 128), 640)],
            dst.at[pl.ds((2 * yl + c) * 128, 128), :],
            s_self.at[a],
        )

    @pl.when(away)
    def _():
        send_lat.wait_recv()
        latf[...] = jnp.zeros((8, 512), F32)
        latf[0:3, :] = latb[...].astype(F32)

    @pl.loop(0, 4)
    def _(i):
        at = pl.multiple_of(i * BLOCK, BLOCK)
        angles = lax.dot_general(
            latf[:, pl.ds(at, BLOCK)], rope_frequency(), (((0,), (0,)), ((), ())),
            precision=lax.Precision.HIGHEST, preferred_element_type=F32,
        )
        column = lax.broadcasted_iota(jnp.int32, (BLOCK, HEAD_SIZE), 1)
        cosb[pl.ds(at, BLOCK), :] = jnp.cos(angles)
        sine = jnp.sin(angles)
        sinb[pl.ds(at, BLOCK), :] = jnp.where(column < HEAD_SIZE // 2, -sine, sine)

    def r2(p, k, ylo):
        spot = rows.at[pl.ds((2 * ylo + p) * 128 + k * ROW_CHUNK, ROW_CHUNK), :]
        return remote(spot, spot, s_r2.at[p, k], r_r2.at[p, k], up if p == 0 else down)

    def ring_step(n):
        for e in range(2):
            for a in range(2):
                ring(a, n, e).wait_recv()
                if n + 2 < 7 and n != 4:
                    ring(a, n + 2, e).start()
                across(a, n + 1, e).start()
        if n == 4:
            for a in range(2):
                for e in range(2):
                    ring(a, 6, e).start()

    def relay(k):
        for p in range(2):
            own = home & (c == p)

            @pl.when(jnp.logical_not(own))
            def _():
                spot = rows.at[pl.ds((2 * yl + p) * 128 + k * ROW_CHUNK, ROW_CHUNK), :]
                remote(
                    made.at[pl.ds(k * ROW_CHUNK, ROW_CHUNK), :],
                    spot, s_r1.at[0, k], r_r1.at[p, k], sib,
                ).wait_recv()

            r2(p, k, yl).start()

    @pl.when(home)
    def _():
        for k in range(4):
            relay(k)

    for k in range(4):
        ring_step(k)

        @pl.when(away)
        def _():
            relay(k)

    ring_step(4)
    for k in range(4):
        for p in range(2):
            r2(p, k, 1 - yl).wait_recv()

    for t in range(2):
        for y2 in range(2):
            own = (2 * pair + t == x) & (y2 == yl) & home

            @pl.when(jnp.logical_not(own))
            def _():
                share(1, t, y2).start()
                share(0, t, y2).start()

    @pl.when(home)
    def _():
        keep(0).start()
        keep(1).start()

    def project(a, zo, first):
        acc, big = ((kacc, bigk), (qacc, bigq))[a]
        cols = pl.ds(pl.multiple_of(zo * 640, 128), 640)

        term = jnp.dot(rows[:, cols], big[zo], preferred_element_type=F32)
        acc[...] = term if first else acc[...] + term

    def at_distance(d):
        return lax.rem(z + d + 8, 8)

    for a in range(2):
        project(a, z, True)
    for n in range(1, 5):
        for a in range(2):
            for e in range(2):
                across(a, n, e).wait_recv()

    @pl.loop(0, 4)
    def _(i):
        d = jnp.where(i == 0, 1, jnp.where(i == 1, -1, jnp.where(i == 2, 2, -2)))
        for a in range(2):
            project(a, at_distance(d), False)

    ring_step(5)
    for n in (5, 6):
        for a in range(2):
            for e in range(2):
                across(a, n, e).wait_recv()

    @pl.loop(0, 2)
    def _(i):
        for a in range(2):
            project(a, at_distance(3 - 6 * i), False)


    def last_in(a, e):
        ring(a, 6, e).wait_recv()
        across(a, 7, e).start()

    def last_step(a):
        for e in range(2):
            across(a, 7, e).wait_recv()
        project(a, at_distance(4), False)

    last_in(0, 0)
    last_in(0, 1)

    def turned(pre, at):
        inverse = lax.rsqrt(jnp.mean(pre * pre, axis=1, keepdims=True) + 1e-06)
        normed = pre * inverse
        rotated = normed * cosb[at, :] + pltpu.roll(normed, HEAD_SIZE // 2, 1) * sinb[at, :]
        return inverse, normed, rotated.astype(BF)

    last_step(0)

    @pl.loop(0, 4)
    def _(i):
        at = pl.ds(pl.multiple_of(i * BLOCK, BLOCK), BLOCK)
        for j in range(3):
            lanes = pl.ds(pl.multiple_of((2 * m + j) * 128, 128), 128)
            krot[at, lanes] = turned(kacc[at, j * 128 : (j + 1) * 128], at)[2]

    def keys(who):
        spot = krot.at[:, pl.ds(pl.multiple_of(who * KW, 128), 256)]
        return remote(spot, spot, s_k, r_k, mate)

    keys(m).start()
    last_in(1, 0)
    last_in(1, 1)
    last_step(1)

    for hd in range(4):
        own = home & (hd == 2 * yl + c)

        @pl.when(jnp.logical_not(own))
        def _():
            for a, (src, dst) in enumerate(((val, vals), (cot, cots))):
                remote(
                    src.at[:, 0:640], dst.at[hd * 128 : (hd + 1) * 128, :],
                    s_v.at[a, 0, 0], r_v.at[a, hd], sib,
                ).wait_recv()

    @pl.when(home)
    def _():
        keep(0).wait()
        keep(1).wait()

    scale = HEAD_SIZE ** (-0.5)

    def attend(first, count):
        @pl.loop(0, 2 * count)
        def _(i):
            lanes = pl.ds(pl.multiple_of((first + i // 2) * 128, 128), 128)
            at = pl.ds(pl.multiple_of(lax.rem(i, 2) * QUERY, QUERY), QUERY)
            inverse, normed, query = turned(qacc[at, lanes], at)
            key, value = krot[:, lanes], vals[:, lanes]
            nt = (((1,), (1,)), ((), ()))
            scores = lax.dot_general(query, key, nt, preferred_element_type=F32)
            raised = jnp.exp2(scores * (scale * math.log2(math.e)))
            grad_probs = lax.dot_general(cots[at, lanes], value, nt, preferred_element_type=F32)
            share_of = 1.0 / jnp.sum(raised, axis=1, keepdims=True)
            probs = raised * share_of
            inner = jnp.sum(probs * grad_probs, axis=1, keepdims=True)
            grad_scores = (probs * (grad_probs - inner)).astype(BF)
            turn = jnp.dot(grad_scores, key, preferred_element_type=F32) * scale
            grad = turn * cosb[at, :] + pltpu.roll(turn * sinb[at, :], HEAD_SIZE // 2, 1)
            mean = jnp.mean(grad * normed, axis=1, keepdims=True)
            gq[at, lanes] = (inverse * (grad - normed * mean)).astype(BF)

    copy_q = remote(wqv, qo, s_q, r_q, mate)
    copy_q.start()

    mine, other = pl.ds(c * HALF, HALF), pl.ds((1 - c) * HALF, HALF)

    def zat(j):
        return lax.rem(z + dz * j + 16, 8)

    class Reduce:
        def __init__(self, g, lane, bufs):
            self.g, self.width = g, bufs[0].shape[2]
            self.lanes = pl.ds(pl.multiple_of(lane, 128), self.width)
            (self.own, self.sib, self.got, self.arrived, self.out, self.last, self.last_got,
             self.last_arr, self.fin) = bufs

        def squares(self, zs, dst):
            cols = pl.ds(pl.multiple_of(zs * 640, 128), 640)
            g = lax.dot_general(
                rows[:, cols], gq[:, self.lanes], (((0,), (0,)), ((), ())),
                preferred_element_type=F32,
            )
            dst[...] = (g * g).astype(BF)

        def pass_on(self, q):
            if q == 0:
                src, dst = self.own.at[3, other, :], self.got.at[3, other, :]
            elif q < 4:
                src, dst = self.sib.at[3 - q], self.got.at[3 - q]
            elif q == 4:
                src, dst = self.last.at[other, :], self.last_got
            else:
                src, dst = self.arrived.at[5, q - 5], self.last_arr.at[q - 5]
            return remote(src, dst, s_sd.at[self.g, q], r_sd.at[self.g, q], sib)

        def passed(self, q):
            if q == 0:
                return remote(
                    self.own.at[3, mine, :], self.got.at[3, mine, :],
                    s_sd.at[self.g, q], r_sd.at[self.g, q], sib,
                )
            return self.pass_on(q)

        def sums(self, n, u):
            return remote(
                self.out.at[n, u], self.arrived.at[n, u], s_sr.at[self.g, n, u],
                r_sr.at[self.g, n, u], (m, znext, x, yl, c),
            )

        def send_on(self, n):
            j = (8 - n) // 2 - 1
            base = (c if n % 2 == 0 else 1 - c) * HALF
            for u in range(2):
                if n >= 2:
                    self.sums(n - 2, u).wait_recv()

                @pl.loop(0, SLICE // 32)
                def _(i):
                    at = pl.ds(pl.multiple_of(i * 32, 32), 32)
                    far = pl.ds(pl.multiple_of(base + u * SLICE + i * 32, 32), 32)
                    total = self.own[j, far, :].astype(F32) + self.got[j, far, :].astype(F32)
                    if n >= 2:
                        total = total + self.arrived[n - 2, u, at, :].astype(F32)
                    self.out[n, u, at, :] = total.astype(BF)

                self.sums(n, u).start()

        def start(self):
            self.squares(zat(4), self.own.at[3])
            self.pass_on(0).start()
            self.squares(zat(-3), self.sib.at[2])
            self.pass_on(1).start()
            self.passed(0).wait_recv()
            self.send_on(0)
            self.squares(zat(3), self.own.at[2])
            self.passed(1).wait_recv()
            self.send_on(1)

        def middle(self, k):
            self.squares(zat(k - 4), self.sib.at[3 - k])
            self.pass_on(k).start()
            self.squares(zat(4 - k), self.own.at[3 - k])
            self.send_on(2 * k - 2)
            self.passed(k).wait_recv()
            self.send_on(2 * k - 1)

        def own_slice(self):
            self.squares(z, self.last)
            self.pass_on(4).start()

        def xs(self, u):
            return remote(
                self.fin.at[u], xb.at[hh, :, self.lanes], s_x.at[self.g, u], r_x.at[self.g, hh],
                (m, z, 2 * c + u, yl, px),
            )

        def finish(self):
            for u in range(2):
                self.sums(5, u).wait_recv()
                self.pass_on(5 + u).start()
            self.passed(4).wait_recv()
            for u in range(2):
                self.passed(5 + u).wait_recv()
                self.sums(6, u).wait_recv()

                @pl.loop(0, SLICE // 32)
                def _(i):
                    at = pl.ds(pl.multiple_of(i * 32, 32), 32)
                    near = pl.ds(pl.multiple_of(u * SLICE + i * 32, 32), 32)
                    far = pl.ds(pl.multiple_of(c * HALF + u * SLICE + i * 32, 32), 32)
                    total = self.last[far, :].astype(F32) + self.last_got[near, :].astype(F32)
                    total = total + self.arrived[6, u, at, :].astype(F32)
                    total = total + self.last_arr[u, at, :].astype(F32)
                    self.fin[u, at, :] = total.astype(BF)

                own = (2 * c + u == x) & home

                @pl.when(jnp.logical_not(own))
                def _():
                    self.xs(u).start()

                @pl.when(own)
                def _():
                    xb[hh, :, self.lanes] = self.fin[u]

        def weigh(self):
            for t in range(2):
                own = (c + 2 * t == x) & (hh == c)

                @pl.when(jnp.logical_not(own))
                def _():
                    remote(
                        self.fin.at[0], xb.at[t, :, self.lanes], s_x.at[self.g, 0],
                        r_x.at[self.g, t], sib,
                    ).wait_recv()

            fisher = xb[0, :, self.lanes].astype(F32) + xb[1, :, self.lanes].astype(F32)
            wo[:, self.lanes] = (fisher + damping).astype(BF)
            self.mate_copy().start()

        def mate_copy(self):
            return remote(
                wo.at[:, self.lanes], wi.at[:, self.lanes], s_w.at[self.g], r_w.at[self.g], mate
            )

        def drain(self):
            for n in range(7):
                for u in range(2):
                    self.sums(n, u).wait_send()
            for q in range(7):
                self.pass_on(q).wait_send()
            for u in range(2):
                own = (2 * c + u == x) & home

                @pl.when(jnp.logical_not(own))
                def _():
                    self.xs(u).wait_send()

            self.mate_copy().wait()

    part_a = Reduce(0, m * 256, (own_a, sib_a, got_a, arr_a, out_a, last_a, lgot_a, larr_a, fin_a))
    part_b = Reduce(
        1, (1 - m) * KW, (own_b, sib_b, got_b, arr_b, out_b, last_b, lgot_b, larr_b, fin_b)
    )

    attend(2 * m, 3)
    part_a.start()
    keys(1 - m).wait_recv()
    attend(3 - 3 * m, 2)
    part_a.middle(2)
    part_b.start()
    part_a.middle(3)
    part_b.middle(2)
    part_a.own_slice()
    part_a.send_on(6)
    part_b.middle(3)
    part_b.own_slice()
    part_a.finish()
    part_b.send_on(6)
    part_b.finish()
    part_a.weigh()
    part_b.weigh()

    for j in range(1, 4):
        m1(j).wait_send()
    for j in range(1, 8):
        m2(j).wait_send()

    @pl.when(home)
    def _():
        send_lat.wait_send()

    for t in range(2):
        own = (c + 2 * t == x) & (hh == c)

        @pl.when(jnp.logical_not(own))
        def _():
            for a in range(2):
                s1(a, t).wait_send()

        own_r = (2 * pair + t == x) & home

        @pl.when(jnp.logical_not(own_r))
        def _():
            for k in range(4):
                r1(t, k).wait_send()

        for y2 in range(2):
            own_v = (2 * pair + t == x) & (y2 == yl) & home

            @pl.when(jnp.logical_not(own_v))
            def _():
                share(0, t, y2).wait_send()
                share(1, t, y2).wait_send()

    for a in range(2):
        for e in range(2):
            for n in range(7):
                ring(a, n, e).wait_send()
            for n in range(8):
                across(a, n, e).wait_send()
    for k in range(4):
        for p in range(2):
            r2(p, k, yl).wait_send()
    keys(m).wait_send()
    copy_q.wait()
    part_a.drain()
    part_b.drain()


def step(timestep, tw, lattice, tokens, own_query, own_key, values, cotangent):
    vmem = pl.BlockSpec(memory_space=pltpu.VMEM)
    hbm = pl.BlockSpec(memory_space=pltpu.HBM)
    dma = pltpu.SemaphoreType.DMA

    def v(shape, dtype=BF):
        return pltpu.VMEM(shape, dtype)

    def sums_of(width):
        return (
            v((4, 640, width)), v((3, 640, width)), v((4, 640, width)),
            v((7, 2, SLICE, width)), v((7, 2, SLICE, width)),
            v((640, width)), v((HALF, width)), v((2, SLICE, width)), v((2, SLICE, width)),
        )

    return pl.pallas_call(
        kernel,
        out_shape=(
            jax.ShapeDtypeStruct((2, SLICE, 640), BF),
            jax.ShapeDtypeStruct((SLICE, 640), BF),
            jax.ShapeDtypeStruct((SLICE, 640), BF),
            jax.ShapeDtypeStruct((SLICE, 640), BF),
            jax.ShapeDtypeStruct((SLICE, 640), BF),
        ),
        in_specs=[pl.BlockSpec(memory_space=pltpu.SMEM), vmem, vmem] + [hbm] * 5,
        out_specs=(vmem,) * 5,
        scratch_shapes=[
            v((128, 5120)), v((SLICE, KW)), v((8, 640, 640)), v((8, 640, KW)),
            v((512, 5120)), v((512, 640)), v((512, 640)), v((128, 5120)),
            v((32, 128), F32), v((2, 640, 256)), v((4, 2, 8, 640), F32), v((4, 2, 8, 640), F32),
            v((8, 2, 640), F32), v((8, 2, 640), F32), v((2, 5120), F32),
            v((3, 512), jnp.int32), v((8, 512), F32), v((512, 128), F32), v((512, 128), F32),
            v((512, 640), F32), v((512, KW), F32), v((512, 640)), v((512, 640)),
            *sums_of(KW), *sums_of(256),
            dma((3,)), dma((2,)), dma, dma,
            dma((4,)), dma((4,)), dma((8,)), dma((8,)), dma((2, 2)), dma((2, 2)),
            dma((2, 7, 2)), dma((2, 7, 2)), dma((2, 8, 2)), dma((2, 8, 2)),
            dma((2, 4)), dma((2, 4)), dma((2, 4)), dma((2, 4)), dma((2, 2, 2)), dma((2, 4)),
            dma, dma,
            dma((2, 7)), dma((2, 7)), dma((2, 7, 2)), dma((2, 7, 2)), dma((2, 2)), dma((2, 2)),
            dma, dma, dma((2,)), dma((2,)),
        ],
        compiler_params=pltpu.CompilerParams(
            collective_id=0, has_side_effects=True, vmem_limit_bytes=58 * 1024 * 1024
        ),
        name="fisher_step",
    )(timestep, tw, lattice, tokens, own_query, own_key, values, cotangent)


def on_device(tokens, lattice, timestep, time_weight, query_weight, key_weight, values, cotangent):
    member = lax.axis_index("member")
    xb, wo, wi, qo, mine = step(
        timestep, time_weight.transpose(0, 2, 1), lattice, tokens,
        query_weight[0], key_weight, values, cotangent[0],
    )
    fisher = xb[0].astype(F32) + xb[1].astype(F32)
    first = member == 0
    w0, w1 = jnp.where(first, wo, wi).astype(F32), jnp.where(first, wi, wo).astype(F32)
    q0, q1 = jnp.where(first, mine, qo).astype(F32), jnp.where(first, qo, mine).astype(F32)
    return (fisher[None], (w0 * q0 + w1 * q1) / (w0 + w1))


def solution(mesh):
    finer = Mesh(mesh.devices.reshape(mesh.shape["member"], 8, 4, 2, 2), AXES)
    in_specs = (
        P(SEQ_HEAD, None),
        P(None, SEQ),
        P(),
        P(None, None, SEQ),
        P("member", SEQ, HEAD),
        P(SEQ, HEAD),
        P(SEQ_HEAD, None),
        P("member", SEQ_HEAD, None),
    )
    out_specs = (P("member", SEQ, HEAD), P(SEQ, HEAD))
    return jax.shard_map(
        on_device, mesh=finer, in_specs=in_specs, out_specs=out_specs, check_vma=False
    )
```

```python
import math

import jax
import jax.numpy as jnp
from jax import lax
from jax.experimental import pallas as pl
from jax.experimental.pallas import tpu as pltpu
from jax.sharding import Mesh
from jax.sharding import PartitionSpec as P

HEAD_SIZE = 128
AXES = ("member", "z", "x", "ylo", "core")
SEQ = ("z", "x")
HEAD = ("ylo", "core")
SEQ_HEAD = ("z", "x", "ylo", "core")
MESH = pl.DeviceIdType.MESH

damping = 0.01
SLICE = 160
HALF = 320
KW = 384
ROW_CHUNK = 32
BLOCK = 128
QUERY = 256
F32, BF = jnp.float32, jnp.bfloat16


def place():
    return tuple(lax.axis_index(a) for a in AXES)


def remote(src, dst, send, recv, to):
    return pltpu.make_async_remote_copy(
        src_ref=src, dst_ref=dst, send_sem=send, recv_sem=recv, device_id=to, device_id_type=MESH
    )


def hello(to):
    pl.semaphore_signal(pltpu.get_barrier_semaphore(), inc=1, device_id=to, device_id_type=MESH)


def rope_frequency():
    halfway, side = HEAD_SIZE // 2, HEAD_SIZE // 6
    frame = halfway - 2 * side
    shape = (8, HEAD_SIZE)
    row = lax.broadcasted_iota(jnp.int32, shape, 0)
    column = lax.broadcasted_iota(jnp.int32, shape, 1)
    pair = jnp.where(column < halfway, column, column - halfway)
    axis = jnp.where(pair < frame, 0, jnp.where(pair < frame + side, 1, 2))
    anchor = jnp.where(axis == 0, 0, jnp.where(axis == 1, frame, frame + side))
    span = jnp.where(axis == 0, frame, side).astype(F32)
    frequency = jnp.exp(-math.log(10000.0) * (pair - anchor).astype(F32) / span)
    return jnp.where(row == axis, frequency, 0.0)


def kernel(
    when, tw_hbm, lat_hbm, tok_hbm, wq_hbm, wk_hbm, val, cot,
    xb, wo, wi, qo, wqv,
    tok, wkv, bigq, bigk, rows, vals, cots, made,
    tw, lat, ang, wide, shl, buf1, tot, buf2, mod, latb, latf, cosb, sinb,
    qacc, kacc, krot, gq,
    own_a, sib_a, got_a, arr_a, out_a, last_a, lgot_a, larr_a, fin_a,
    own_b, sib_b, got_b, arr_b, out_b, last_b, lgot_b, larr_b, fin_b,
    s_in, s_self, s_l, r_l,
    s_m1, r_m1, s_m2, r_m2, s_s1, r_s1, s_rg, r_rg, s_dd, r_dd,
    s_r1, r_r1, s_r2, r_r2, s_v, r_v, s_k, r_k,
    s_sd, r_sd, s_sr, r_sr, s_x, r_x, s_q, r_q, s_w, r_w,
):
    m, z, x, yl, c = place()
    px, pair, hh = lax.rem(x, 2), x // 2, x // 2
    sib = (m, z, x, yl, 1 - c)
    mate = (1 - m, z, x, yl, c)
    dz = 1 - 2 * c
    znext = lax.rem(z + dz + 8, 8)
    home = c == px
    up = (jnp.where(yl == 0, m, 1 - m), z, x, 1 - yl, c)
    down = (jnp.where(yl == 0, 1 - m, m), z, x, 1 - yl, c)
    away = jnp.logical_not(home)

    loads = [
        pltpu.make_async_copy(wk_hbm.at[:, pl.ds(pl.multiple_of(m * 256, 128), KW)], wkv, s_in.at[0]),
        pltpu.make_async_copy(wq_hbm, wqv, s_in.at[1]),
        pltpu.make_async_copy(tok_hbm, tok, s_in.at[2]),
        pltpu.make_async_copy(tw_hbm, tw, s_in.at[5]),
        pltpu.make_async_copy(lat_hbm, lat, s_in.at[6]),
    ]
    for load in loads:
        load.start()
    key_columns = pl.ds(pl.multiple_of(m * 256, 128), KW)
    own_weights = [
        pltpu.make_async_copy(
            wk_hbm.at[:, key_columns], bigk.at[z, pl.ds(x * SLICE, SLICE), :], s_in.at[3]
        ),
        pltpu.make_async_copy(wq_hbm, bigq.at[z, pl.ds(x * SLICE, SLICE), :], s_in.at[4]),
    ]

    @pl.when(home)
    def _():
        for load in own_weights:
            load.start()

    for j in range(1, 16):
        q = lax.rem(x * 4 + yl * 2 + c + j, 16)
        hello((m, z, q // 4, lax.rem(q, 4) // 2, lax.rem(q, 2)))
    for j in range(1, 8):
        hello((m, lax.rem(z + j, 8), x, yl, c))
    hello((1 - m, z, x, 1 - yl, c))
    hello(mate)

    ladder = lax.broadcasted_iota(jnp.int32, (1, 128), 1).astype(F32)
    frequency = jnp.exp(-math.log(10000.0) * 2.0 * ladder / 256)
    for a in range(4):
        for b in range(8):
            r = a * 8 + b
            ang[r : r + 1, :] = when[b * 4 + a].astype(F32) * frequency
    loads[3].wait()
    loads[4].wait()
    for j in range(2):
        wide[j] = jnp.zeros((640, 256), BF)
        wide[j, pl.ds(pl.multiple_of(x * SLICE, SLICE), SLICE), :] = tw[j]
    angle = ang[...]
    feature = jnp.concatenate([jnp.cos(angle), jnp.sin(angle)], axis=1).astype(BF)
    for j in range(2):
        part = lax.dot_general(
            feature, wide[j], (((1,), (1,)), ((), ())), preferred_element_type=F32
        )
        for a in range(4):
            shl[a, j] = part[a * 8 : (a + 1) * 8, :]
    for load in loads[:2]:
        load.wait()

    pl.semaphore_wait(pltpu.get_barrier_semaphore(), 24)

    def m1(j):
        to = lax.rem(x + j, 4)
        return remote(shl.at[to], buf1.at[x], s_m1.at[j], r_m1.at[j], (m, z, to, yl, c))

    for j in range(1, 4):
        m1(j).start()

    def s1(a, t):
        src, dst = ((wkv, bigk), (wqv, bigq))[a]
        return remote(
            src, dst.at[z, pl.ds(x * SLICE, SLICE), :], s_s1.at[a, t],
            r_s1.at[a, lax.rem(x, 2)], (m, z, c + 2 * t, yl, hh),
        )

    def s1_sends(two_hops):
        for a in range(2):
            for t in range(2):
                own = (c + 2 * t == x) & (hh == c)
                far = home & (c + 2 * t != x)

                @pl.when(far if two_hops else jnp.logical_not(own | far))
                def _():
                    s1(a, t).start()

    s1_sends(False)

    @pl.when(home)
    def _():
        for load in own_weights:
            load.wait()

    def half_of(n):
        return c if n == 6 else (hh if n % 2 == 0 else 1 - hh)

    def piece(half, e):
        near = jnp.where(hh == half, px, 1 - px)
        return pl.ds((2 * half + (near if e == 0 else 1 - near)) * SLICE, SLICE)

    def ring(a, n, e):
        origin = lax.rem(z - dz * (n // 2) + 8, 8)
        spot = (bigk, bigq)[a].at[origin, piece(half_of(n), e), :]
        return remote(spot, spot, s_rg.at[a, n, e], r_rg.at[a, n, e], (m, znext, x, yl, c))

    def across(a, n, e):
        k = n - 1
        big = (bigk, bigq)[a]
        if n == 0:
            spot = big.at[z, piece(c, e), :]
        else:
            origin = lax.rem(z - dz * (k // 2 + 1) + 8, 8)
            spot = big.at[origin, piece(half_of(k), e), :]
        return remote(spot, spot, s_dd.at[a, n, e], r_dd.at[a, n, e], sib)

    def s1_arrived(a, e):
        near = jnp.where(hh == c, px, 1 - px)
        u = near if e == 0 else 1 - near
        own = (2 * c + u == x) & home

        @pl.when(jnp.logical_not(own))
        def _():
            src, dst = ((wkv, bigk), (wqv, bigq))[a]
            remote(
                src, dst.at[z, pl.ds((2 * c + u) * SLICE, SLICE), :],
                s_s1.at[a, 0], r_s1.at[a, u], sib,
            ).wait_recv()

    collector = hh == c

    def set_off(n, e):
        gathers = collector if n == 0 else jnp.logical_not(collector)

        @pl.when(gathers)
        def _():
            for a in range(2):
                s1_arrived(a, e)
                ring(a, n, e).start()
                if (n, e) == (0, 0):

                    @pl.when(home)
                    def _():
                        across(a, 0, e).start()
                else:
                    across(a, 0, e).start()

        @pl.when(jnp.logical_not(gathers))
        def _():
            for a in range(2):
                if (n, e) == (0, 0):

                    @pl.when(away)
                    def _():
                        across(a, 0, e).wait_recv()
                else:
                    across(a, 0, e).wait_recv()
                ring(a, n, e).start()

    def share(a, t, y2):
        h2 = 2 * y2 + t
        src, dst = ((val, vals), (cot, cots))[a]
        return remote(
            src.at[:, h2 * 640 : (h2 + 1) * 640],
            dst.at[pl.ds((2 * yl + c) * 128, 128), :],
            s_v.at[a, t, y2], r_v.at[a, 2 * yl + c], (m, z, 2 * pair + t, y2, px),
        )

    def keep(a):
        src, dst = ((val, vals), (cot, cots))[a]
        return pltpu.make_async_copy(
            src.at[:, pl.ds(pl.multiple_of((2 * yl + px) * 640, 128), 640)],
            dst.at[pl.ds((2 * yl + c) * 128, 128), :],
            s_self.at[a],
        )

    def shares(x_moves, y_moves):
        for t in range(2):
            for y2 in range(2):
                own = (2 * pair + t == x) & (y2 == yl) & home
                kind = ((2 * pair + t != x) == x_moves) & ((y2 != yl) == y_moves)

                @pl.when(kind & jnp.logical_not(own))
                def _():
                    share(1, t, y2).start()
                    share(0, t, y2).start()

    set_off(0, 0)
    shares(False, True)
    shares(False, False)

    @pl.when(home)
    def _():
        keep(0).start()
        keep(1).start()


    send_lat = remote(lat, latb, s_l, r_l, (m, z, 2 * pair + 1 - px, yl, px))

    @pl.when(home)
    def _():
        latf[...] = jnp.zeros((8, 512), F32)
        latf[0:3, :] = lat[...].astype(F32)

    @pl.when(home)
    def _():
        send_lat.start()

    buf1[x] = shl[x]
    for j in range(1, 4):
        m1(j).wait_recv()
    total = buf1[0] + buf1[1] + buf1[2] + buf1[3]
    for k in range(8):
        for j in range(2):
            tot[k, j : j + 1, :] = total[j, k : k + 1, :]

    def m2(j):
        to = lax.rem(z + j, 8)
        return remote(tot.at[to], buf2.at[z], s_m2.at[j], r_m2.at[j], (m, to, x, yl, c))

    for j in range(1, 8):
        m2(j).start()
    buf2[z] = tot[z]

    set_off(0, 1)
    s1_sends(True)

    for j in range(1, 8):
        m2(j).wait_recv()
    for k in range(8):
        mod[:, k * 640 : (k + 1) * 640] = buf2[k]
    loads[2].wait()

    def r1(t, k):
        return remote(
            made.at[pl.ds(k * ROW_CHUNK, ROW_CHUNK), :],
            rows.at[pl.ds((2 * yl + c) * 128 + k * ROW_CHUNK, ROW_CHUNK), :],
            s_r1.at[t, k], r_r1.at[c, k], (m, z, 2 * pair + t, yl, px),
        )

    for k in range(4):

        @pl.loop(0, ROW_CHUNK // 16)
        def _(i):
            at = pl.multiple_of(k * ROW_CHUNK + i * 16, 16)
            hidden = tok[pl.ds(at, 16), :].astype(F32)
            average = jnp.mean(hidden, axis=1, keepdims=True)
            centred = hidden - average
            variance = jnp.mean(centred * centred, axis=1, keepdims=True)
            normed = centred * lax.rsqrt(variance + 1e-06)
            made[pl.ds(at, 16), :] = (normed * (1.0 + mod[1:2, :]) + mod[0:1, :]).astype(BF)

        for t in range(2):
            own = (2 * pair + t == x) & home

            @pl.when(jnp.logical_not(own))
            def _():
                r1(t, k).start()

            @pl.when(own)
            def _():
                at = pl.multiple_of((2 * yl + c) * 128 + k * ROW_CHUNK, ROW_CHUNK)
                rows[pl.ds(at, ROW_CHUNK), :] = made[k * ROW_CHUNK : (k + 1) * ROW_CHUNK, :]

    def r2(p, k, ylo):
        spot = rows.at[pl.ds((2 * ylo + p) * 128 + k * ROW_CHUNK, ROW_CHUNK), :]
        return remote(spot, spot, s_r2.at[p, k], r_r2.at[p, k], up if p == 0 else down)

    def relay(k):
        for p in range(2):
            own = home & (c == p)

            @pl.when(jnp.logical_not(own))
            def _():
                spot = rows.at[pl.ds((2 * yl + p) * 128 + k * ROW_CHUNK, ROW_CHUNK), :]
                remote(
                    made.at[pl.ds(k * ROW_CHUNK, ROW_CHUNK), :],
                    spot, s_r1.at[0, k], r_r1.at[p, k], sib,
                ).wait_recv()

            r2(p, k, yl).start()

    @pl.when(home)
    def _():
        for k in range(4):
            relay(k)

    set_off(1, 0)
    set_off(1, 1)
    shares(True, False)


    @pl.when(away)
    def _():
        send_lat.wait_recv()
        latf[...] = jnp.zeros((8, 512), F32)
        latf[0:3, :] = latb[...].astype(F32)

    @pl.loop(0, 4)
    def _(i):
        at = pl.multiple_of(i * BLOCK, BLOCK)
        angles = lax.dot_general(
            latf[:, pl.ds(at, BLOCK)], rope_frequency(), (((0,), (0,)), ((), ())),
            precision=lax.Precision.HIGHEST, preferred_element_type=F32,
        )
        column = lax.broadcasted_iota(jnp.int32, (BLOCK, HEAD_SIZE), 1)
        cosb[pl.ds(at, BLOCK), :] = jnp.cos(angles)
        sine = jnp.sin(angles)
        sinb[pl.ds(at, BLOCK), :] = jnp.where(column < HEAD_SIZE // 2, -sine, sine)

    def ring_step(n):
        for e in range(2):
            for a in range(2):
                ring(a, n, e).wait_recv()
                if n < 4:
                    ring(a, n + 2, e).start()
                across(a, n + 1, e).start()
        if n >= 4:

            @pl.when(collector if n == 4 else jnp.logical_not(collector))
            def _():
                for a in range(2):
                    for e in range(2):
                        ring(a, 6, e).start()

    ring_step(0)
    for k in range(4):
        ring_step(k + 1)

        @pl.when(away)
        def _():
            relay(k)

    def project(a, zo, first, part=None):
        acc, big = ((kacc, bigk), (qacc, bigq))[a]
        cols = pl.ds(pl.multiple_of(zo * 640, 128), 640)

        at = slice(None) if part is None else pl.ds(pl.multiple_of(part * 256, 256), 256)
        term = jnp.dot(rows[at, cols], big[zo], preferred_element_type=F32)
        acc[at, :] = term if first else acc[at, :] + term

    def at_distance(d):
        return lax.rem(z + d + 8, 8)

    def near_slices(part):
        for a in range(2):
            project(a, z, True, part)

        @pl.loop(0, 4)
        def _(i):
            d = jnp.where(i == 0, 1, jnp.where(i == 1, -1, jnp.where(i == 2, 2, -2)))
            for a in range(2):
                project(a, at_distance(d), False, part)

    def crossed(*steps):
        for n in steps:
            for a in range(2):
                for e in range(2):
                    across(a, n, e).wait_recv()

    crossed(1, 2, 3, 4)
    near_slices(yl)
    ring_step(5)
    for k in range(4):
        for p in range(2):
            r2(p, k, 1 - yl).wait_recv()

    shares(True, True)
    near_slices(1 - yl)
    crossed(5, 6)

    @pl.loop(0, 2)
    def _(i):
        for a in range(2):
            project(a, at_distance(3 - 6 * i), False)


    def last_in(a, e):
        ring(a, 6, e).wait_recv()
        across(a, 7, e).start()

    def last_step(a):
        for e in range(2):
            across(a, 7, e).wait_recv()
        project(a, at_distance(4), False)

    last_in(0, 0)
    last_in(0, 1)

    def turned(pre, at):
        inverse = lax.rsqrt(jnp.mean(pre * pre, axis=1, keepdims=True) + 1e-06)
        normed = pre * inverse
        rotated = normed * cosb[at, :] + pltpu.roll(normed, HEAD_SIZE // 2, 1) * sinb[at, :]
        return inverse, normed, rotated.astype(BF)

    last_step(0)

    @pl.loop(0, 4)
    def _(i):
        at = pl.ds(pl.multiple_of(i * BLOCK, BLOCK), BLOCK)
        for j in range(3):
            lanes = pl.ds(pl.multiple_of((2 * m + j) * 128, 128), 128)
            krot[at, lanes] = turned(kacc[at, j * 128 : (j + 1) * 128], at)[2]

    def keys(who):
        spot = krot.at[:, pl.ds(pl.multiple_of(who * KW, 128), 256)]
        return remote(spot, spot, s_k, r_k, mate)

    keys(m).start()
    last_in(1, 0)
    last_in(1, 1)
    last_step(1)

    for hd in range(4):
        own = home & (hd == 2 * yl + c)

        @pl.when(jnp.logical_not(own))
        def _():
            for a, (src, dst) in enumerate(((val, vals), (cot, cots))):
                remote(
                    src.at[:, 0:640], dst.at[hd * 128 : (hd + 1) * 128, :],
                    s_v.at[a, 0, 0], r_v.at[a, hd], sib,
                ).wait_recv()

    @pl.when(home)
    def _():
        keep(0).wait()
        keep(1).wait()

    scale = HEAD_SIZE ** (-0.5)

    def one_block(lanes, at):
        inverse, normed, query = turned(qacc[at, lanes], at)
        key, value = krot[:, lanes], vals[:, lanes]
        nt = (((1,), (1,)), ((), ()))
        scores = lax.dot_general(query, key, nt, preferred_element_type=F32)
        raised = jnp.exp2(scores * (scale * math.log2(math.e)))
        grad_probs = lax.dot_general(cots[at, lanes], value, nt, preferred_element_type=F32)
        share_of = 1.0 / jnp.sum(raised, axis=1, keepdims=True)
        probs = raised * share_of
        inner = jnp.sum(probs * grad_probs, axis=1, keepdims=True)
        grad_scores = (probs * (grad_probs - inner)).astype(BF)
        turn = jnp.dot(grad_scores, key, preferred_element_type=F32) * scale
        grad = turn * cosb[at, :] + pltpu.roll(turn * sinb[at, :], HEAD_SIZE // 2, 1)
        mean = jnp.mean(grad * normed, axis=1, keepdims=True)
        gq[at, lanes] = (inverse * (grad - normed * mean)).astype(BF)

    def attend(first, count):
        @pl.loop(0, count)
        def _(i):
            lanes = pl.ds(pl.multiple_of((first + i) * 128, 128), 128)
            for b in range(512 // QUERY):
                one_block(lanes, pl.ds(b * QUERY, QUERY))

    copy_q = remote(wqv, qo, s_q, r_q, mate)
    copy_q.start()

    mine, other = pl.ds(c * HALF, HALF), pl.ds((1 - c) * HALF, HALF)

    def zat(j):
        return lax.rem(z + dz * j + 16, 8)

    class Reduce:
        def __init__(self, g, lane, bufs):
            self.g, self.width = g, bufs[0].shape[2]
            self.lanes = pl.ds(pl.multiple_of(lane, 128), self.width)
            (self.own, self.sib, self.got, self.arrived, self.out, self.last, self.last_got,
             self.last_arr, self.fin) = bufs

        def squares(self, zs, dst):
            cols = pl.ds(pl.multiple_of(zs * 640, 128), 640)
            g = lax.dot_general(
                rows[:, cols], gq[:, self.lanes], (((0,), (0,)), ((), ())),
                preferred_element_type=F32,
            )
            dst[...] = (g * g).astype(BF)

        def pass_on(self, q):
            if q == 0:
                src, dst = self.own.at[3, other, :], self.got.at[3, other, :]
            elif q < 4:
                src, dst = self.sib.at[3 - q], self.got.at[3 - q]
            elif q == 4:
                src, dst = self.last.at[other, :], self.last_got
            else:
                src, dst = self.arrived.at[5, q - 5], self.last_arr.at[q - 5]
            return remote(src, dst, s_sd.at[self.g, q], r_sd.at[self.g, q], sib)

        def passed(self, q):
            if q == 0:
                return remote(
                    self.own.at[3, mine, :], self.got.at[3, mine, :],
                    s_sd.at[self.g, q], r_sd.at[self.g, q], sib,
                )
            return self.pass_on(q)

        def sums(self, n, u):
            return remote(
                self.out.at[n, u], self.arrived.at[n, u], s_sr.at[self.g, n, u],
                r_sr.at[self.g, n, u], (m, znext, x, yl, c),
            )

        def send_on(self, n):
            j = (8 - n) // 2 - 1
            base = (c if n % 2 == 0 else 1 - c) * HALF
            for u in range(2):
                if n >= 2:
                    self.sums(n - 2, u).wait_recv()

                @pl.loop(0, SLICE // 32)
                def _(i):
                    at = pl.ds(pl.multiple_of(i * 32, 32), 32)
                    far = pl.ds(pl.multiple_of(base + u * SLICE + i * 32, 32), 32)
                    total = self.own[j, far, :].astype(F32) + self.got[j, far, :].astype(F32)
                    if n >= 2:
                        total = total + self.arrived[n - 2, u, at, :].astype(F32)
                    self.out[n, u, at, :] = total.astype(BF)

                self.sums(n, u).start()

        def start(self):
            self.squares(zat(4), self.own.at[3])
            self.pass_on(0).start()
            self.squares(zat(-3), self.sib.at[2])
            self.pass_on(1).start()
            self.passed(0).wait_recv()
            self.send_on(0)
            self.squares(zat(3), self.own.at[2])
            self.passed(1).wait_recv()
            self.send_on(1)

        def middle(self, k):
            self.squares(zat(k - 4), self.sib.at[3 - k])
            self.pass_on(k).start()
            self.squares(zat(4 - k), self.own.at[3 - k])
            self.send_on(2 * k - 2)
            self.passed(k).wait_recv()
            self.send_on(2 * k - 1)

        def own_slice(self):
            self.squares(z, self.last)
            self.pass_on(4).start()

        def xs(self, u):
            return remote(
                self.fin.at[u], xb.at[hh, :, self.lanes], s_x.at[self.g, u], r_x.at[self.g, hh],
                (m, z, 2 * c + u, yl, px),
            )

        def finish(self):
            for u in range(2):
                self.sums(5, u).wait_recv()
                self.pass_on(5 + u).start()
            self.passed(4).wait_recv()
            for u in range(2):
                self.passed(5 + u).wait_recv()
                self.sums(6, u).wait_recv()

                @pl.loop(0, SLICE // 32)
                def _(i):
                    at = pl.ds(pl.multiple_of(i * 32, 32), 32)
                    near = pl.ds(pl.multiple_of(u * SLICE + i * 32, 32), 32)
                    far = pl.ds(pl.multiple_of(c * HALF + u * SLICE + i * 32, 32), 32)
                    total = self.last[far, :].astype(F32) + self.last_got[near, :].astype(F32)
                    total = total + self.arrived[6, u, at, :].astype(F32)
                    total = total + self.last_arr[u, at, :].astype(F32)
                    self.fin[u, at, :] = total.astype(BF)

                own = (2 * c + u == x) & home

                @pl.when(jnp.logical_not(own))
                def _():
                    self.xs(u).start()

                @pl.when(own)
                def _():
                    xb[hh, :, self.lanes] = self.fin[u]

        def weigh(self):
            for t in range(2):
                own = (c + 2 * t == x) & (hh == c)

                @pl.when(jnp.logical_not(own))
                def _():
                    remote(
                        self.fin.at[0], xb.at[t, :, self.lanes], s_x.at[self.g, 0],
                        r_x.at[self.g, t], sib,
                    ).wait_recv()

            fisher = xb[0, :, self.lanes].astype(F32) + xb[1, :, self.lanes].astype(F32)
            wo[:, self.lanes] = (fisher + damping).astype(BF)
            self.mate_copy().start()

        def mate_copy(self):
            return remote(
                wo.at[:, self.lanes], wi.at[:, self.lanes], s_w.at[self.g], r_w.at[self.g], mate
            )

        def drain(self):
            for n in range(7):
                for u in range(2):
                    self.sums(n, u).wait_send()
            for q in range(7):
                self.pass_on(q).wait_send()
            for u in range(2):
                own = (2 * c + u == x) & home

                @pl.when(jnp.logical_not(own))
                def _():
                    self.xs(u).wait_send()

            self.mate_copy().wait()

    part_a = Reduce(0, m * 256, (own_a, sib_a, got_a, arr_a, out_a, last_a, lgot_a, larr_a, fin_a))
    part_b = Reduce(
        1, (1 - m) * KW, (own_b, sib_b, got_b, arr_b, out_b, last_b, lgot_b, larr_b, fin_b)
    )

    attend(2 * m, 3)
    part_a.start()
    keys(1 - m).wait_recv()
    attend(3 - 3 * m, 2)
    part_a.middle(2)
    part_b.start()
    part_a.middle(3)
    part_b.middle(2)
    part_a.own_slice()
    part_a.send_on(6)
    part_b.middle(3)
    part_b.own_slice()
    part_a.finish()
    part_b.send_on(6)
    part_b.finish()
    part_a.weigh()
    part_b.weigh()

    for j in range(1, 4):
        m1(j).wait_send()
    for j in range(1, 8):
        m2(j).wait_send()

    @pl.when(home)
    def _():
        send_lat.wait_send()

    for t in range(2):
        own = (c + 2 * t == x) & (hh == c)

        @pl.when(jnp.logical_not(own))
        def _():
            for a in range(2):
                s1(a, t).wait_send()

        own_r = (2 * pair + t == x) & home

        @pl.when(jnp.logical_not(own_r))
        def _():
            for k in range(4):
                r1(t, k).wait_send()

        for y2 in range(2):
            own_v = (2 * pair + t == x) & (y2 == yl) & home

            @pl.when(jnp.logical_not(own_v))
            def _():
                share(0, t, y2).wait_send()
                share(1, t, y2).wait_send()

    for a in range(2):
        for e in range(2):
            for n in range(7):
                ring(a, n, e).wait_send()
            for n in range(1, 8):
                across(a, n, e).wait_send()
        across(a, 0, 1).wait_send()

        @pl.when(jnp.logical_not(collector & away))
        def _():
            across(a, 0, 0).wait_send()
    for k in range(4):
        for p in range(2):
            r2(p, k, yl).wait_send()
    keys(m).wait_send()
    copy_q.wait()
    part_a.drain()
    part_b.drain()


def step(timestep, tw, lattice, tokens, own_query, own_key, values, cotangent):
    vmem = pl.BlockSpec(memory_space=pltpu.VMEM)
    hbm = pl.BlockSpec(memory_space=pltpu.HBM)
    dma = pltpu.SemaphoreType.DMA

    def v(shape, dtype=BF):
        return pltpu.VMEM(shape, dtype)

    def in_hbm(a):
        return pltpu.with_memory_space_constraint(a, pltpu.HBM)

    def sums_of(width):
        return (
            v((4, 640, width)), v((3, 640, width)), v((4, 640, width)),
            v((7, 2, SLICE, width)), v((7, 2, SLICE, width)),
            v((640, width)), v((HALF, width)), v((2, SLICE, width)), v((2, SLICE, width)),
        )

    return pl.pallas_call(
        kernel,
        out_shape=(
            jax.ShapeDtypeStruct((2, SLICE, 640), BF),
            jax.ShapeDtypeStruct((SLICE, 640), BF),
            jax.ShapeDtypeStruct((SLICE, 640), BF),
            jax.ShapeDtypeStruct((SLICE, 640), BF),
            jax.ShapeDtypeStruct((SLICE, 640), BF),
        ),
        in_specs=[pl.BlockSpec(memory_space=pltpu.SMEM)] + [hbm] * 7,
        out_specs=(vmem,) * 5,
        scratch_shapes=[
            v((128, 5120)), v((SLICE, KW)), v((8, 640, 640)), v((8, 640, KW)),
            v((512, 5120)), v((512, 640)), v((512, 640)), v((128, 5120)),
            v((2, SLICE, 256)), v((3, 512), jnp.int32), v((32, 128), F32), v((2, 640, 256)), v((4, 2, 8, 640), F32), v((4, 2, 8, 640), F32),
            v((8, 2, 640), F32), v((8, 2, 640), F32), v((2, 5120), F32),
            v((3, 512), jnp.int32), v((8, 512), F32), v((512, 128), F32), v((512, 128), F32),
            v((512, 640), F32), v((512, KW), F32), v((512, 640)), v((512, 640)),
            *sums_of(KW), *sums_of(256),
            dma((7,)), dma((2,)), dma, dma,
            dma((4,)), dma((4,)), dma((8,)), dma((8,)), dma((2, 2)), dma((2, 2)),
            dma((2, 7, 2)), dma((2, 7, 2)), dma((2, 8, 2)), dma((2, 8, 2)),
            dma((2, 4)), dma((2, 4)), dma((2, 4)), dma((2, 4)), dma((2, 2, 2)), dma((2, 4)),
            dma, dma,
            dma((2, 7)), dma((2, 7)), dma((2, 7, 2)), dma((2, 7, 2)), dma((2, 2)), dma((2, 2)),
            dma, dma, dma((2,)), dma((2,)),
        ],
        compiler_params=pltpu.CompilerParams(
            collective_id=0, has_side_effects=True, vmem_limit_bytes=52 * 1024 * 1024
        ),
        name="fisher_step",
    )(timestep, *(in_hbm(a) for a in (tw, lattice, tokens, own_query, own_key, values, cotangent)))


def on_device(tokens, lattice, timestep, time_weight, query_weight, key_weight, values, cotangent):
    member = lax.axis_index("member")
    xb, wo, wi, qo, mine = step(
        timestep, time_weight.transpose(0, 2, 1), lattice, tokens,
        query_weight[0], key_weight, values, cotangent[0],
    )
    fisher = xb[0].astype(F32) + xb[1].astype(F32)
    first = member == 0
    w0, w1 = jnp.where(first, wo, wi).astype(F32), jnp.where(first, wi, wo).astype(F32)
    q0, q1 = jnp.where(first, mine, qo).astype(F32), jnp.where(first, qo, mine).astype(F32)
    return (fisher[None], (w0 * q0 + w1 * q1) / (w0 + w1))


def solution(mesh):
    finer = Mesh(mesh.devices.reshape(mesh.shape["member"], 8, 4, 2, 2), AXES)
    in_specs = (
        P(SEQ_HEAD, None),
        P(None, SEQ),
        P(),
        P(None, None, SEQ),
        P("member", SEQ, HEAD),
        P(SEQ, HEAD),
        P(SEQ_HEAD, None),
        P("member", SEQ_HEAD, None),
    )
    out_specs = (P("member", SEQ, HEAD), P(SEQ, HEAD))
    return jax.shard_map(
        on_device, mesh=finer, in_specs=in_specs, out_specs=out_specs, check_vma=False
    )
```

```python
import math

import jax
import jax.numpy as jnp
from jax import lax
from jax.experimental import pallas as pl
from jax.experimental.pallas import tpu as pltpu
from jax.sharding import Mesh
from jax.sharding import PartitionSpec as P

HEAD_SIZE = 128
AXES = ("member", "z", "x", "ylo", "core")
SEQ = ("z", "x")
HEAD = ("ylo", "core")
SEQ_HEAD = ("z", "x", "ylo", "core")
MESH = pl.DeviceIdType.MESH

damping = 0.01
SLICE = 160
HALF = 320
KW = 384
ROW_CHUNK = 32
BLOCK = 128
QUERY = 256
F32, BF = jnp.float32, jnp.bfloat16


def place():
    return tuple(lax.axis_index(a) for a in AXES)


def remote(src, dst, send, recv, to):
    return pltpu.make_async_remote_copy(
        src_ref=src, dst_ref=dst, send_sem=send, recv_sem=recv, device_id=to, device_id_type=MESH
    )


def hello(to):
    pl.semaphore_signal(pltpu.get_barrier_semaphore(), inc=1, device_id=to, device_id_type=MESH)


def rope_frequency():
    halfway, side = HEAD_SIZE // 2, HEAD_SIZE // 6
    frame = halfway - 2 * side
    shape = (8, HEAD_SIZE)
    row = lax.broadcasted_iota(jnp.int32, shape, 0)
    column = lax.broadcasted_iota(jnp.int32, shape, 1)
    pair = jnp.where(column < halfway, column, column - halfway)
    axis = jnp.where(pair < frame, 0, jnp.where(pair < frame + side, 1, 2))
    anchor = jnp.where(axis == 0, 0, jnp.where(axis == 1, frame, frame + side))
    span = jnp.where(axis == 0, frame, side).astype(F32)
    frequency = jnp.exp(-math.log(10000.0) * (pair - anchor).astype(F32) / span)
    return jnp.where(row == axis, frequency, 0.0)


def kernel(
    when, tw_hbm, lat_hbm, tok_hbm, wq_hbm, wk_hbm, val, cot,
    xb, wi, qo, wqv,
    wo, tok, wkv, bigq, bigk, rows, vals, cots, made,
    tw, lat, ang, wide, shl, buf1, tot, buf2, mod, latb, latf, cosb, sinb,
    qacc, kacc, krot, gq,
    own_a, sib_a, got_a, arr_a, out_a, last_a, lgot_a, larr_a, fin_a,
    own_b, sib_b, got_b, arr_b, out_b, last_b, lgot_b, larr_b, fin_b,
    s_in, s_self, s_l, r_l,
    s_m1, r_m1, s_m2, r_m2, s_s1, r_s1, s_rg, r_rg, s_dd, r_dd,
    s_r1, r_r1, s_r2, r_r2, s_v, r_v, s_k, r_k,
    s_sd, r_sd, s_sr, r_sr, s_x, r_x, s_q, r_q, s_w, r_w,
):
    m, z, x, yl, c = place()
    px, pair, hh = lax.rem(x, 2), x // 2, x // 2
    sib = (m, z, x, yl, 1 - c)
    mate = (1 - m, z, x, yl, c)
    dz = 1 - 2 * c
    znext = lax.rem(z + dz + 8, 8)
    home = c == px
    up = (jnp.where(yl == 0, m, 1 - m), z, x, 1 - yl, c)
    down = (jnp.where(yl == 0, 1 - m, m), z, x, 1 - yl, c)
    away = jnp.logical_not(home)

    loads = [
        pltpu.make_async_copy(wk_hbm.at[:, pl.ds(pl.multiple_of(m * 256, 128), KW)], wkv, s_in.at[0]),
        pltpu.make_async_copy(wq_hbm, wqv, s_in.at[1]),
        pltpu.make_async_copy(tok_hbm, tok, s_in.at[2]),
        pltpu.make_async_copy(tw_hbm, tw, s_in.at[5]),
        pltpu.make_async_copy(lat_hbm, lat, s_in.at[6]),
    ]
    for load in loads:
        load.start()
    key_columns = pl.ds(pl.multiple_of(m * 256, 128), KW)
    own_weights = [
        pltpu.make_async_copy(
            wk_hbm.at[:, key_columns], bigk.at[z, pl.ds(x * SLICE, SLICE), :], s_in.at[3]
        ),
        pltpu.make_async_copy(wq_hbm, bigq.at[z, pl.ds(x * SLICE, SLICE), :], s_in.at[4]),
    ]

    @pl.when(home)
    def _():
        for load in own_weights:
            load.start()

    for j in range(1, 16):
        q = lax.rem(x * 4 + yl * 2 + c + j, 16)
        hello((m, z, q // 4, lax.rem(q, 4) // 2, lax.rem(q, 2)))
    for j in range(1, 8):
        hello((m, lax.rem(z + j, 8), x, yl, c))
    hello((1 - m, z, x, 1 - yl, c))
    hello(mate)

    ladder = lax.broadcasted_iota(jnp.int32, (1, 128), 1).astype(F32)
    frequency = jnp.exp(-math.log(10000.0) * 2.0 * ladder / 256)
    for a in range(4):
        for b in range(8):
            r = a * 8 + b
            ang[r : r + 1, :] = when[b * 4 + a].astype(F32) * frequency
    loads[3].wait()
    loads[4].wait()
    for j in range(2):
        wide[j] = jnp.zeros((640, 256), BF)
        wide[j, pl.ds(pl.multiple_of(x * SLICE, SLICE), SLICE), :] = tw[j]
    angle = ang[...]
    feature = jnp.concatenate([jnp.cos(angle), jnp.sin(angle)], axis=1).astype(BF)
    for j in range(2):
        part = lax.dot_general(
            feature, wide[j], (((1,), (1,)), ((), ())), preferred_element_type=F32
        )
        for a in range(4):
            shl[a, j] = part[a * 8 : (a + 1) * 8, :]
    for load in loads[:2]:
        load.wait()

    pl.semaphore_wait(pltpu.get_barrier_semaphore(), 24)

    window = pl.ds(pl.multiple_of(x * 128, 128), 256)

    def m1(j):
        to = lax.rem(x + j, 4)
        return remote(
            shl.at[to, :, :, window], buf1.at[x], s_m1.at[j], r_m1.at[j], (m, z, to, yl, c)
        )

    for j in range(1, 4):
        m1(j).start()

    def s1(a, t):
        src, dst = ((wkv, bigk), (wqv, bigq))[a]
        return remote(
            src, dst.at[z, pl.ds(x * SLICE, SLICE), :], s_s1.at[a, t],
            r_s1.at[a, lax.rem(x, 2)], (m, z, c + 2 * t, yl, hh),
        )

    def s1_sends(two_hops):
        for a in range(2):
            for t in range(2):
                own = (c + 2 * t == x) & (hh == c)
                far = home & (c + 2 * t != x)

                @pl.when(far if two_hops else jnp.logical_not(own | far))
                def _():
                    s1(a, t).start()

    s1_sends(False)

    @pl.when(home)
    def _():
        for load in own_weights:
            load.wait()

    def half_of(n):
        return c if n == 6 else (hh if n % 2 == 0 else 1 - hh)

    def piece(half, e):
        near = jnp.where(hh == half, px, 1 - px)
        return pl.ds((2 * half + (near if e == 0 else 1 - near)) * SLICE, SLICE)

    def ring(a, n, e):
        origin = lax.rem(z - dz * (n // 2) + 8, 8)
        spot = (bigk, bigq)[a].at[origin, piece(half_of(n), e), :]
        return remote(spot, spot, s_rg.at[a, n, e], r_rg.at[a, n, e], (m, znext, x, yl, c))

    def across(a, n, e):
        k = n - 1
        big = (bigk, bigq)[a]
        if n == 0:
            spot = big.at[z, piece(c, e), :]
        else:
            origin = lax.rem(z - dz * (k // 2 + 1) + 8, 8)
            spot = big.at[origin, piece(half_of(k), e), :]
        return remote(spot, spot, s_dd.at[a, n, e], r_dd.at[a, n, e], sib)

    def s1_arrived(a, e):
        near = jnp.where(hh == c, px, 1 - px)
        u = near if e == 0 else 1 - near
        own = (2 * c + u == x) & home

        @pl.when(jnp.logical_not(own))
        def _():
            src, dst = ((wkv, bigk), (wqv, bigq))[a]
            remote(
                src, dst.at[z, pl.ds((2 * c + u) * SLICE, SLICE), :],
                s_s1.at[a, 0], r_s1.at[a, u], sib,
            ).wait_recv()

    collector = hh == c

    def set_off(n, e):
        gathers = collector if n == 0 else jnp.logical_not(collector)

        @pl.when(gathers)
        def _():
            for a in range(2):
                s1_arrived(a, e)
                ring(a, n, e).start()
                if (n, e) == (0, 0):

                    @pl.when(home)
                    def _():
                        across(a, 0, e).start()
                else:
                    across(a, 0, e).start()

        @pl.when(jnp.logical_not(gathers))
        def _():
            for a in range(2):
                if (n, e) == (0, 0):

                    @pl.when(away)
                    def _():
                        across(a, 0, e).wait_recv()
                else:
                    across(a, 0, e).wait_recv()
                ring(a, n, e).start()

    def share(a, t, y2):
        h2 = 2 * y2 + t
        src, dst = ((val, vals), (cot, cots))[a]
        return remote(
            src.at[:, h2 * 640 : (h2 + 1) * 640],
            dst.at[pl.ds((2 * yl + c) * 128, 128), :],
            s_v.at[a, t, y2], r_v.at[a, 2 * yl + c], (m, z, 2 * pair + t, y2, px),
        )

    def keep(a):
        src, dst = ((val, vals), (cot, cots))[a]
        return pltpu.make_async_copy(
            src.at[:, pl.ds(pl.multiple_of((2 * yl + px) * 640, 128), 640)],
            dst.at[pl.ds((2 * yl + c) * 128, 128), :],
            s_self.at[a],
        )

    def shares(x_moves, y_moves):
        for t in range(2):
            for y2 in range(2):
                own = (2 * pair + t == x) & (y2 == yl) & home
                kind = ((2 * pair + t != x) == x_moves) & ((y2 != yl) == y_moves)

                @pl.when(kind & jnp.logical_not(own))
                def _():
                    share(1, t, y2).start()
                    share(0, t, y2).start()

    set_off(0, 0)
    shares(False, True)
    shares(False, False)

    @pl.when(home)
    def _():
        keep(0).start()
        keep(1).start()


    send_lat = remote(lat, latb, s_l, r_l, (m, z, 2 * pair + 1 - px, yl, px))

    @pl.when(home)
    def _():
        latf[...] = jnp.zeros((8, 512), F32)
        latf[0:3, :] = lat[...].astype(F32)

    @pl.when(home)
    def _():
        send_lat.start()

    buf1[x] = shl[x, :, :, window]
    for j in range(1, 4):
        m1(j).wait_recv()
    for j in range(2):
        lower = [buf1[a, j, :, 0:128] for a in range(4)]
        upper = [buf1[a, j, :, 128:256] for a in range(4)]
        tiles = [lower[0], *(upper[a] + lower[a + 1] for a in range(3)), upper[3]]
        total = jnp.concatenate(tiles, axis=1)
        for k in range(8):
            tot[k, j : j + 1, :] = total[k : k + 1, :]

    def m2(j):
        to = lax.rem(z + j, 8)
        return remote(tot.at[to], buf2.at[z], s_m2.at[j], r_m2.at[j], (m, to, x, yl, c))

    for j in range(1, 8):
        m2(j).start()
    buf2[z] = tot[z]

    set_off(0, 1)
    s1_sends(True)
    set_off(1, 0)

    for j in range(1, 8):
        m2(j).wait_recv()
    for k in range(8):
        mod[:, k * 640 : (k + 1) * 640] = buf2[k]
    loads[2].wait()

    def r1(t, k):
        return remote(
            made.at[pl.ds(k * ROW_CHUNK, ROW_CHUNK), :],
            rows.at[pl.ds((2 * yl + c) * 128 + k * ROW_CHUNK, ROW_CHUNK), :],
            s_r1.at[t, k], r_r1.at[c, k], (m, z, 2 * pair + t, yl, px),
        )

    for k in range(4):

        @pl.loop(0, ROW_CHUNK // 16)
        def _(i):
            at = pl.multiple_of(k * ROW_CHUNK + i * 16, 16)
            hidden = tok[pl.ds(at, 16), :].astype(F32)
            average = jnp.mean(hidden, axis=1, keepdims=True)
            centred = hidden - average
            variance = jnp.mean(centred * centred, axis=1, keepdims=True)
            normed = centred * lax.rsqrt(variance + 1e-06)
            made[pl.ds(at, 16), :] = (normed * (1.0 + mod[1:2, :]) + mod[0:1, :]).astype(BF)

        for t in range(2):
            own = (2 * pair + t == x) & home

            @pl.when(jnp.logical_not(own))
            def _():
                r1(t, k).start()

            @pl.when(own)
            def _():
                at = pl.multiple_of((2 * yl + c) * 128 + k * ROW_CHUNK, ROW_CHUNK)
                rows[pl.ds(at, ROW_CHUNK), :] = made[k * ROW_CHUNK : (k + 1) * ROW_CHUNK, :]

    def r2(p, k, ylo):
        spot = rows.at[pl.ds((2 * ylo + p) * 128 + k * ROW_CHUNK, ROW_CHUNK), :]
        return remote(spot, spot, s_r2.at[p, k], r_r2.at[p, k], up if p == 0 else down)

    def relay(k):
        for p in range(2):
            own = home & (c == p)

            @pl.when(jnp.logical_not(own))
            def _():
                spot = rows.at[pl.ds((2 * yl + p) * 128 + k * ROW_CHUNK, ROW_CHUNK), :]
                remote(
                    made.at[pl.ds(k * ROW_CHUNK, ROW_CHUNK), :],
                    spot, s_r1.at[0, k], r_r1.at[p, k], sib,
                ).wait_recv()

            r2(p, k, yl).start()

    @pl.when(home)
    def _():
        for k in range(4):
            relay(k)

    set_off(1, 1)
    shares(True, False)


    @pl.when(away)
    def _():
        send_lat.wait_recv()
        latf[...] = jnp.zeros((8, 512), F32)
        latf[0:3, :] = latb[...].astype(F32)

    @pl.loop(0, 4)
    def _(i):
        at = pl.multiple_of(i * BLOCK, BLOCK)
        angles = lax.dot_general(
            latf[:, pl.ds(at, BLOCK)], rope_frequency(), (((0,), (0,)), ((), ())),
            precision=lax.Precision.HIGHEST, preferred_element_type=F32,
        )
        column = lax.broadcasted_iota(jnp.int32, (BLOCK, HEAD_SIZE), 1)
        cosb[pl.ds(at, BLOCK), :] = jnp.cos(angles)
        sine = jnp.sin(angles)
        sinb[pl.ds(at, BLOCK), :] = jnp.where(column < HEAD_SIZE // 2, -sine, sine)

    def ring_step(n):
        for e in range(2):
            for a in range(2):
                ring(a, n, e).wait_recv()
                if n < 4:
                    ring(a, n + 2, e).start()
                across(a, n + 1, e).start()
        if n >= 4:

            @pl.when(collector if n == 4 else jnp.logical_not(collector))
            def _():
                for a in range(2):
                    for e in range(2):
                        ring(a, 6, e).start()

    ring_step(0)
    for k in range(4):
        ring_step(k + 1)

        @pl.when(away)
        def _():
            relay(k)

    def project(a, zo, first, part=None):
        acc, big = ((kacc, bigk), (qacc, bigq))[a]
        cols = pl.ds(pl.multiple_of(zo * 640, 128), 640)

        at = slice(None) if part is None else pl.ds(pl.multiple_of(part * 256, 256), 256)
        term = jnp.dot(rows[at, cols], big[zo], preferred_element_type=F32)
        acc[at, :] = term if first else acc[at, :] + term

    def at_distance(d):
        return lax.rem(z + d + 8, 8)

    def near_slices(part):
        for a in range(2):
            project(a, z, True, part)

        @pl.loop(0, 4)
        def _(i):
            d = jnp.where(i == 0, 1, jnp.where(i == 1, -1, jnp.where(i == 2, 2, -2)))
            for a in range(2):
                project(a, at_distance(d), False, part)

    def crossed(*steps):
        for n in steps:
            for a in range(2):
                for e in range(2):
                    across(a, n, e).wait_recv()

    crossed(1, 2, 3, 4)
    near_slices(yl)
    ring_step(5)
    for k in range(4):
        for p in range(2):
            r2(p, k, 1 - yl).wait_recv()

    shares(True, True)
    near_slices(1 - yl)
    crossed(5, 6)

    @pl.loop(0, 2)
    def _(i):
        for a in range(2):
            project(a, at_distance(3 - 6 * i), False)


    def last_in(a, e):
        ring(a, 6, e).wait_recv()
        across(a, 7, e).start()

    def last_step(a):
        for e in range(2):
            across(a, 7, e).wait_recv()
        project(a, at_distance(4), False)

    last_in(0, 0)
    last_in(0, 1)

    def turned(pre, at):
        inverse = lax.rsqrt(jnp.mean(pre * pre, axis=1, keepdims=True) + 1e-06)
        normed = pre * inverse
        rotated = normed * cosb[at, :] + pltpu.roll(normed, HEAD_SIZE // 2, 1) * sinb[at, :]
        return inverse, normed, rotated.astype(BF)

    last_step(0)

    @pl.loop(0, 4)
    def _(i):
        at = pl.ds(pl.multiple_of(i * BLOCK, BLOCK), BLOCK)
        for j in range(3):
            lanes = pl.ds(pl.multiple_of((2 * m + j) * 128, 128), 128)
            krot[at, lanes] = turned(kacc[at, j * 128 : (j + 1) * 128], at)[2]

    def keys(who):
        spot = krot.at[:, pl.ds(pl.multiple_of(who * KW, 128), 256)]
        return remote(spot, spot, s_k, r_k, mate)

    keys(m).start()
    last_in(1, 0)
    last_in(1, 1)
    last_step(1)

    for hd in range(4):
        own = home & (hd == 2 * yl + c)

        @pl.when(jnp.logical_not(own))
        def _():
            for a, (src, dst) in enumerate(((val, vals), (cot, cots))):
                remote(
                    src.at[:, 0:640], dst.at[hd * 128 : (hd + 1) * 128, :],
                    s_v.at[a, 0, 0], r_v.at[a, hd], sib,
                ).wait_recv()

    @pl.when(home)
    def _():
        keep(0).wait()
        keep(1).wait()

    scale = HEAD_SIZE ** (-0.5)

    def one_block(lanes, at):
        inverse, normed, query = turned(qacc[at, lanes], at)
        key, value = krot[:, lanes], vals[:, lanes]
        nt = (((1,), (1,)), ((), ()))
        scores = lax.dot_general(query, key, nt, preferred_element_type=F32)
        raised = jnp.exp2(scores * (scale * math.log2(math.e)))
        grad_probs = lax.dot_general(cots[at, lanes], value, nt, preferred_element_type=F32)
        share_of = 1.0 / jnp.sum(raised, axis=1, keepdims=True)
        probs = raised * share_of
        inner = jnp.sum(probs * grad_probs, axis=1, keepdims=True)
        grad_scores = (probs * (grad_probs - inner)).astype(BF)
        turn = jnp.dot(grad_scores, key, preferred_element_type=F32) * scale
        grad = turn * cosb[at, :] + pltpu.roll(turn * sinb[at, :], HEAD_SIZE // 2, 1)
        mean = jnp.mean(grad * normed, axis=1, keepdims=True)
        gq[at, lanes] = (inverse * (grad - normed * mean)).astype(BF)

    def attend(first, count):
        @pl.loop(0, count)
        def _(i):
            lanes = pl.ds(pl.multiple_of((first + i) * 128, 128), 128)
            for b in range(512 // QUERY):
                one_block(lanes, pl.ds(b * QUERY, QUERY))

    copy_q = remote(wqv, qo, s_q, r_q, mate)
    copy_q.start()

    mine, other = pl.ds(c * HALF, HALF), pl.ds((1 - c) * HALF, HALF)

    def zat(j):
        return lax.rem(z + dz * j + 16, 8)

    class Reduce:
        def __init__(self, g, lane, bufs):
            self.g, self.width = g, bufs[0].shape[2]
            self.lanes = pl.ds(pl.multiple_of(lane, 128), self.width)
            (self.own, self.sib, self.got, self.arrived, self.out, self.last, self.last_got,
             self.last_arr, self.fin) = bufs

        def squares(self, zs, dst):
            cols = pl.ds(pl.multiple_of(zs * 640, 128), 640)
            g = lax.dot_general(
                rows[:, cols], gq[:, self.lanes], (((0,), (0,)), ((), ())),
                preferred_element_type=F32,
            )
            dst[...] = (g * g).astype(BF)

        def pass_on(self, q):
            if q == 0:
                src, dst = self.own.at[3, other, :], self.got.at[3, other, :]
            elif q < 4:
                src, dst = self.sib.at[3 - q], self.got.at[3 - q]
            elif q == 4:
                src, dst = self.last.at[other, :], self.last_got
            else:
                src, dst = self.arrived.at[5, q - 5], self.last_arr.at[q - 5]
            return remote(src, dst, s_sd.at[self.g, q], r_sd.at[self.g, q], sib)

        def passed(self, q):
            if q == 0:
                return remote(
                    self.own.at[3, mine, :], self.got.at[3, mine, :],
                    s_sd.at[self.g, q], r_sd.at[self.g, q], sib,
                )
            return self.pass_on(q)

        def sums(self, n, u):
            return remote(
                self.out.at[n, u], self.arrived.at[n, u], s_sr.at[self.g, n, u],
                r_sr.at[self.g, n, u], (m, znext, x, yl, c),
            )

        def send_on(self, n):
            j = (8 - n) // 2 - 1
            base = (c if n % 2 == 0 else 1 - c) * HALF
            for u in range(2):
                if n >= 2:
                    self.sums(n - 2, u).wait_recv()

                @pl.loop(0, SLICE // 32)
                def _(i):
                    at = pl.ds(pl.multiple_of(i * 32, 32), 32)
                    far = pl.ds(pl.multiple_of(base + u * SLICE + i * 32, 32), 32)
                    total = self.own[j, far, :].astype(F32) + self.got[j, far, :].astype(F32)
                    if n >= 2:
                        total = total + self.arrived[n - 2, u, at, :].astype(F32)
                    self.out[n, u, at, :] = total.astype(BF)

                self.sums(n, u).start()

        def start(self):
            self.squares(zat(4), self.own.at[3])
            self.pass_on(0).start()
            self.squares(zat(-3), self.sib.at[2])
            self.pass_on(1).start()
            self.passed(0).wait_recv()
            self.send_on(0)
            self.squares(zat(3), self.own.at[2])
            self.passed(1).wait_recv()
            self.send_on(1)

        def middle(self, k):
            self.squares(zat(k - 4), self.sib.at[3 - k])
            self.pass_on(k).start()
            self.squares(zat(4 - k), self.own.at[3 - k])
            self.send_on(2 * k - 2)
            self.passed(k).wait_recv()
            self.send_on(2 * k - 1)

        def own_slice(self):
            self.squares(z, self.last)
            self.pass_on(4).start()

        def xs(self, u):
            return remote(
                self.fin.at[u], xb.at[hh, :, self.lanes], s_x.at[self.g, u], r_x.at[self.g, hh],
                (m, z, 2 * c + u, yl, px),
            )

        def finish(self):
            for u in range(2):
                self.sums(5, u).wait_recv()
                self.pass_on(5 + u).start()
            self.passed(4).wait_recv()
            for u in range(2):
                self.passed(5 + u).wait_recv()
                self.sums(6, u).wait_recv()

                @pl.loop(0, SLICE // 32)
                def _(i):
                    at = pl.ds(pl.multiple_of(i * 32, 32), 32)
                    near = pl.ds(pl.multiple_of(u * SLICE + i * 32, 32), 32)
                    far = pl.ds(pl.multiple_of(c * HALF + u * SLICE + i * 32, 32), 32)
                    total = self.last[far, :].astype(F32) + self.last_got[near, :].astype(F32)
                    total = total + self.arrived[6, u, at, :].astype(F32)
                    total = total + self.last_arr[u, at, :].astype(F32)
                    self.fin[u, at, :] = total.astype(BF)

                own = (2 * c + u == x) & home

                @pl.when(jnp.logical_not(own))
                def _():
                    self.xs(u).start()

                @pl.when(own)
                def _():
                    xb[hh, :, self.lanes] = self.fin[u]

        def weigh(self):
            for t in range(2):
                own = (c + 2 * t == x) & (hh == c)

                @pl.when(jnp.logical_not(own))
                def _():
                    remote(
                        self.fin.at[0], xb.at[t, :, self.lanes], s_x.at[self.g, 0],
                        r_x.at[self.g, t], sib,
                    ).wait_recv()

            fisher = xb[0, :, self.lanes].astype(F32) + xb[1, :, self.lanes].astype(F32)
            wo[:, self.lanes] = (fisher + damping).astype(BF)
            self.mate_copy().start()

        def mate_copy(self):
            return remote(
                wo.at[:, self.lanes], wi.at[:, self.lanes], s_w.at[self.g], r_w.at[self.g], mate
            )

        def drain(self):
            for n in range(7):
                for u in range(2):
                    self.sums(n, u).wait_send()
            for q in range(7):
                self.pass_on(q).wait_send()
            for u in range(2):
                own = (2 * c + u == x) & home

                @pl.when(jnp.logical_not(own))
                def _():
                    self.xs(u).wait_send()

            self.mate_copy().wait()

    part_a = Reduce(0, m * 256, (own_a, sib_a, got_a, arr_a, out_a, last_a, lgot_a, larr_a, fin_a))
    part_b = Reduce(
        1, (1 - m) * KW, (own_b, sib_b, got_b, arr_b, out_b, last_b, lgot_b, larr_b, fin_b)
    )

    attend(2 * m, 3)
    part_a.start()
    keys(1 - m).wait_recv()
    attend(3 - 3 * m, 2)
    part_a.middle(2)
    part_b.start()
    part_a.middle(3)
    part_b.middle(2)
    part_a.own_slice()
    part_a.send_on(6)
    part_b.middle(3)
    part_b.own_slice()
    part_a.finish()
    part_b.send_on(6)
    part_b.finish()
    part_a.weigh()
    part_b.weigh()

    for j in range(1, 4):
        m1(j).wait_send()
    for j in range(1, 8):
        m2(j).wait_send()

    @pl.when(home)
    def _():
        send_lat.wait_send()

    for t in range(2):
        own = (c + 2 * t == x) & (hh == c)

        @pl.when(jnp.logical_not(own))
        def _():
            for a in range(2):
                s1(a, t).wait_send()

        own_r = (2 * pair + t == x) & home

        @pl.when(jnp.logical_not(own_r))
        def _():
            for k in range(4):
                r1(t, k).wait_send()

        for y2 in range(2):
            own_v = (2 * pair + t == x) & (y2 == yl) & home

            @pl.when(jnp.logical_not(own_v))
            def _():
                share(0, t, y2).wait_send()
                share(1, t, y2).wait_send()

    for a in range(2):
        for e in range(2):
            for n in range(7):
                ring(a, n, e).wait_send()
            for n in range(1, 8):
                across(a, n, e).wait_send()
        across(a, 0, 1).wait_send()

        @pl.when(jnp.logical_not(collector & away))
        def _():
            across(a, 0, 0).wait_send()
    for k in range(4):
        for p in range(2):
            r2(p, k, yl).wait_send()
    keys(m).wait_send()
    copy_q.wait()
    part_a.drain()
    part_b.drain()


def step(timestep, tw, lattice, tokens, own_query, own_key, values, cotangent):
    vmem = pl.BlockSpec(memory_space=pltpu.VMEM)
    hbm = pl.BlockSpec(memory_space=pltpu.HBM)
    dma = pltpu.SemaphoreType.DMA

    def v(shape, dtype=BF):
        return pltpu.VMEM(shape, dtype)

    def in_hbm(a):
        return pltpu.with_memory_space_constraint(a, pltpu.HBM)

    def sums_of(width):
        return (
            v((4, 640, width)), v((3, 640, width)), v((4, 640, width)),
            v((7, 2, SLICE, width)), v((7, 2, SLICE, width)),
            v((640, width)), v((HALF, width)), v((2, SLICE, width)), v((2, SLICE, width)),
        )

    return pl.pallas_call(
        kernel,
        out_shape=(
            jax.ShapeDtypeStruct((2, SLICE, 640), BF),
            jax.ShapeDtypeStruct((SLICE, 640), BF),
            jax.ShapeDtypeStruct((SLICE, 640), BF),
            jax.ShapeDtypeStruct((SLICE, 640), BF),
        ),
        in_specs=[pl.BlockSpec(memory_space=pltpu.SMEM)] + [hbm] * 7,
        out_specs=(vmem,) * 4,
        scratch_shapes=[
            v((SLICE, 640)), v((128, 5120)), v((SLICE, KW)), v((8, 640, 640)), v((8, 640, KW)),
            v((512, 5120)), v((512, 640)), v((512, 640)), v((128, 5120)),
            v((2, SLICE, 256)), v((3, 512), jnp.int32), v((32, 128), F32), v((2, 640, 256)), v((4, 2, 8, 640), F32), v((4, 2, 8, 256), F32),
            v((8, 2, 640), F32), v((8, 2, 640), F32), v((2, 5120), F32),
            v((3, 512), jnp.int32), v((8, 512), F32), v((512, 128), F32), v((512, 128), F32),
            v((512, 640), F32), v((512, KW), F32), v((512, 640)), v((512, 640)),
            *sums_of(KW), *sums_of(256),
            dma((7,)), dma((2,)), dma, dma,
            dma((4,)), dma((4,)), dma((8,)), dma((8,)), dma((2, 2)), dma((2, 2)),
            dma((2, 7, 2)), dma((2, 7, 2)), dma((2, 8, 2)), dma((2, 8, 2)),
            dma((2, 4)), dma((2, 4)), dma((2, 4)), dma((2, 4)), dma((2, 2, 2)), dma((2, 4)),
            dma, dma,
            dma((2, 7)), dma((2, 7)), dma((2, 7, 2)), dma((2, 7, 2)), dma((2, 2)), dma((2, 2)),
            dma, dma, dma((2,)), dma((2,)),
        ],
        compiler_params=pltpu.CompilerParams(
            collective_id=0, has_side_effects=True, vmem_limit_bytes=52 * 1024 * 1024
        ),
        name="fisher_step",
    )(in_hbm(timestep), *(in_hbm(a) for a in (tw, lattice, tokens, own_query, own_key, values, cotangent)))


def on_device(tokens, lattice, timestep, time_weight, query_weight, key_weight, values, cotangent):
    member = lax.axis_index("member")
    xb, other, qo, mine = step(
        timestep, time_weight.transpose(0, 2, 1), lattice, tokens,
        query_weight[0], key_weight, values, cotangent[0],
    )
    fisher = xb[0].astype(F32) + xb[1].astype(F32)
    first = member == 0
    own, other = lax.reduce_precision(fisher + damping, 8, 7), other.astype(F32)
    w0, w1 = jnp.where(first, own, other), jnp.where(first, other, own)
    q0, q1 = jnp.where(first, mine, qo).astype(F32), jnp.where(first, qo, mine).astype(F32)
    return (fisher[None], (w0 * q0 + w1 * q1) / (w0 + w1))


def solution(mesh):
    finer = Mesh(mesh.devices.reshape(mesh.shape["member"], 8, 4, 2, 2), AXES)
    in_specs = (
        P(SEQ_HEAD, None),
        P(None, SEQ),
        P(),
        P(None, None, SEQ),
        P("member", SEQ, HEAD),
        P(SEQ, HEAD),
        P(SEQ_HEAD, None),
        P("member", SEQ_HEAD, None),
    )
    out_specs = (P("member", SEQ, HEAD), P(SEQ, HEAD))
    return jax.shard_map(
        on_device, mesh=finer, in_specs=in_specs, out_specs=out_specs, check_vma=False
    )
```

```python
import math

import jax
import jax.numpy as jnp
from jax import lax
from jax.experimental import pallas as pl
from jax.experimental.pallas import tpu as pltpu
from jax.sharding import Mesh
from jax.sharding import PartitionSpec as P

HEAD_SIZE = 128
AXES = ("member", "z", "x", "ylo", "core")
SEQ = ("z", "x")
HEAD = ("ylo", "core")
SEQ_HEAD = ("z", "x", "ylo", "core")
MESH = pl.DeviceIdType.MESH

damping = 0.01
SLICE = 160
HALF = 320
KW = 384
ROW_CHUNK = 32
BLOCK = 128
QUERY = 256
F32, BF = jnp.float32, jnp.bfloat16


def place():
    return tuple(lax.axis_index(a) for a in AXES)


def remote(src, dst, send, recv, to):
    return pltpu.make_async_remote_copy(
        src_ref=src, dst_ref=dst, send_sem=send, recv_sem=recv, device_id=to, device_id_type=MESH
    )


def hello(to):
    pl.semaphore_signal(pltpu.get_barrier_semaphore(), inc=1, device_id=to, device_id_type=MESH)


def rope_frequency():
    halfway, side = HEAD_SIZE // 2, HEAD_SIZE // 6
    frame = halfway - 2 * side
    shape = (8, HEAD_SIZE)
    row = lax.broadcasted_iota(jnp.int32, shape, 0)
    column = lax.broadcasted_iota(jnp.int32, shape, 1)
    pair = jnp.where(column < halfway, column, column - halfway)
    axis = jnp.where(pair < frame, 0, jnp.where(pair < frame + side, 1, 2))
    anchor = jnp.where(axis == 0, 0, jnp.where(axis == 1, frame, frame + side))
    span = jnp.where(axis == 0, frame, side).astype(F32)
    frequency = jnp.exp(-math.log(10000.0) * (pair - anchor).astype(F32) / span)
    return jnp.where(row == axis, frequency, 0.0)


def kernel(
    when, tw_hbm, lat_hbm, tok_hbm, wq_hbm, wk_hbm, val, cot,
    xb, wi, qo, wqv,
    wo, tok, wkv, bigq, bigqb, bigk, rows, vals, cots, made,
    tw, lat, ang, wide, shl, buf1, tot, buf2, mod, latb, latf, cosb, sinb,
    qacc, kacc, krot, gq,
    own_a, sib_a, got_a, arr_a, out_a, last_a, lgot_a, larr_a, fin_a,
    own_b, sib_b, got_b, arr_b, out_b, last_b, lgot_b, larr_b, fin_b,
    s_in, s_self, s_l, r_l,
    s_m1, r_m1, s_m2, r_m2, s_s1, r_s1, s_rg, r_rg, s_dd, r_dd,
    s_r1, r_r1, s_r2, r_r2, s_v, r_v, s_k, r_k,
    s_sd, r_sd, s_sr, r_sr, s_x, r_x, s_q, r_q, s_w, r_w,
):
    m, z, x, yl, c = place()
    px, pair, hh = lax.rem(x, 2), x // 2, x // 2
    sib = (m, z, x, yl, 1 - c)
    mate = (1 - m, z, x, yl, c)
    dz = 1 - 2 * c
    znext = lax.rem(z + dz + 8, 8)
    home = c == px
    up = (jnp.where(yl == 0, m, 1 - m), z, x, 1 - yl, c)
    down = (jnp.where(yl == 0, 1 - m, m), z, x, 1 - yl, c)
    away = jnp.logical_not(home)

    loads = [
        pltpu.make_async_copy(wk_hbm.at[:, pl.ds(pl.multiple_of(m * 256, 128), KW)], wkv, s_in.at[0]),
        pltpu.make_async_copy(wq_hbm, wqv, s_in.at[1]),
        pltpu.make_async_copy(tok_hbm, tok, s_in.at[2]),
        pltpu.make_async_copy(tw_hbm, tw, s_in.at[5]),
        pltpu.make_async_copy(lat_hbm, lat, s_in.at[6]),
    ]
    for load in loads:
        load.start()
    lanes_a = pl.ds(pl.multiple_of(m * 256, 128), KW)
    lanes_b = pl.ds(pl.multiple_of((1 - m) * KW, 128), 256)
    gathered = (bigk, bigq, bigqb)

    def weights_of(a):
        return (wkv, wqv.at[:, lanes_a], wqv.at[:, lanes_b])[a]

    own_weights = [
        pltpu.make_async_copy(
            wk_hbm.at[:, lanes_a], bigk.at[z, pl.ds(x * SLICE, SLICE), :], s_in.at[3]
        ),
        pltpu.make_async_copy(
            wq_hbm.at[:, lanes_a], bigq.at[z, pl.ds(x * SLICE, SLICE), :], s_in.at[4]
        ),
        pltpu.make_async_copy(
            wq_hbm.at[:, lanes_b], bigqb.at[z, pl.ds(x * SLICE, SLICE), :], s_in.at[7]
        ),
    ]

    @pl.when(home)
    def _():
        for load in own_weights:
            load.start()

    for j in range(1, 16):
        q = lax.rem(x * 4 + yl * 2 + c + j, 16)
        hello((m, z, q // 4, lax.rem(q, 4) // 2, lax.rem(q, 2)))
    for j in range(1, 8):
        hello((m, lax.rem(z + j, 8), x, yl, c))
    hello((1 - m, z, x, 1 - yl, c))
    hello(mate)

    ladder = lax.broadcasted_iota(jnp.int32, (1, 128), 1).astype(F32)
    frequency = jnp.exp(-math.log(10000.0) * 2.0 * ladder / 256)
    for a in range(4):
        for b in range(8):
            r = a * 8 + b
            ang[r : r + 1, :] = when[b * 4 + a].astype(F32) * frequency
    loads[3].wait()
    loads[4].wait()
    for j in range(2):
        wide[j] = jnp.zeros((640, 256), BF)
        wide[j, pl.ds(pl.multiple_of(x * SLICE, SLICE), SLICE), :] = tw[j]
    angle = ang[...]
    feature = jnp.concatenate([jnp.cos(angle), jnp.sin(angle)], axis=1).astype(BF)
    for j in range(2):
        part = lax.dot_general(
            feature, wide[j], (((1,), (1,)), ((), ())), preferred_element_type=F32
        )
        for a in range(4):
            shl[a, j] = part[a * 8 : (a + 1) * 8, :]
    for load in loads[:2]:
        load.wait()

    pl.semaphore_wait(pltpu.get_barrier_semaphore(), 24)

    window = pl.ds(pl.multiple_of(x * 128, 128), 256)

    def m1(j):
        to = lax.rem(x + j, 4)
        return remote(
            shl.at[to, :, :, window], buf1.at[x], s_m1.at[j], r_m1.at[j], (m, z, to, yl, c)
        )

    for j in range(1, 4):
        m1(j).start()

    def s1(a, t):
        src, dst = weights_of(a), gathered[a]
        return remote(
            src, dst.at[z, pl.ds(x * SLICE, SLICE), :], s_s1.at[a, t],
            r_s1.at[a, lax.rem(x, 2)], (m, z, c + 2 * t, yl, hh),
        )

    def s1_sends(two_hops, arrays=(0, 1)):
        for a in arrays:
            for t in range(2):
                own = (c + 2 * t == x) & (hh == c)
                far = home & (c + 2 * t != x)

                @pl.when(far if two_hops else jnp.logical_not(own | far))
                def _():
                    s1(a, t).start()

    s1_sends(False)

    @pl.when(home)
    def _():
        for load in own_weights:
            load.wait()

    def half_of(n):
        return c if n == 6 else (hh if n % 2 == 0 else 1 - hh)

    def piece(half, e):
        near = jnp.where(hh == half, px, 1 - px)
        return pl.ds((2 * half + (near if e == 0 else 1 - near)) * SLICE, SLICE)

    def ring(a, n, e):
        origin = lax.rem(z - dz * (n // 2) + 8, 8)
        spot = gathered[a].at[origin, piece(half_of(n), e), :]
        return remote(spot, spot, s_rg.at[a, n, e], r_rg.at[a, n, e], (m, znext, x, yl, c))

    def across(a, n, e):
        k = n - 1
        big = gathered[a]
        if n == 0:
            spot = big.at[z, piece(c, e), :]
        else:
            origin = lax.rem(z - dz * (k // 2 + 1) + 8, 8)
            spot = big.at[origin, piece(half_of(k), e), :]
        return remote(spot, spot, s_dd.at[a, n, e], r_dd.at[a, n, e], sib)

    def s1_arrived(a, e):
        near = jnp.where(hh == c, px, 1 - px)
        u = near if e == 0 else 1 - near
        own = (2 * c + u == x) & home

        @pl.when(jnp.logical_not(own))
        def _():
            src, dst = weights_of(a), gathered[a]
            remote(
                src, dst.at[z, pl.ds((2 * c + u) * SLICE, SLICE), :],
                s_s1.at[a, 0], r_s1.at[a, u], sib,
            ).wait_recv()

    collector = hh == c

    def set_off(n, e, arrays=(0, 1)):
        gathers = collector if n == 0 else jnp.logical_not(collector)

        @pl.when(gathers)
        def _():
            for a in arrays:
                s1_arrived(a, e)
                ring(a, n, e).start()
                if (n, e) == (0, 0):

                    @pl.when(home)
                    def _():
                        across(a, 0, e).start()
                else:
                    across(a, 0, e).start()

        @pl.when(jnp.logical_not(gathers))
        def _():
            for a in arrays:
                if (n, e) == (0, 0):

                    @pl.when(away)
                    def _():
                        across(a, 0, e).wait_recv()
                else:
                    across(a, 0, e).wait_recv()
                ring(a, n, e).start()

    def share(a, t, y2):
        h2 = 2 * y2 + t
        src, dst = ((val, vals), (cot, cots))[a]
        return remote(
            src.at[:, h2 * 640 : (h2 + 1) * 640],
            dst.at[pl.ds((2 * yl + c) * 128, 128), :],
            s_v.at[a, t, y2], r_v.at[a, 2 * yl + c], (m, z, 2 * pair + t, y2, px),
        )

    def keep(a):
        src, dst = ((val, vals), (cot, cots))[a]
        return pltpu.make_async_copy(
            src.at[:, pl.ds(pl.multiple_of((2 * yl + px) * 640, 128), 640)],
            dst.at[pl.ds((2 * yl + c) * 128, 128), :],
            s_self.at[a],
        )

    def shares(x_moves, y_moves):
        for t in range(2):
            for y2 in range(2):
                own = (2 * pair + t == x) & (y2 == yl) & home
                kind = ((2 * pair + t != x) == x_moves) & ((y2 != yl) == y_moves)

                @pl.when(kind & jnp.logical_not(own))
                def _():
                    share(1, t, y2).start()
                    share(0, t, y2).start()

    set_off(0, 0)
    shares(False, True)
    shares(False, False)

    @pl.when(home)
    def _():
        keep(0).start()
        keep(1).start()


    send_lat = remote(lat, latb, s_l, r_l, (m, z, 2 * pair + 1 - px, yl, px))

    @pl.when(home)
    def _():
        latf[...] = jnp.zeros((8, 512), F32)
        latf[0:3, :] = lat[...].astype(F32)

    @pl.when(home)
    def _():
        send_lat.start()

    buf1[x] = shl[x, :, :, window]
    for j in range(1, 4):
        m1(j).wait_recv()
    for j in range(2):
        lower = [buf1[a, j, :, 0:128] for a in range(4)]
        upper = [buf1[a, j, :, 128:256] for a in range(4)]
        tiles = [lower[0], *(upper[a] + lower[a + 1] for a in range(3)), upper[3]]
        total = jnp.concatenate(tiles, axis=1)
        for k in range(8):
            tot[k, j : j + 1, :] = total[k : k + 1, :]

    def m2(j):
        to = lax.rem(z + j, 8)
        return remote(tot.at[to], buf2.at[z], s_m2.at[j], r_m2.at[j], (m, to, x, yl, c))

    for j in range(1, 8):
        m2(j).start()
    buf2[z] = tot[z]

    set_off(0, 1)
    s1_sends(True)
    s1_sends(False, (2,))
    s1_sends(True, (2,))
    set_off(1, 0)

    for j in range(1, 8):
        m2(j).wait_recv()
    for k in range(8):
        mod[:, k * 640 : (k + 1) * 640] = buf2[k]
    loads[2].wait()

    def r1(t, k):
        return remote(
            made.at[pl.ds(k * ROW_CHUNK, ROW_CHUNK), :],
            rows.at[pl.ds((2 * yl + c) * 128 + k * ROW_CHUNK, ROW_CHUNK), :],
            s_r1.at[t, k], r_r1.at[c, k], (m, z, 2 * pair + t, yl, px),
        )

    for k in range(4):

        @pl.loop(0, ROW_CHUNK // 16)
        def _(i):
            at = pl.multiple_of(k * ROW_CHUNK + i * 16, 16)
            hidden = tok[pl.ds(at, 16), :].astype(F32)
            average = jnp.mean(hidden, axis=1, keepdims=True)
            centred = hidden - average
            variance = jnp.mean(centred * centred, axis=1, keepdims=True)
            normed = centred * lax.rsqrt(variance + 1e-06)
            made[pl.ds(at, 16), :] = (normed * (1.0 + mod[1:2, :]) + mod[0:1, :]).astype(BF)

        for t in range(2):
            own = (2 * pair + t == x) & home

            @pl.when(jnp.logical_not(own))
            def _():
                r1(t, k).start()

            @pl.when(own)
            def _():
                at = pl.multiple_of((2 * yl + c) * 128 + k * ROW_CHUNK, ROW_CHUNK)
                rows[pl.ds(at, ROW_CHUNK), :] = made[k * ROW_CHUNK : (k + 1) * ROW_CHUNK, :]

    def r2(p, k, ylo):
        spot = rows.at[pl.ds((2 * ylo + p) * 128 + k * ROW_CHUNK, ROW_CHUNK), :]
        return remote(spot, spot, s_r2.at[p, k], r_r2.at[p, k], up if p == 0 else down)

    def relay(k):
        for p in range(2):
            own = home & (c == p)

            @pl.when(jnp.logical_not(own))
            def _():
                spot = rows.at[pl.ds((2 * yl + p) * 128 + k * ROW_CHUNK, ROW_CHUNK), :]
                remote(
                    made.at[pl.ds(k * ROW_CHUNK, ROW_CHUNK), :],
                    spot, s_r1.at[0, k], r_r1.at[p, k], sib,
                ).wait_recv()

            r2(p, k, yl).start()

    @pl.when(home)
    def _():
        for k in range(4):
            relay(k)

    set_off(1, 1)
    shares(True, False)


    @pl.when(away)
    def _():
        send_lat.wait_recv()
        latf[...] = jnp.zeros((8, 512), F32)
        latf[0:3, :] = latb[...].astype(F32)

    @pl.loop(0, 4)
    def _(i):
        at = pl.multiple_of(i * BLOCK, BLOCK)
        angles = lax.dot_general(
            latf[:, pl.ds(at, BLOCK)], rope_frequency(), (((0,), (0,)), ((), ())),
            precision=lax.Precision.HIGHEST, preferred_element_type=F32,
        )
        column = lax.broadcasted_iota(jnp.int32, (BLOCK, HEAD_SIZE), 1)
        cosb[pl.ds(at, BLOCK), :] = jnp.cos(angles)
        sine = jnp.sin(angles)
        sinb[pl.ds(at, BLOCK), :] = jnp.where(column < HEAD_SIZE // 2, -sine, sine)

    def ring_step(n):
        for e in range(2):
            for a in range(2):
                ring(a, n, e).wait_recv()
                if n < 4:
                    ring(a, n + 2, e).start()
                across(a, n + 1, e).start()
        if n >= 4:

            @pl.when(collector if n == 4 else jnp.logical_not(collector))
            def _():
                for a in range(2):
                    for e in range(2):
                        ring(a, 6, e).start()

    def relay_away(k):
        @pl.when(away)
        def _():
            relay(k)

    def rest_step(n):
        for e in range(2):
            ring(2, n, e).wait_recv()
            if n < 4:
                ring(2, n + 2, e).start()
            across(2, n + 1, e).start()
        if n >= 4 and n < 6:

            @pl.when(collector if n == 4 else jnp.logical_not(collector))
            def _():
                for e in range(2):
                    ring(2, 6, e).start()

    ring_step(0)
    ring_step(1)
    ring_step(2)
    relay_away(0)
    ring_step(3)
    relay_away(1)
    ring_step(4)
    relay_away(2)
    ring_step(5)
    for n in range(2):
        for e in range(2):
            set_off(n, e, (2,))
    relay_away(3)

    def project(a, zo, first, part=None):
        acc, big = (kacc, qacc, qacc)[a], gathered[a]
        lanes = (slice(None), lanes_a, lanes_b)[a]
        cols = pl.ds(pl.multiple_of(zo * 640, 128), 640)

        at = slice(None) if part is None else pl.ds(pl.multiple_of(part * 256, 256), 256)
        term = jnp.dot(rows[at, cols], big[zo], preferred_element_type=F32)
        acc[at, lanes] = term if first else acc[at, lanes] + term

    def at_distance(d):
        return lax.rem(z + d + 8, 8)

    def near_slices(part):
        for a in range(2):
            project(a, z, True, part)

        @pl.loop(0, 4)
        def _(i):
            d = jnp.where(i == 0, 1, jnp.where(i == 1, -1, jnp.where(i == 2, 2, -2)))
            for a in range(2):
                project(a, at_distance(d), False, part)

    def crossed(*steps):
        for n in steps:
            for a in range(2):
                for e in range(2):
                    across(a, n, e).wait_recv()

    def last_in(a, e):
        ring(a, 6, e).wait_recv()
        across(a, 7, e).start()

    crossed(1, 2, 3, 4)
    near_slices(yl)
    for a in range(2):
        for e in range(2):
            last_in(a, e)
    rest_step(0)
    for k in range(4):
        for p in range(2):
            r2(p, k, 1 - yl).wait_recv()

    shares(True, True)
    rest_step(1)
    near_slices(1 - yl)
    rest_step(2)
    crossed(5, 6)

    @pl.loop(0, 2)
    def _(i):
        for a in range(2):
            project(a, at_distance(3 - 6 * i), False)


    def last_step(a):
        for e in range(2):
            across(a, 7, e).wait_recv()
        project(a, at_distance(4), False)


    def turned(pre, at):
        inverse = lax.rsqrt(jnp.mean(pre * pre, axis=1, keepdims=True) + 1e-06)
        normed = pre * inverse
        rotated = normed * cosb[at, :] + pltpu.roll(normed, HEAD_SIZE // 2, 1) * sinb[at, :]
        return inverse, normed, rotated.astype(BF)

    rest_step(3)
    last_step(0)

    @pl.loop(0, 4)
    def _(i):
        at = pl.ds(pl.multiple_of(i * BLOCK, BLOCK), BLOCK)
        for j in range(3):
            lanes = pl.ds(pl.multiple_of((2 * m + j) * 128, 128), 128)
            krot[at, lanes] = turned(kacc[at, j * 128 : (j + 1) * 128], at)[2]

    def keys(who):
        spot = krot.at[:, pl.ds(pl.multiple_of(who * KW, 128), 256)]
        return remote(spot, spot, s_k, r_k, mate)

    keys(m).start()
    last_step(1)
    rest_step(4)

    for hd in range(4):
        own = home & (hd == 2 * yl + c)

        @pl.when(jnp.logical_not(own))
        def _():
            for a, (src, dst) in enumerate(((val, vals), (cot, cots))):
                remote(
                    src.at[:, 0:640], dst.at[hd * 128 : (hd + 1) * 128, :],
                    s_v.at[a, 0, 0], r_v.at[a, hd], sib,
                ).wait_recv()

    @pl.when(home)
    def _():
        keep(0).wait()
        keep(1).wait()

    scale = HEAD_SIZE ** (-0.5)

    def one_block(lanes, at):
        inverse, normed, query = turned(qacc[at, lanes], at)
        key, value = krot[:, lanes], vals[:, lanes]
        nt = (((1,), (1,)), ((), ()))
        scores = lax.dot_general(query, key, nt, preferred_element_type=F32)
        raised = jnp.exp2(scores * (scale * math.log2(math.e)))
        grad_probs = lax.dot_general(cots[at, lanes], value, nt, preferred_element_type=F32)
        share_of = 1.0 / jnp.sum(raised, axis=1, keepdims=True)
        probs = raised * share_of
        inner = jnp.sum(probs * grad_probs, axis=1, keepdims=True)
        grad_scores = (probs * (grad_probs - inner)).astype(BF)
        turn = jnp.dot(grad_scores, key, preferred_element_type=F32) * scale
        grad = turn * cosb[at, :] + pltpu.roll(turn * sinb[at, :], HEAD_SIZE // 2, 1)
        mean = jnp.mean(grad * normed, axis=1, keepdims=True)
        gq[at, lanes] = (inverse * (grad - normed * mean)).astype(BF)

    def attend(first, count):
        @pl.loop(0, count)
        def _(i):
            lanes = pl.ds(pl.multiple_of((first + i) * 128, 128), 128)
            for b in range(512 // QUERY):
                one_block(lanes, pl.ds(b * QUERY, QUERY))

    copy_q = remote(wqv, qo, s_q, r_q, mate)
    copy_q.start()

    mine, other = pl.ds(c * HALF, HALF), pl.ds((1 - c) * HALF, HALF)

    def zat(j):
        return lax.rem(z + dz * j + 16, 8)

    class Reduce:
        def __init__(self, g, lane, bufs):
            self.g, self.width = g, bufs[0].shape[2]
            self.lanes = pl.ds(pl.multiple_of(lane, 128), self.width)
            (self.own, self.sib, self.got, self.arrived, self.out, self.last, self.last_got,
             self.last_arr, self.fin) = bufs

        def squares(self, zs, dst):
            cols = pl.ds(pl.multiple_of(zs * 640, 128), 640)
            g = lax.dot_general(
                rows[:, cols], gq[:, self.lanes], (((0,), (0,)), ((), ())),
                preferred_element_type=F32,
            )
            dst[...] = (g * g).astype(BF)

        def pass_on(self, q):
            if q == 0:
                src, dst = self.own.at[3, other, :], self.got.at[3, other, :]
            elif q < 4:
                src, dst = self.sib.at[3 - q], self.got.at[3 - q]
            elif q == 4:
                src, dst = self.last.at[other, :], self.last_got
            else:
                src, dst = self.arrived.at[5, q - 5], self.last_arr.at[q - 5]
            return remote(src, dst, s_sd.at[self.g, q], r_sd.at[self.g, q], sib)

        def passed(self, q):
            if q == 0:
                return remote(
                    self.own.at[3, mine, :], self.got.at[3, mine, :],
                    s_sd.at[self.g, q], r_sd.at[self.g, q], sib,
                )
            return self.pass_on(q)

        def sums(self, n, u):
            return remote(
                self.out.at[n, u], self.arrived.at[n, u], s_sr.at[self.g, n, u],
                r_sr.at[self.g, n, u], (m, znext, x, yl, c),
            )

        def send_on(self, n):
            j = (8 - n) // 2 - 1
            base = (c if n % 2 == 0 else 1 - c) * HALF
            for u in range(2):
                if n >= 2:
                    self.sums(n - 2, u).wait_recv()

                @pl.loop(0, SLICE // 32)
                def _(i):
                    at = pl.ds(pl.multiple_of(i * 32, 32), 32)
                    far = pl.ds(pl.multiple_of(base + u * SLICE + i * 32, 32), 32)
                    total = self.own[j, far, :].astype(F32) + self.got[j, far, :].astype(F32)
                    if n >= 2:
                        total = total + self.arrived[n - 2, u, at, :].astype(F32)
                    self.out[n, u, at, :] = total.astype(BF)

                self.sums(n, u).start()

        def start(self):
            self.squares(zat(4), self.own.at[3])
            self.pass_on(0).start()
            self.squares(zat(-3), self.sib.at[2])
            self.pass_on(1).start()
            self.passed(0).wait_recv()
            self.send_on(0)
            self.squares(zat(3), self.own.at[2])
            self.passed(1).wait_recv()
            self.send_on(1)

        def middle(self, k):
            self.squares(zat(k - 4), self.sib.at[3 - k])
            self.pass_on(k).start()
            self.squares(zat(4 - k), self.own.at[3 - k])
            self.send_on(2 * k - 2)
            self.passed(k).wait_recv()
            self.send_on(2 * k - 1)

        def own_slice(self):
            self.squares(z, self.last)
            self.pass_on(4).start()

        def xs(self, u):
            return remote(
                self.fin.at[u], xb.at[hh, :, self.lanes], s_x.at[self.g, u], r_x.at[self.g, hh],
                (m, z, 2 * c + u, yl, px),
            )

        def finish(self):
            for u in range(2):
                self.sums(5, u).wait_recv()
                self.pass_on(5 + u).start()
            self.passed(4).wait_recv()
            for u in range(2):
                self.passed(5 + u).wait_recv()
                self.sums(6, u).wait_recv()

                @pl.loop(0, SLICE // 32)
                def _(i):
                    at = pl.ds(pl.multiple_of(i * 32, 32), 32)
                    near = pl.ds(pl.multiple_of(u * SLICE + i * 32, 32), 32)
                    far = pl.ds(pl.multiple_of(c * HALF + u * SLICE + i * 32, 32), 32)
                    total = self.last[far, :].astype(F32) + self.last_got[near, :].astype(F32)
                    total = total + self.arrived[6, u, at, :].astype(F32)
                    total = total + self.last_arr[u, at, :].astype(F32)
                    self.fin[u, at, :] = total.astype(BF)

                own = (2 * c + u == x) & home

                @pl.when(jnp.logical_not(own))
                def _():
                    self.xs(u).start()

                @pl.when(own)
                def _():
                    xb[hh, :, self.lanes] = self.fin[u]

        def weigh(self):
            for t in range(2):
                own = (c + 2 * t == x) & (hh == c)

                @pl.when(jnp.logical_not(own))
                def _():
                    remote(
                        self.fin.at[0], xb.at[t, :, self.lanes], s_x.at[self.g, 0],
                        r_x.at[self.g, t], sib,
                    ).wait_recv()

            fisher = xb[0, :, self.lanes].astype(F32) + xb[1, :, self.lanes].astype(F32)
            wo[:, self.lanes] = (fisher + damping).astype(BF)
            self.mate_copy().start()

        def mate_copy(self):
            return remote(
                wo.at[:, self.lanes], wi.at[:, self.lanes], s_w.at[self.g], r_w.at[self.g], mate
            )

        def drain(self):
            for n in range(7):
                for u in range(2):
                    self.sums(n, u).wait_send()
            for q in range(7):
                self.pass_on(q).wait_send()
            for u in range(2):
                own = (2 * c + u == x) & home

                @pl.when(jnp.logical_not(own))
                def _():
                    self.xs(u).wait_send()

            self.mate_copy().wait()

    part_a = Reduce(0, m * 256, (own_a, sib_a, got_a, arr_a, out_a, last_a, lgot_a, larr_a, fin_a))
    part_b = Reduce(
        1, (1 - m) * KW, (own_b, sib_b, got_b, arr_b, out_b, last_b, lgot_b, larr_b, fin_b)
    )

    attend(2 * m, 1)
    rest_step(5)
    attend(2 * m + 1, 2)
    part_a.start()
    rest_step(6)
    for n in range(1, 8):
        for e in range(2):
            across(2, n, e).wait_recv()
    project(2, 0, True)

    @pl.loop(1, 8)
    def _(i):
        project(2, i, False)

    part_a.middle(2)
    keys(1 - m).wait_recv()
    attend(3 - 3 * m, 2)
    part_b.start()
    part_a.middle(3)
    part_b.middle(2)
    part_a.own_slice()
    part_a.send_on(6)
    part_b.middle(3)
    part_b.own_slice()
    part_a.finish()
    part_b.send_on(6)
    part_b.finish()
    part_a.weigh()
    part_b.weigh()

    for j in range(1, 4):
        m1(j).wait_send()
    for j in range(1, 8):
        m2(j).wait_send()

    @pl.when(home)
    def _():
        send_lat.wait_send()

    for t in range(2):
        own = (c + 2 * t == x) & (hh == c)

        @pl.when(jnp.logical_not(own))
        def _():
            for a in range(3):
                s1(a, t).wait_send()

        own_r = (2 * pair + t == x) & home

        @pl.when(jnp.logical_not(own_r))
        def _():
            for k in range(4):
                r1(t, k).wait_send()

        for y2 in range(2):
            own_v = (2 * pair + t == x) & (y2 == yl) & home

            @pl.when(jnp.logical_not(own_v))
            def _():
                share(0, t, y2).wait_send()
                share(1, t, y2).wait_send()

    for a in range(3):
        for e in range(2):
            for n in range(7):
                ring(a, n, e).wait_send()
            for n in range(1, 8):
                across(a, n, e).wait_send()
        across(a, 0, 1).wait_send()

        @pl.when(jnp.logical_not(collector & away))
        def _():
            across(a, 0, 0).wait_send()
    for k in range(4):
        for p in range(2):
            r2(p, k, yl).wait_send()
    keys(m).wait_send()
    copy_q.wait()
    part_a.drain()
    part_b.drain()


def step(timestep, tw, lattice, tokens, own_query, own_key, values, cotangent):
    vmem = pl.BlockSpec(memory_space=pltpu.VMEM)
    hbm = pl.BlockSpec(memory_space=pltpu.HBM)
    dma = pltpu.SemaphoreType.DMA

    def v(shape, dtype=BF):
        return pltpu.VMEM(shape, dtype)

    def in_hbm(a):
        return pltpu.with_memory_space_constraint(a, pltpu.HBM)

    def sums_of(width):
        return (
            v((4, 640, width)), v((3, 640, width)), v((4, 640, width)),
            v((7, 2, SLICE, width)), v((7, 2, SLICE, width)),
            v((640, width)), v((HALF, width)), v((2, SLICE, width)), v((2, SLICE, width)),
        )

    return pl.pallas_call(
        kernel,
        out_shape=(
            jax.ShapeDtypeStruct((2, SLICE, 640), BF),
            jax.ShapeDtypeStruct((SLICE, 640), BF),
            jax.ShapeDtypeStruct((SLICE, 640), BF),
            jax.ShapeDtypeStruct((SLICE, 640), BF),
        ),
        in_specs=[pl.BlockSpec(memory_space=pltpu.SMEM)] + [hbm] * 7,
        out_specs=(vmem,) * 4,
        scratch_shapes=[
            v((SLICE, 640)), v((128, 5120)), v((SLICE, KW)), v((8, 640, KW)), v((8, 640, 256)), v((8, 640, KW)),
            v((512, 5120)), v((512, 640)), v((512, 640)), v((128, 5120)),
            v((2, SLICE, 256)), v((3, 512), jnp.int32), v((32, 128), F32), v((2, 640, 256)), v((4, 2, 8, 640), F32), v((4, 2, 8, 256), F32),
            v((8, 2, 640), F32), v((8, 2, 640), F32), v((2, 5120), F32),
            v((3, 512), jnp.int32), v((8, 512), F32), v((512, 128), F32), v((512, 128), F32),
            v((512, 640), F32), v((512, KW), F32), v((512, 640)), v((512, 640)),
            *sums_of(KW), *sums_of(256),
            dma((8,)), dma((2,)), dma, dma,
            dma((4,)), dma((4,)), dma((8,)), dma((8,)), dma((3, 2)), dma((3, 2)),
            dma((3, 7, 2)), dma((3, 7, 2)), dma((3, 8, 2)), dma((3, 8, 2)),
            dma((2, 4)), dma((2, 4)), dma((2, 4)), dma((2, 4)), dma((2, 2, 2)), dma((2, 4)),
            dma, dma,
            dma((2, 7)), dma((2, 7)), dma((2, 7, 2)), dma((2, 7, 2)), dma((2, 2)), dma((2, 2)),
            dma, dma, dma((2,)), dma((2,)),
        ],
        compiler_params=pltpu.CompilerParams(
            collective_id=0, has_side_effects=True, vmem_limit_bytes=52 * 1024 * 1024
        ),
        name="fisher_step",
    )(in_hbm(timestep), *(in_hbm(a) for a in (tw, lattice, tokens, own_query, own_key, values, cotangent)))


def on_device(tokens, lattice, timestep, time_weight, query_weight, key_weight, values, cotangent):
    member = lax.axis_index("member")
    xb, other, qo, mine = step(
        timestep, time_weight.transpose(0, 2, 1), lattice, tokens,
        query_weight[0], key_weight, values, cotangent[0],
    )
    fisher = xb[0].astype(F32) + xb[1].astype(F32)
    first = member == 0
    own, other = lax.reduce_precision(fisher + damping, 8, 7), other.astype(F32)
    w0, w1 = jnp.where(first, own, other), jnp.where(first, other, own)
    q0, q1 = jnp.where(first, mine, qo).astype(F32), jnp.where(first, qo, mine).astype(F32)
    return (fisher[None], (w0 * q0 + w1 * q1) / (w0 + w1))


def solution(mesh):
    finer = Mesh(mesh.devices.reshape(mesh.shape["member"], 8, 4, 2, 2), AXES)
    in_specs = (
        P(SEQ_HEAD, None),
        P(None, SEQ),
        P(),
        P(None, None, SEQ),
        P("member", SEQ, HEAD),
        P(SEQ, HEAD),
        P(SEQ_HEAD, None),
        P("member", SEQ_HEAD, None),
    )
    out_specs = (P("member", SEQ, HEAD), P(SEQ, HEAD))
    return jax.shard_map(
        on_device, mesh=finer, in_specs=in_specs, out_specs=out_specs, check_vma=False
    )
```

```python
import math

import jax
import jax.numpy as jnp
from jax import lax
from jax.experimental import pallas as pl
from jax.experimental.pallas import tpu as pltpu
from jax.sharding import Mesh
from jax.sharding import PartitionSpec as P

HEAD_SIZE = 128
AXES = ("member", "z", "x", "ylo", "core")
SEQ = ("z", "x")
HEAD = ("ylo", "core")
SEQ_HEAD = ("z", "x", "ylo", "core")
MESH = pl.DeviceIdType.MESH

damping = 0.01
SLICE = 160
HALF = 320
KW = 384
ROW_CHUNK = 32
BLOCK = 128
QUERY = 256
F32, BF = jnp.float32, jnp.bfloat16


def place():
    return tuple(lax.axis_index(a) for a in AXES)


def remote(src, dst, send, recv, to):
    return pltpu.make_async_remote_copy(
        src_ref=src, dst_ref=dst, send_sem=send, recv_sem=recv, device_id=to, device_id_type=MESH
    )


def hello(to):
    pl.semaphore_signal(pltpu.get_barrier_semaphore(), inc=1, device_id=to, device_id_type=MESH)


def rope_frequency():
    halfway, side = HEAD_SIZE // 2, HEAD_SIZE // 6
    frame = halfway - 2 * side
    shape = (8, HEAD_SIZE)
    row = lax.broadcasted_iota(jnp.int32, shape, 0)
    column = lax.broadcasted_iota(jnp.int32, shape, 1)
    pair = jnp.where(column < halfway, column, column - halfway)
    axis = jnp.where(pair < frame, 0, jnp.where(pair < frame + side, 1, 2))
    anchor = jnp.where(axis == 0, 0, jnp.where(axis == 1, frame, frame + side))
    span = jnp.where(axis == 0, frame, side).astype(F32)
    frequency = jnp.exp(-math.log(10000.0) * (pair - anchor).astype(F32) / span)
    return jnp.where(row == axis, frequency, 0.0)


def kernel(
    when, tw_hbm, lat_hbm, tok_hbm, wq_hbm, wk_hbm, val, cot,
    xb, wi, qo, wqv,
    wo, tok, wkv, bigq, bigqb, bigk, rows, vals, cots, made,
    tw, lat, ang, wide, shl, buf1, tot, buf2, mod, latb, latf, cosb, sinb,
    qacc, kacc, krot, gq,
    own_a, sib_a, got_a, arr_a, out_a, last_a, lgot_a, larr_a, fin_a,
    own_b, sib_b, got_b, arr_b, out_b, last_b, lgot_b, larr_b, fin_b,
    s_in, s_self, s_l, r_l,
    s_m1, r_m1, s_m2, r_m2, s_s1, r_s1, s_rg, r_rg, s_dd, r_dd,
    s_r1, r_r1, s_r2, r_r2, s_v, r_v, s_k, r_k,
    s_sd, r_sd, s_sr, r_sr, s_x, r_x, s_q, r_q, s_w, r_w,
):
    m, z, x, yl, c = place()
    px, pair, hh = lax.rem(x, 2), x // 2, x // 2
    sib = (m, z, x, yl, 1 - c)
    mate = (1 - m, z, x, yl, c)
    dz = 1 - 2 * c
    znext = lax.rem(z + dz + 8, 8)
    home = c == px
    up = (jnp.where(yl == 0, m, 1 - m), z, x, 1 - yl, c)
    down = (jnp.where(yl == 0, 1 - m, m), z, x, 1 - yl, c)
    away = jnp.logical_not(home)

    loads = [
        pltpu.make_async_copy(wk_hbm.at[:, pl.ds(pl.multiple_of(m * 256, 128), KW)], wkv, s_in.at[0]),
        pltpu.make_async_copy(wq_hbm, wqv, s_in.at[1]),
        pltpu.make_async_copy(tok_hbm, tok, s_in.at[2]),
        pltpu.make_async_copy(tw_hbm, tw, s_in.at[5]),
        pltpu.make_async_copy(lat_hbm, lat, s_in.at[6]),
    ]
    for load in loads:
        load.start()
    lanes_a = pl.ds(pl.multiple_of(m * 256, 128), KW)
    lanes_b = pl.ds(pl.multiple_of((1 - m) * KW, 128), 256)
    gathered = (bigk, bigq, bigqb)

    def weights_of(a):
        return (wkv, wqv.at[:, lanes_a], wqv.at[:, lanes_b])[a]

    own_weights = [
        pltpu.make_async_copy(
            wk_hbm.at[:, lanes_a], bigk.at[z, pl.ds(x * SLICE, SLICE), :], s_in.at[3]
        ),
        pltpu.make_async_copy(
            wq_hbm.at[:, lanes_a], bigq.at[z, pl.ds(x * SLICE, SLICE), :], s_in.at[4]
        ),
        pltpu.make_async_copy(
            wq_hbm.at[:, lanes_b], bigqb.at[z, pl.ds(x * SLICE, SLICE), :], s_in.at[7]
        ),
    ]

    @pl.when(home)
    def _():
        for load in own_weights:
            load.start()

    for j in range(1, 16):
        q = lax.rem(x * 4 + yl * 2 + c + j, 16)
        hello((m, z, q // 4, lax.rem(q, 4) // 2, lax.rem(q, 2)))
    for j in range(1, 8):
        hello((m, lax.rem(z + j, 8), x, yl, c))
    hello((1 - m, z, x, 1 - yl, c))
    hello(mate)

    ladder = lax.broadcasted_iota(jnp.int32, (1, 128), 1).astype(F32)
    frequency = jnp.exp(-math.log(10000.0) * 2.0 * ladder / 256)
    for a in range(4):
        for b in range(8):
            r = a * 8 + b
            ang[r : r + 1, :] = when[b * 4 + a].astype(F32) * frequency
    loads[3].wait()
    loads[4].wait()
    for j in range(2):
        wide[j] = jnp.zeros((640, 256), BF)
        wide[j, pl.ds(pl.multiple_of(x * SLICE, SLICE), SLICE), :] = tw[j]
    angle = ang[...]
    feature = jnp.concatenate([jnp.cos(angle), jnp.sin(angle)], axis=1).astype(BF)
    for j in range(2):
        part = lax.dot_general(
            feature, wide[j], (((1,), (1,)), ((), ())), preferred_element_type=F32
        )
        for a in range(4):
            shl[a, j] = part[a * 8 : (a + 1) * 8, :]
    for load in loads[:2]:
        load.wait()

    pl.semaphore_wait(pltpu.get_barrier_semaphore(), 24)

    window = pl.ds(pl.multiple_of(x * 128, 128), 256)

    def m1(j):
        to = lax.rem(x + j, 4)
        return remote(
            shl.at[to, :, :, window], buf1.at[x], s_m1.at[j], r_m1.at[j], (m, z, to, yl, c)
        )

    for j in range(1, 4):
        m1(j).start()

    def s1(a, t):
        src, dst = weights_of(a), gathered[a]
        return remote(
            src, dst.at[z, pl.ds(x * SLICE, SLICE), :], s_s1.at[a, t],
            r_s1.at[a, lax.rem(x, 2)], (m, z, c + 2 * t, yl, hh),
        )

    def s1_sends(two_hops, arrays=(0, 1)):
        for a in arrays:
            for t in range(2):
                own = (c + 2 * t == x) & (hh == c)
                far = home & (c + 2 * t != x)

                @pl.when(far if two_hops else jnp.logical_not(own | far))
                def _():
                    s1(a, t).start()

    s1_sends(False)

    @pl.when(home)
    def _():
        for load in own_weights:
            load.wait()

    def half_of(n):
        return c if n == 6 else (hh if n % 2 == 0 else 1 - hh)

    def piece(half, e):
        near = jnp.where(hh == half, px, 1 - px)
        return pl.ds((2 * half + (near if e == 0 else 1 - near)) * SLICE, SLICE)

    def ring(a, n, e):
        origin = lax.rem(z - dz * (n // 2) + 8, 8)
        spot = gathered[a].at[origin, piece(half_of(n), e), :]
        return remote(spot, spot, s_rg.at[a, n, e], r_rg.at[a, n, e], (m, znext, x, yl, c))

    def across(a, n, e):
        k = n - 1
        big = gathered[a]
        if n == 0:
            spot = big.at[z, piece(c, e), :]
        else:
            origin = lax.rem(z - dz * (k // 2 + 1) + 8, 8)
            spot = big.at[origin, piece(half_of(k), e), :]
        return remote(spot, spot, s_dd.at[a, n, e], r_dd.at[a, n, e], sib)

    def s1_arrived(a, e):
        near = jnp.where(hh == c, px, 1 - px)
        u = near if e == 0 else 1 - near
        own = (2 * c + u == x) & home

        @pl.when(jnp.logical_not(own))
        def _():
            src, dst = weights_of(a), gathered[a]
            remote(
                src, dst.at[z, pl.ds((2 * c + u) * SLICE, SLICE), :],
                s_s1.at[a, 0], r_s1.at[a, u], sib,
            ).wait_recv()

    collector = hh == c

    def set_off(n, e, arrays=(0, 1)):
        gathers = collector if n == 0 else jnp.logical_not(collector)

        @pl.when(gathers)
        def _():
            for a in arrays:
                s1_arrived(a, e)
                ring(a, n, e).start()
                if (n, e) == (0, 0):

                    @pl.when(home)
                    def _():
                        across(a, 0, e).start()
                else:
                    across(a, 0, e).start()

        @pl.when(jnp.logical_not(gathers))
        def _():
            for a in arrays:
                if (n, e) == (0, 0):

                    @pl.when(away)
                    def _():
                        across(a, 0, e).wait_recv()
                else:
                    across(a, 0, e).wait_recv()
                ring(a, n, e).start()

    def share(a, t, y2):
        h2 = 2 * y2 + t
        src, dst = ((val, vals), (cot, cots))[a]
        return remote(
            src.at[:, h2 * 640 : (h2 + 1) * 640],
            dst.at[pl.ds((2 * yl + c) * 128, 128), :],
            s_v.at[a, t, y2], r_v.at[a, 2 * yl + c], (m, z, 2 * pair + t, y2, px),
        )

    def keep(a):
        src, dst = ((val, vals), (cot, cots))[a]
        return pltpu.make_async_copy(
            src.at[:, pl.ds(pl.multiple_of((2 * yl + px) * 640, 128), 640)],
            dst.at[pl.ds((2 * yl + c) * 128, 128), :],
            s_self.at[a],
        )

    def shares(x_moves, y_moves):
        for t in range(2):
            for y2 in range(2):
                own = (2 * pair + t == x) & (y2 == yl) & home
                kind = ((2 * pair + t != x) == x_moves) & ((y2 != yl) == y_moves)

                @pl.when(kind & jnp.logical_not(own))
                def _():
                    share(1, t, y2).start()
                    share(0, t, y2).start()

    set_off(0, 0)
    shares(False, True)
    shares(False, False)

    @pl.when(home)
    def _():
        keep(0).start()
        keep(1).start()


    send_lat = remote(lat, latb, s_l, r_l, (m, z, 2 * pair + 1 - px, yl, px))

    @pl.when(home)
    def _():
        latf[...] = jnp.zeros((8, 512), F32)
        latf[0:3, :] = lat[...].astype(F32)

    @pl.when(home)
    def _():
        send_lat.start()

    buf1[x] = shl[x, :, :, window]
    for j in range(1, 4):
        m1(j).wait_recv()
    for j in range(2):
        lower = [buf1[a, j, :, 0:128] for a in range(4)]
        upper = [buf1[a, j, :, 128:256] for a in range(4)]
        tiles = [lower[0], *(upper[a] + lower[a + 1] for a in range(3)), upper[3]]
        total = jnp.concatenate(tiles, axis=1)
        for k in range(8):
            tot[k, j : j + 1, :] = total[k : k + 1, :]

    def m2(j):
        to = lax.rem(z + j, 8)
        return remote(tot.at[to], buf2.at[z], s_m2.at[j], r_m2.at[j], (m, to, x, yl, c))

    for j in range(1, 8):
        m2(j).start()
    buf2[z] = tot[z]

    set_off(0, 1)
    s1_sends(True)
    s1_sends(False, (2,))
    s1_sends(True, (2,))
    set_off(1, 0)

    for j in range(1, 8):
        m2(j).wait_recv()
    for k in range(8):
        mod[:, k * 640 : (k + 1) * 640] = buf2[k]
    loads[2].wait()

    def r1(t, k):
        return remote(
            made.at[pl.ds(k * ROW_CHUNK, ROW_CHUNK), :],
            rows.at[pl.ds((2 * yl + c) * 128 + k * ROW_CHUNK, ROW_CHUNK), :],
            s_r1.at[t, k], r_r1.at[c, k], (m, z, 2 * pair + t, yl, px),
        )

    for k in range(4):

        @pl.loop(0, ROW_CHUNK // 16)
        def _(i):
            at = pl.multiple_of(k * ROW_CHUNK + i * 16, 16)
            hidden = tok[pl.ds(at, 16), :].astype(F32)
            average = jnp.mean(hidden, axis=1, keepdims=True)
            centred = hidden - average
            variance = jnp.mean(centred * centred, axis=1, keepdims=True)
            normed = centred * lax.rsqrt(variance + 1e-06)
            made[pl.ds(at, 16), :] = (normed * (1.0 + mod[1:2, :]) + mod[0:1, :]).astype(BF)

        for t in range(2):
            own = (2 * pair + t == x) & home

            @pl.when(jnp.logical_not(own))
            def _():
                r1(t, k).start()

            @pl.when(own)
            def _():
                at = pl.multiple_of((2 * yl + c) * 128 + k * ROW_CHUNK, ROW_CHUNK)
                rows[pl.ds(at, ROW_CHUNK), :] = made[k * ROW_CHUNK : (k + 1) * ROW_CHUNK, :]

    def r2(p, k, ylo):
        spot = rows.at[pl.ds((2 * ylo + p) * 128 + k * ROW_CHUNK, ROW_CHUNK), :]
        return remote(spot, spot, s_r2.at[p, k], r_r2.at[p, k], up if p == 0 else down)

    def relay(k):
        for p in range(2):
            own = home & (c == p)

            @pl.when(jnp.logical_not(own))
            def _():
                spot = rows.at[pl.ds((2 * yl + p) * 128 + k * ROW_CHUNK, ROW_CHUNK), :]
                remote(
                    made.at[pl.ds(k * ROW_CHUNK, ROW_CHUNK), :],
                    spot, s_r1.at[0, k], r_r1.at[p, k], sib,
                ).wait_recv()

            r2(p, k, yl).start()

    @pl.when(home)
    def _():
        for k in range(4):
            relay(k)

    set_off(1, 1)
    shares(True, False)


    @pl.when(away)
    def _():
        send_lat.wait_recv()
        latf[...] = jnp.zeros((8, 512), F32)
        latf[0:3, :] = latb[...].astype(F32)

    @pl.loop(0, 4)
    def _(i):
        at = pl.multiple_of(i * BLOCK, BLOCK)
        angles = lax.dot_general(
            latf[:, pl.ds(at, BLOCK)], rope_frequency(), (((0,), (0,)), ((), ())),
            precision=lax.Precision.HIGHEST, preferred_element_type=F32,
        )
        column = lax.broadcasted_iota(jnp.int32, (BLOCK, HEAD_SIZE), 1)
        cosb[pl.ds(at, BLOCK), :] = jnp.cos(angles)
        sine = jnp.sin(angles)
        sinb[pl.ds(at, BLOCK), :] = jnp.where(column < HEAD_SIZE // 2, -sine, sine)

    def ring_step(n):
        for e in range(2):
            for a in range(2):
                ring(a, n, e).wait_recv()
                if n < 4:
                    ring(a, n + 2, e).start()
                across(a, n + 1, e).start()
        if n >= 4:

            @pl.when(collector if n == 4 else jnp.logical_not(collector))
            def _():
                for a in range(2):
                    for e in range(2):
                        ring(a, 6, e).start()

    def relay_away(k):
        @pl.when(away)
        def _():
            relay(k)

    def rest_step(n):
        for e in range(2):
            ring(2, n, e).wait_recv()
            if n < 4:
                ring(2, n + 2, e).start()
            across(2, n + 1, e).start()
        if n >= 4 and n < 6:

            @pl.when(collector if n == 4 else jnp.logical_not(collector))
            def _():
                for e in range(2):
                    ring(2, 6, e).start()

    ring_step(0)
    ring_step(1)
    ring_step(2)
    relay_away(0)
    ring_step(3)
    relay_away(1)
    ring_step(4)
    relay_away(2)
    ring_step(5)
    for n in range(2):
        for e in range(2):
            set_off(n, e, (2,))
    relay_away(3)

    def project(a, zo, first, part=None):
        acc, big = (kacc, qacc, qacc)[a], gathered[a]
        lanes = (slice(None), lanes_a, lanes_b)[a]
        cols = pl.ds(pl.multiple_of(zo * 640, 128), 640)

        at = slice(None) if part is None else pl.ds(pl.multiple_of(part * 256, 256), 256)
        term = jnp.dot(rows[at, cols], big[zo], preferred_element_type=F32)
        acc[at, lanes] = term if first else acc[at, lanes] + term

    def at_distance(d):
        return lax.rem(z + d + 8, 8)

    def near_slices(part):
        for a in range(2):
            project(a, z, True, part)

        @pl.loop(0, 4)
        def _(i):
            d = jnp.where(i == 0, 1, jnp.where(i == 1, -1, jnp.where(i == 2, 2, -2)))
            for a in range(2):
                project(a, at_distance(d), False, part)

    def far_slices(part):
        @pl.loop(0, 2)
        def _(i):
            for a in range(2):
                project(a, at_distance(3 - 6 * i), False, part)

    def crossed(*steps):
        for n in steps:
            for a in range(2):
                for e in range(2):
                    across(a, n, e).wait_recv()

    def last_in(a, e):
        ring(a, 6, e).wait_recv()
        across(a, 7, e).start()

    crossed(1, 2, 3, 4)
    near_slices(yl)
    for a in range(2):
        for e in range(2):
            last_in(a, e)
    rest_step(0)
    shares(True, True)
    crossed(5, 6)
    far_slices(yl)
    crossed(7)
    for a in range(2):
        project(a, at_distance(4), False, yl)
    for k in range(4):
        for p in range(2):
            r2(p, k, 1 - yl).wait_recv()

    rest_step(1)
    near_slices(1 - yl)
    rest_step(2)

    far_slices(1 - yl)

    def last_step(a):
        project(a, at_distance(4), False, 1 - yl)


    def turned(pre, at):
        inverse = lax.rsqrt(jnp.mean(pre * pre, axis=1, keepdims=True) + 1e-06)
        normed = pre * inverse
        rotated = normed * cosb[at, :] + pltpu.roll(normed, HEAD_SIZE // 2, 1) * sinb[at, :]
        return inverse, normed, rotated.astype(BF)

    rest_step(3)
    last_step(0)

    @pl.loop(0, 4)
    def _(i):
        at = pl.ds(pl.multiple_of(i * BLOCK, BLOCK), BLOCK)
        for j in range(3):
            lanes = pl.ds(pl.multiple_of((2 * m + j) * 128, 128), 128)
            krot[at, lanes] = turned(kacc[at, j * 128 : (j + 1) * 128], at)[2]

    def keys(who):
        spot = krot.at[:, pl.ds(pl.multiple_of(who * KW, 128), 256)]
        return remote(spot, spot, s_k, r_k, mate)

    keys(m).start()
    last_step(1)
    rest_step(4)

    for hd in range(4):
        own = home & (hd == 2 * yl + c)

        @pl.when(jnp.logical_not(own))
        def _():
            for a, (src, dst) in enumerate(((val, vals), (cot, cots))):
                remote(
                    src.at[:, 0:640], dst.at[hd * 128 : (hd + 1) * 128, :],
                    s_v.at[a, 0, 0], r_v.at[a, hd], sib,
                ).wait_recv()

    @pl.when(home)
    def _():
        keep(0).wait()
        keep(1).wait()

    scale = HEAD_SIZE ** (-0.5)

    def one_block(lanes, at):
        inverse, normed, query = turned(qacc[at, lanes], at)
        key, value = krot[:, lanes], vals[:, lanes]
        nt = (((1,), (1,)), ((), ()))
        scores = lax.dot_general(query, key, nt, preferred_element_type=F32)
        raised = jnp.exp2(scores * (scale * math.log2(math.e)))
        grad_probs = lax.dot_general(cots[at, lanes], value, nt, preferred_element_type=F32)
        share_of = 1.0 / jnp.sum(raised, axis=1, keepdims=True)
        probs = raised * share_of
        inner = jnp.sum(probs * grad_probs, axis=1, keepdims=True)
        grad_scores = (probs * (grad_probs - inner)).astype(BF)
        turn = jnp.dot(grad_scores, key, preferred_element_type=F32) * scale
        grad = turn * cosb[at, :] + pltpu.roll(turn * sinb[at, :], HEAD_SIZE // 2, 1)
        mean = jnp.mean(grad * normed, axis=1, keepdims=True)
        gq[at, lanes] = (inverse * (grad - normed * mean)).astype(BF)

    def attend(first, count):
        @pl.loop(0, count)
        def _(i):
            lanes = pl.ds(pl.multiple_of((first + i) * 128, 128), 128)
            for b in range(512 // QUERY):
                one_block(lanes, pl.ds(b * QUERY, QUERY))

    copy_q = remote(wqv, qo, s_q, r_q, mate)
    copy_q.start()

    mine, other = pl.ds(c * HALF, HALF), pl.ds((1 - c) * HALF, HALF)

    def zat(j):
        return lax.rem(z + dz * j + 16, 8)

    class Reduce:
        def __init__(self, g, lane, bufs):
            self.g, self.width = g, bufs[0].shape[2]
            self.lanes = pl.ds(pl.multiple_of(lane, 128), self.width)
            (self.own, self.sib, self.got, self.arrived, self.out, self.last, self.last_got,
             self.last_arr, self.fin) = bufs

        def squares(self, zs, dst):
            cols = pl.ds(pl.multiple_of(zs * 640, 128), 640)
            g = lax.dot_general(
                rows[:, cols], gq[:, self.lanes], (((0,), (0,)), ((), ())),
                preferred_element_type=F32,
            )
            dst[...] = (g * g).astype(BF)

        def pass_on(self, q):
            if q == 0:
                src, dst = self.own.at[3, other, :], self.got.at[3, other, :]
            elif q < 4:
                src, dst = self.sib.at[3 - q], self.got.at[3 - q]
            elif q == 4:
                src, dst = self.last.at[other, :], self.last_got
            else:
                src, dst = self.arrived.at[5, q - 5], self.last_arr.at[q - 5]
            return remote(src, dst, s_sd.at[self.g, q], r_sd.at[self.g, q], sib)

        def passed(self, q):
            if q == 0:
                return remote(
                    self.own.at[3, mine, :], self.got.at[3, mine, :],
                    s_sd.at[self.g, q], r_sd.at[self.g, q], sib,
                )
            return self.pass_on(q)

        def sums(self, n, u):
            return remote(
                self.out.at[n, u], self.arrived.at[n, u], s_sr.at[self.g, n, u],
                r_sr.at[self.g, n, u], (m, znext, x, yl, c),
            )

        def send_on(self, n):
            j = (8 - n) // 2 - 1
            base = (c if n % 2 == 0 else 1 - c) * HALF
            for u in range(2):
                if n >= 2:
                    self.sums(n - 2, u).wait_recv()

                @pl.loop(0, SLICE // 32)
                def _(i):
                    at = pl.ds(pl.multiple_of(i * 32, 32), 32)
                    far = pl.ds(pl.multiple_of(base + u * SLICE + i * 32, 32), 32)
                    total = self.own[j, far, :].astype(F32) + self.got[j, far, :].astype(F32)
                    if n >= 2:
                        total = total + self.arrived[n - 2, u, at, :].astype(F32)
                    self.out[n, u, at, :] = total.astype(BF)

                self.sums(n, u).start()

        def start(self):
            self.squares(zat(4), self.own.at[3])
            self.pass_on(0).start()
            self.squares(zat(-3), self.sib.at[2])
            self.pass_on(1).start()
            self.passed(0).wait_recv()
            self.send_on(0)
            self.squares(zat(3), self.own.at[2])
            self.passed(1).wait_recv()
            self.send_on(1)

        def middle(self, k):
            self.squares(zat(k - 4), self.sib.at[3 - k])
            self.pass_on(k).start()
            self.squares(zat(4 - k), self.own.at[3 - k])
            self.send_on(2 * k - 2)
            self.passed(k).wait_recv()
            self.send_on(2 * k - 1)

        def own_slice(self):
            self.squares(z, self.last)
            self.pass_on(4).start()

        def xs(self, u):
            return remote(
                self.fin.at[u], xb.at[hh, :, self.lanes], s_x.at[self.g, u], r_x.at[self.g, hh],
                (m, z, 2 * c + u, yl, px),
            )

        def finish(self):
            for u in range(2):
                self.sums(5, u).wait_recv()
                self.pass_on(5 + u).start()
            self.passed(4).wait_recv()
            for u in range(2):
                self.passed(5 + u).wait_recv()
                self.sums(6, u).wait_recv()

                @pl.loop(0, SLICE // 32)
                def _(i):
                    at = pl.ds(pl.multiple_of(i * 32, 32), 32)
                    near = pl.ds(pl.multiple_of(u * SLICE + i * 32, 32), 32)
                    far = pl.ds(pl.multiple_of(c * HALF + u * SLICE + i * 32, 32), 32)
                    total = self.last[far, :].astype(F32) + self.last_got[near, :].astype(F32)
                    total = total + self.arrived[6, u, at, :].astype(F32)
                    total = total + self.last_arr[u, at, :].astype(F32)
                    self.fin[u, at, :] = total.astype(BF)

                own = (2 * c + u == x) & home

                @pl.when(jnp.logical_not(own))
                def _():
                    self.xs(u).start()

                @pl.when(own)
                def _():
                    xb[hh, :, self.lanes] = self.fin[u]

        def weigh(self):
            for t in range(2):
                own = (c + 2 * t == x) & (hh == c)

                @pl.when(jnp.logical_not(own))
                def _():
                    remote(
                        self.fin.at[0], xb.at[t, :, self.lanes], s_x.at[self.g, 0],
                        r_x.at[self.g, t], sib,
                    ).wait_recv()

            fisher = xb[0, :, self.lanes].astype(F32) + xb[1, :, self.lanes].astype(F32)
            wo[:, self.lanes] = (fisher + damping).astype(BF)
            self.mate_copy().start()

        def mate_copy(self):
            return remote(
                wo.at[:, self.lanes], wi.at[:, self.lanes], s_w.at[self.g], r_w.at[self.g], mate
            )

        def drain(self):
            for n in range(7):
                for u in range(2):
                    self.sums(n, u).wait_send()
            for q in range(7):
                self.pass_on(q).wait_send()
            for u in range(2):
                own = (2 * c + u == x) & home

                @pl.when(jnp.logical_not(own))
                def _():
                    self.xs(u).wait_send()

            self.mate_copy().wait()

    part_a = Reduce(0, m * 256, (own_a, sib_a, got_a, arr_a, out_a, last_a, lgot_a, larr_a, fin_a))
    part_b = Reduce(
        1, (1 - m) * KW, (own_b, sib_b, got_b, arr_b, out_b, last_b, lgot_b, larr_b, fin_b)
    )

    attend(2 * m, 1)
    rest_step(5)
    attend(2 * m + 1, 2)
    part_a.start()
    rest_step(6)
    for n in range(1, 8):
        for e in range(2):
            across(2, n, e).wait_recv()
    project(2, 0, True)

    @pl.loop(1, 8)
    def _(i):
        project(2, i, False)

    part_a.middle(2)
    keys(1 - m).wait_recv()
    attend(3 - 3 * m, 2)
    part_b.start()
    part_a.middle(3)
    part_b.middle(2)
    part_a.own_slice()
    part_a.send_on(6)
    part_b.middle(3)
    part_b.own_slice()
    part_a.finish()
    part_b.send_on(6)
    part_b.finish()
    part_a.weigh()
    part_b.weigh()

    for j in range(1, 4):
        m1(j).wait_send()
    for j in range(1, 8):
        m2(j).wait_send()

    @pl.when(home)
    def _():
        send_lat.wait_send()

    for t in range(2):
        own = (c + 2 * t == x) & (hh == c)

        @pl.when(jnp.logical_not(own))
        def _():
            for a in range(3):
                s1(a, t).wait_send()

        own_r = (2 * pair + t == x) & home

        @pl.when(jnp.logical_not(own_r))
        def _():
            for k in range(4):
                r1(t, k).wait_send()

        for y2 in range(2):
            own_v = (2 * pair + t == x) & (y2 == yl) & home

            @pl.when(jnp.logical_not(own_v))
            def _():
                share(0, t, y2).wait_send()
                share(1, t, y2).wait_send()

    for a in range(3):
        for e in range(2):
            for n in range(7):
                ring(a, n, e).wait_send()
            for n in range(1, 8):
                across(a, n, e).wait_send()
        across(a, 0, 1).wait_send()

        @pl.when(jnp.logical_not(collector & away))
        def _():
            across(a, 0, 0).wait_send()
    for k in range(4):
        for p in range(2):
            r2(p, k, yl).wait_send()
    keys(m).wait_send()
    copy_q.wait()
    part_a.drain()
    part_b.drain()


def step(timestep, tw, lattice, tokens, own_query, own_key, values, cotangent):
    vmem = pl.BlockSpec(memory_space=pltpu.VMEM)
    hbm = pl.BlockSpec(memory_space=pltpu.HBM)
    dma = pltpu.SemaphoreType.DMA

    def v(shape, dtype=BF):
        return pltpu.VMEM(shape, dtype)

    def in_hbm(a):
        return pltpu.with_memory_space_constraint(a, pltpu.HBM)

    def sums_of(width):
        return (
            v((4, 640, width)), v((3, 640, width)), v((4, 640, width)),
            v((7, 2, SLICE, width)), v((7, 2, SLICE, width)),
            v((640, width)), v((HALF, width)), v((2, SLICE, width)), v((2, SLICE, width)),
        )

    return pl.pallas_call(
        kernel,
        out_shape=(
            jax.ShapeDtypeStruct((2, SLICE, 640), BF),
            jax.ShapeDtypeStruct((SLICE, 640), BF),
            jax.ShapeDtypeStruct((SLICE, 640), BF),
            jax.ShapeDtypeStruct((SLICE, 640), BF),
        ),
        in_specs=[pl.BlockSpec(memory_space=pltpu.SMEM)] + [hbm] * 7,
        out_specs=(vmem,) * 4,
        scratch_shapes=[
            v((SLICE, 640)), v((128, 5120)), v((SLICE, KW)), v((8, 640, KW)), v((8, 640, 256)), v((8, 640, KW)),
            v((512, 5120)), v((512, 640)), v((512, 640)), v((128, 5120)),
            v((2, SLICE, 256)), v((3, 512), jnp.int32), v((32, 128), F32), v((2, 640, 256)), v((4, 2, 8, 640), F32), v((4, 2, 8, 256), F32),
            v((8, 2, 640), F32), v((8, 2, 640), F32), v((2, 5120), F32),
            v((3, 512), jnp.int32), v((8, 512), F32), v((512, 128), F32), v((512, 128), F32),
            v((512, 640), F32), v((512, KW), F32), v((512, 640)), v((512, 640)),
            *sums_of(KW), *sums_of(256),
            dma((8,)), dma((2,)), dma, dma,
            dma((4,)), dma((4,)), dma((8,)), dma((8,)), dma((3, 2)), dma((3, 2)),
            dma((3, 7, 2)), dma((3, 7, 2)), dma((3, 8, 2)), dma((3, 8, 2)),
            dma((2, 4)), dma((2, 4)), dma((2, 4)), dma((2, 4)), dma((2, 2, 2)), dma((2, 4)),
            dma, dma,
            dma((2, 7)), dma((2, 7)), dma((2, 7, 2)), dma((2, 7, 2)), dma((2, 2)), dma((2, 2)),
            dma, dma, dma((2,)), dma((2,)),
        ],
        compiler_params=pltpu.CompilerParams(
            collective_id=0, has_side_effects=True, vmem_limit_bytes=52 * 1024 * 1024
        ),
        name="fisher_step",
    )(in_hbm(timestep), *(in_hbm(a) for a in (tw, lattice, tokens, own_query, own_key, values, cotangent)))


def on_device(tokens, lattice, timestep, time_weight, query_weight, key_weight, values, cotangent):
    member = lax.axis_index("member")
    xb, other, qo, mine = step(
        timestep, time_weight.transpose(0, 2, 1), lattice, tokens,
        query_weight[0], key_weight, values, cotangent[0],
    )
    fisher = xb[0].astype(F32) + xb[1].astype(F32)
    first = member == 0
    own, other = lax.reduce_precision(fisher + damping, 8, 7), other.astype(F32)
    w0, w1 = jnp.where(first, own, other), jnp.where(first, other, own)
    q0, q1 = jnp.where(first, mine, qo).astype(F32), jnp.where(first, qo, mine).astype(F32)
    return (fisher[None], (w0 * q0 + w1 * q1) / (w0 + w1))


def solution(mesh):
    finer = Mesh(mesh.devices.reshape(mesh.shape["member"], 8, 4, 2, 2), AXES)
    in_specs = (
        P(SEQ_HEAD, None),
        P(None, SEQ),
        P(),
        P(None, None, SEQ),
        P("member", SEQ, HEAD),
        P(SEQ, HEAD),
        P(SEQ_HEAD, None),
        P("member", SEQ_HEAD, None),
    )
    out_specs = (P("member", SEQ, HEAD), P(SEQ, HEAD))
    return jax.shard_map(
        on_device, mesh=finer, in_specs=in_specs, out_specs=out_specs, check_vma=False
    )
```
